64 devices in a mesh: dp: 4 (over x, y), tp: 16 (over z, core).
Axes of the slice: x: 2, y: 2, z: 8, core: 2. Of those that a mesh axis runs over, the one named last changes fastest.
The devices are a block of a 4x4x8 slice.
Arguments:
- x_in: bfloat16 [4096, 6144], P(('dp', 'tp')), parts along dimension 0
- grad_out: bfloat16 [4096, 6144], P(('dp', 'tp')), parts along dimension 0
- positions: int32 [4096], P('dp'), parts along dimension 0
- norm_gain: float32 [6144], replicated
- w_query: bfloat16 [6144, 6144], P(None, 'tp')
- w_key: bfloat16 [6144, 1024], replicated
- w_value: bfloat16 [6144, 1024], replicated
- w_out: bfloat16 [6144, 6144], P('tp')
Outputs:
- output 1: bfloat16 [4096, 6144], P(('dp', 'tp')), parts along dimension 0
- output 2: bfloat16 [4096, 6144], P(('dp', 'tp')), parts along dimension 0
- output 3: bfloat16 [24576, 6144], P('dp', 'tp'), parts along dimension 0
- output 4: float32 [24576, 2048], P('dp', 'tp'), parts along dimension 0
- output 5: float32 [24576, 2048], P('dp', 'tp'), parts along dimension 0
- output 6: bfloat16 [24576, 6144], P(('dp', 'tp')), parts along dimension 0
- output 7: float32 [24576], P('dp'), parts along dimension 0
There are 4 independent parts. The reference program is written for one: setup_inputs(seed, part) draws one part's arguments, and reference() takes and returns one part's arrays. A program takes and returns all parts, laid end to end along the dimension named above; an argument that names none is the same for every part.
All inputs are finite; a program needn't handle non-finite values.
Results may differ from the reference program's by a relative error of at most 0.02.
Values are sent between devices in bfloat16 or wider.
A program may use at most 768 MiB of HBM per device.

```python
import functools
import jax
import jax.numpy as jnp
from jax import lax

D_MODEL = 6144
Q_HEADS = 48
KV_HEADS = 8
HEAD_DIM = 128
TP_SIZE = 16
SEQ_LEN = 1024
QUERY_BLOCK = 128
NUM_DOCS = 4
KV_REPEAT = TP_SIZE // KV_HEADS
GROUP_SIZE = Q_HEADS // KV_HEADS
SCORE_SCALE = HEAD_DIM ** -0.5
ROPE_THETA = 1000000.0
NORM_EPS = 1e-05


def draw_positions(pos_key):
    starts = jax.random.randint(pos_key, (NUM_DOCS - 1,), 1, SEQ_LEN)
    tok_idx = jnp.arange(SEQ_LEN, dtype=jnp.int32)
    doc_start = jnp.max(jnp.where(starts[None, :] <= tok_idx[:, None], starts[None, :], 0), axis=1)
    return (tok_idx - doc_start).astype(jnp.int32)


def setup_inputs(seed: int = 0, part: int = 0) -> dict:
    root_key = jax.random.key(seed)
    shared_key, part_root = jax.random.split(root_key)
    part_key = jax.random.fold_in(part_root, part)
    key_x, key_dy, key_pos = jax.random.split(part_key, 3)
    key_g, key_q, key_k, key_v, key_o = jax.random.split(shared_key, 5)
    q_width = Q_HEADS * HEAD_DIM
    kv_width = KV_HEADS * HEAD_DIM
    in_scale = D_MODEL ** -0.5
    x_in = 0.25 * jax.random.normal(key_x, (SEQ_LEN, D_MODEL), jnp.float32)
    grad_out = jax.random.normal(key_dy, (SEQ_LEN, D_MODEL), jnp.float32)
    positions = draw_positions(key_pos)
    norm_gain = jax.random.uniform(key_g, (D_MODEL,), jnp.float32, 0.5, 1.5)
    w_query = jax.random.normal(key_q, (D_MODEL, q_width), jnp.float32) * in_scale
    w_key = jax.random.normal(key_k, (D_MODEL, kv_width), jnp.float32) * in_scale
    w_value = jax.random.normal(key_v, (D_MODEL, kv_width), jnp.float32) * in_scale
    w_out = jax.random.normal(key_o, (q_width, D_MODEL), jnp.float32) * (2.0 * q_width ** -0.5)
    return {'x_in': x_in.astype(jnp.bfloat16), 'grad_out': grad_out.astype(jnp.bfloat16), 'positions': positions, 'norm_gain': norm_gain, 'w_query': w_query.astype(jnp.bfloat16), 'w_key': w_key.astype(jnp.bfloat16), 'w_value': w_value.astype(jnp.bfloat16), 'w_out': w_out.astype(jnp.bfloat16)}


def apply_rope(tensor, cos_t, sin_t):
    half_dim = HEAD_DIM // 2
    t_f32 = tensor.astype(jnp.float32)
    lead_half = t_f32[..., :half_dim]
    tail_half = t_f32[..., half_dim:]
    return jnp.concatenate([lead_half * cos_t - tail_half * sin_t, tail_half * cos_t + lead_half * sin_t], axis=-1).astype(jnp.bfloat16)


def forward_one(x_f32, norm_gain, w_query, w_key_f32, w_value_f32, w_out, positions):
    inv_rms = lax.rsqrt(jnp.mean(x_f32 * x_f32, axis=-1, keepdims=True) + NORM_EPS)
    hidden = (x_f32 * inv_rms * norm_gain).astype(jnp.bfloat16)
    hidden_f32 = hidden.astype(jnp.float32)
    query_proj = jnp.dot(hidden, w_query, preferred_element_type=jnp.float32).astype(jnp.bfloat16)
    key_proj = jnp.dot(hidden_f32, w_key_f32, preferred_element_type=jnp.float32).astype(jnp.bfloat16)
    value_proj = jnp.dot(hidden_f32, w_value_f32, preferred_element_type=jnp.float32).astype(jnp.bfloat16)
    exponents = jnp.arange(0, HEAD_DIM, 2, dtype=jnp.float32) / HEAD_DIM
    angles = positions.astype(jnp.float32)[:, None] * jnp.power(ROPE_THETA, -exponents)[None, :]
    cos_t = jnp.cos(angles)
    sin_t = jnp.sin(angles)
    q_rot = apply_rope(query_proj.reshape(SEQ_LEN, KV_HEADS, GROUP_SIZE, HEAD_DIM), cos_t[:, None, None, :], sin_t[:, None, None, :])
    k_rot = apply_rope(key_proj.reshape(SEQ_LEN, KV_HEADS, HEAD_DIM), cos_t[:, None, :], sin_t[:, None, :])
    key_f32 = k_rot.astype(jnp.float32)
    value_f32 = value_proj.reshape(SEQ_LEN, KV_HEADS, HEAD_DIM).astype(jnp.float32)
    col_idx = jnp.arange(SEQ_LEN, dtype=jnp.int32)
    key_doc = positions - col_idx

    def one_block(blk_item):
        q_blk, q_pos, row_idx = blk_item
        scores = jnp.einsum('qkgd,skd->kgqs', q_blk.astype(jnp.float32), key_f32) * SCORE_SCALE
        keep_mask = (col_idx[None, :] <= row_idx[:, None]) & (key_doc[None, :] == (q_pos - row_idx)[:, None])
        scores = jnp.where(keep_mask, scores, -1e30)
        prob_blk = jax.nn.softmax(scores, axis=-1).astype(jnp.bfloat16).astype(jnp.float32)
        return jnp.einsum('kgqs,skd->qkgd', prob_blk, value_f32).astype(jnp.bfloat16)

    num_blk = SEQ_LEN // QUERY_BLOCK
    blk_out = lax.map(jax.checkpoint(one_block), (q_rot.reshape(num_blk, QUERY_BLOCK, KV_HEADS, GROUP_SIZE, HEAD_DIM), positions.reshape(num_blk, QUERY_BLOCK), col_idx.reshape(num_blk, QUERY_BLOCK)))
    attn_flat = blk_out.reshape(SEQ_LEN, Q_HEADS * HEAD_DIM)
    attn_mix = jnp.dot(attn_flat, w_out, preferred_element_type=jnp.float32)
    return (x_f32 + attn_mix).astype(jnp.bfloat16)


def reference(x_in, grad_out, positions, norm_gain, w_query, w_key, w_value, w_out):
    x_f32 = x_in.astype(jnp.float32)
    forward = functools.partial(forward_one, positions=positions)
    result, pull_back = jax.vjp(forward, x_f32, norm_gain, w_query, w_key.astype(jnp.float32), w_value.astype(jnp.float32), w_out)
    d_x, d_gain, d_wq, d_wk, d_wv, d_wo = pull_back(grad_out)
    copy_shape = (D_MODEL, KV_HEADS, KV_REPEAT, HEAD_DIM)
    grad_wk = jnp.broadcast_to(d_wk.reshape(D_MODEL, KV_HEADS, 1, HEAD_DIM), copy_shape).reshape(D_MODEL, TP_SIZE * HEAD_DIM)
    grad_wv = jnp.broadcast_to(d_wv.reshape(D_MODEL, KV_HEADS, 1, HEAD_DIM), copy_shape).reshape(D_MODEL, TP_SIZE * HEAD_DIM)
    return (result, d_x.astype(jnp.bfloat16), d_wq, grad_wk, grad_wv, d_wo, d_gain)
```

```python
import functools
import jax
import jax.numpy as jnp
from jax import lax
from jax.experimental import pallas as pl
from jax.experimental.pallas import tpu as pltpu
from jax.sharding import PartitionSpec as P

HEAD_DIM = 128
TILE = 128
SUBS = 4
SCORE_SCALE = HEAD_DIM ** -0.5
ROPE_THETA = 1000000.0
NORM_EPS = 1e-05
MASKED = -1e30
MESH = pl.DeviceIdType.MESH
F32 = jnp.float32
BF16 = jnp.bfloat16
ANY = pl.BlockSpec(memory_space=pl.ANY)
VM = pl.BlockSpec(memory_space=pltpu.VMEM)
NT = (((1,), (1,)), ((), ()))
TN = (((0,), (0,)), ((), ()))
VMEM_LIMIT = 63 * 1024 * 1024


def dot(a, b, dims=(((1,), (0,)), ((), ()))):
    return lax.dot_general(a, b, dims, preferred_element_type=F32)


class Ring:
    def __init__(self, tp):
        self.tp = tp
        self.nz = tp // 2
        self.me = lax.axis_index("tp")
        self.c = self.me // 2
        self.k = self.me % 2
        self.up = lax.rem(self.c + 1, self.nz) * 2 + self.k
        self.dn = lax.rem(self.c + self.nz - 1, self.nz) * 2 + self.k
        self.pt = self.c * 2 + 1 - self.k

    def barrier(self):
        bar = pltpu.get_barrier_semaphore()
        for d in (self.up, self.dn, self.pt):
            pl.semaphore_signal(bar, inc=1, device_id={"tp": d}, device_id_type=MESH)
        pl.semaphore_wait(bar, 3)

    def barrier_all(self):
        bar = pltpu.get_barrier_semaphore()
        for o in range(1, self.tp):
            pl.semaphore_signal(bar, inc=1, device_id={"tp": lax.rem(self.me + o, self.tp)}, device_id_type=MESH)
        pl.semaphore_wait(bar, self.tp - 1)

    def chip(self, n):
        return lax.rem(n + 2 * self.nz, self.nz)


def remote(src, dst, ss, rs, dev):
    return pltpu.make_async_remote_copy(src, dst, ss, rs, device_id={"tp": dev}, device_id_type=MESH)


class Gather:
    def __init__(self, rg, src, dst, rows, ss, rs, dss, drs, ls):
        self.rg, self.src, self.dst, self.R = rg, src, dst, rows
        self.ss, self.rs, self.dss, self.drs, self.ls = ss, rs, dss, drs, ls
        self.H = rows // 2
        self.steps = rg.nz - 1

    def rows(self, chip, core, half):
        return pl.ds(pl.multiple_of((self.rg.chip(chip) * 2 + core) * self.R + half * self.H, self.H), self.H)

    def half(self, d, s):
        return s % 2 if d == 0 else 1 - s % 2

    def origin(self, d, s):
        h = (s + 2) // 2
        return self.rg.c - h if d == 0 else self.rg.c + h

    def dev(self, d):
        return self.rg.up if d == 0 else self.rg.dn

    def own(self, d, s):
        h = self.half(d, s)
        return remote(self.src.at[pl.ds(h * self.H, self.H), :], self.dst.at[self.rows(self.rg.c, self.rg.k, h), :],
                      self.ss.at[d, s], self.rs.at[d, s], self.dev(d))

    def recv_rows(self, d, s, core):
        return self.rows(self.origin(d, s), core, self.half(d, s))

    def fwd(self, d, s):
        r = self.recv_rows(d, s - 2, self.rg.k)
        return remote(self.dst.at[r, :], self.dst.at[r, :], self.ss.at[d, s], self.rs.at[d, s], self.dev(d))

    def recv(self, d, s):
        r = self.recv_rows(d, s, self.rg.k)
        return remote(self.dst.at[r, :], self.dst.at[r, :], self.ss.at[d, s], self.rs.at[d, s], self.dev(d))

    def pair(self, i, r):
        return remote(self.dst.at[r, :], self.dst.at[r, :], self.dss.at[i], self.drs.at[i], self.rg.pt)

    def block(self, dev):
        return pl.ds(pl.multiple_of(dev * self.R, self.R), self.R)

    def pair_own(self):
        return remote(self.src, self.dst.at[self.block(self.rg.me), :], self.dss.at[0], self.drs.at[0], self.rg.pt)

    def local(self):
        return pltpu.make_async_copy(self.src, self.dst.at[self.block(self.rg.me), :], self.ls)

    def start_ring(self, s):
        for d in range(2):
            self.own(d, s).start()

    def start_local(self):
        self.local().start()
        self.pair_own().start()

    def tick(self, s, forward=True):
        for d in range(2):
            self.recv(d, s).wait_recv()
            if isinstance(s, int):
                if s + 2 < self.steps:
                    self.fwd(d, s + 2).start()
            else:
                @pl.when(s + 2 < self.steps)
                def _():
                    self.fwd(d, s + 2).start()
            self.pair(1 + 2 * s + d, self.recv_rows(d, s, self.rg.k)).start()

    def wait_pair(self):
        self.local().wait()
        self.pair(0, self.block(self.rg.pt)).wait_recv()
        for s in range(self.steps):
            for d in range(2):
                self.pair(1 + 2 * s + d, self.recv_rows(d, s, 1 - self.rg.k)).wait_recv()

    def drain(self):
        self.pair_own().wait_send()
        for s in range(self.steps):
            for d in range(2):
                self.pair(1 + 2 * s + d, self.recv_rows(d, s, self.rg.k)).wait_send()
                if s < 2:
                    self.own(d, s).wait_send()
                else:
                    self.fwd(d, s).wait_send()

    @staticmethod
    def scratch(tp):
        n = tp // 2 - 1
        dma = pltpu.SemaphoreType.DMA
        return [dma((2, n)), dma((2, n)), dma((1 + 2 * n,)), dma((1 + 2 * n,)), dma]


class Scatter:
    def __init__(self, rg, own, peer, pre, psem, buf, ss, rs, final):
        self.rg, self.own, self.peer, self.pre, self.psem = rg, own, peer, pre, psem
        self.buf, self.ss, self.rs, self.final = buf, ss, rs, final
        self.W = pre.shape[-1]
        self.CW = self.W // SUBS

    def blk(self, d, s):
        return self.rg.chip(self.rg.c - 1 - s) if d == 0 else self.rg.chip(self.rg.c + 1 + s)

    def load(self, w, d, s):
        src = (self.own, self.peer)[w].at[self.blk(d, s), :, pl.ds(d * self.W, self.W)]
        return pltpu.make_async_copy(src, self.pre.at[s % 2, w, d], self.psem.at[s % 2, w, d])

    def loads(self, s):
        return [self.load(w, d, s) for w in range(2) for d in range(2)]

    def send(self, d, u, s):
        return remote(self.buf.at[d, u, s], self.buf.at[d, u, s + 1], self.ss.at[d, u, s], self.rs.at[d, u, s],
                      self.rg.up if d == 0 else self.rg.dn)

    def tick(self, s, u):
        nz = self.rg.nz
        if u == 0:
            for cp in self.loads(s):
                cp.wait()

            @pl.when(s + 1 < nz)
            def _():
                for cp in self.loads(s + 1):
                    cp.start()
        cols = slice(u * self.CW, (u + 1) * self.CW)
        slot = s % 2

        def mine(d):
            return self.pre[slot, 0, d, :, cols].astype(F32) + self.pre[slot, 1, d, :, cols].astype(F32)

        for d in range(2):
            @pl.when(s == 0)
            def _():
                self.buf[d, u, s] = mine(d).astype(BF16)
                self.send(d, u, s).start()

            @pl.when((s > 0) & (s < nz - 1))
            def _():
                self.send(d, u, s - 1).wait_recv()
                self.buf[d, u, s] = (mine(d) + self.buf[d, u, s].astype(F32)).astype(BF16)
                self.send(d, u, s).start()

            @pl.when(s == nz - 1)
            def _():
                self.send(d, u, s - 1).wait_recv()
                self.final(d, u, mine(d) + self.buf[d, u, s].astype(F32))

    def drain(self):
        @pl.loop(0, self.rg.nz - 1)
        def _(s):
            for d in range(2):
                for u in range(SUBS):
                    self.send(d, u, s).wait_send()

    @staticmethod
    def scratch(tp, rows, d_model):
        nz = tp // 2
        dma = pltpu.SemaphoreType.DMA
        W = d_model // 2
        return [pltpu.VMEM((2, 2, 2, rows, W), BF16), dma((2, 2, 2)), pltpu.VMEM((2, SUBS, nz, rows, W // SUBS), BF16),
                dma((2, SUBS, nz - 1)), dma((2, SUBS, nz - 1))]


def weight_copies(kv, wq, wk, wv, wo, w_all, wo_v, sem):
    dq = wq.shape[1]
    kvc = pl.ds(pl.multiple_of(kv * HEAD_DIM, HEAD_DIM), HEAD_DIM)
    return [pltpu.make_async_copy(wq, w_all.at[:, pl.ds(0, dq)], sem.at[0]),
            pltpu.make_async_copy(wk.at[:, kvc], w_all.at[:, pl.ds(dq, HEAD_DIM)], sem.at[1]),
            pltpu.make_async_copy(wv.at[:, kvc], w_all.at[:, pl.ds(dq + HEAD_DIM, HEAD_DIM)], sem.at[2]),
            pltpu.make_async_copy(wo, wo_v, sem.at[3])]


def rope(t, cos, sin):
    return t * cos + pltpu.roll(t, HEAD_DIM // 2, 1) * sin


def rope_t(t, cos, sin):
    return t * cos - pltpu.roll(t, HEAD_DIM // 2, 1) * sin


def to_col(row):
    return jnp.broadcast_to(row, (TILE, TILE)).T


def trow(i, n=TILE):
    return pl.ds(pl.multiple_of(i * n, n), n)


def keep_t(kdc, kdr, i, seq):
    key = lax.broadcasted_iota(jnp.int32, (seq, TILE), 0)
    qry = lax.broadcasted_iota(jnp.int32, (seq, TILE), 1) + i * TILE
    return (key <= qry) & (kdc == kdr)


def fwd_kernel(tp, kvr, x_ref, g_ref, pos_ref, frq_ref, dy_ref, wq, wk, wv, wo,
               h_full, dy_full, mix_own, mix_peer, q3_ref, k_ref, v_ref, ot_ref, st_ref, cos_ref, sin_ref, kdc_ref, kdr_ref,
               hown, w_all, wo_v, htile, stage, vt, wsem, hsem, osem, pss, prs, *gsem):
    rg = Ring(tp)
    rows, dm = x_ref.shape
    seq = rows * tp
    nt = seq // TILE
    nh = wq.shape[1] // HEAD_DIM
    half = TILE // 2
    ga = Gather(rg, hown, h_full, rows, *gsem[:5])
    gd = Gather(rg, dy_ref, dy_full, rows, *gsem[5:])
    wcp = weight_copies(rg.me // kvr, wq, wk, wv, wo, w_all, wo_v, wsem)
    for cp in wcp:
        cp.start()
    RB = 16

    @pl.loop(0, rows // RB)
    def _(r):
        xf = x_ref[trow(r, RB), :].astype(F32)
        inv = lax.rsqrt(jnp.mean(xf * xf, axis=-1, keepdims=True) + NORM_EPS)
        hown[trow(r, RB), :] = (xf * inv * g_ref[...]).astype(BF16)

    rg.barrier()
    ga.start_ring(0)
    ga.start_ring(1)
    ga.start_local()
    gd.start_local()
    lane = lax.broadcasted_iota(jnp.int32, (TILE, TILE), 1)
    sgn = jnp.where(lane < HEAD_DIM // 2, -1.0, 1.0).astype(F32)

    kdr_ref[...] = pos_ref[...] - (lax.broadcasted_iota(jnp.int32, pos_ref.shape, 0) * TILE
                                   + lax.broadcasted_iota(jnp.int32, pos_ref.shape, 1)).astype(F32)

    @pl.loop(0, nt)
    def _(i):
        ang = to_col(pos_ref[pl.ds(i, 1), :]) * frq_ref[...]
        cos_ref[trow(i), :] = jnp.cos(ang)
        sin_ref[trow(i), :] = jnp.sin(ang) * sgn
        kdc_ref[trow(i), :] = to_col(kdr_ref[pl.ds(i, 1), :])

    for s in range(ga.steps):
        ga.tick(s)
        if s >= ga.steps - 2:
            gd.start_ring(s - (ga.steps - 2))
    ga.wait_pair()
    for cp in wcp:
        cp.wait()

    def hload(i):
        return pltpu.make_async_copy(h_full.at[trow(i), :], htile.at[i % 2], hsem.at[i % 2])

    hload(0).start()

    @pl.loop(0, nt)
    def _(i):
        hload(i).wait()

        @pl.when(i + 1 < nt)
        def _():
            hload(i + 1).start()
        qkv = dot(htile[i % 2], w_all[...])
        cos, sin = cos_ref[trow(i), :], sin_ref[trow(i), :]
        for h in range(nh + 1):
            t = qkv[:, h * HEAD_DIM:(h + 1) * HEAD_DIM].astype(BF16).astype(F32)
            t = rope(t, cos, sin).astype(BF16)
            if h < nh:
                q3_ref[i, pl.ds(h * TILE, TILE), :] = t
            else:
                k_ref[trow(i), :] = t
        v = qkv[:, (nh + 1) * HEAD_DIM:].astype(BF16)
        v_ref[trow(i), :] = v
        vt[:, trow(i)] = v.astype(F32).T.astype(BF16)

    def outs(i):
        sl = i % 2
        mine = stage.at[sl, trow(rg.k, half), :]
        other = stage.at[sl, trow(1 - rg.k, half), :]
        return (pltpu.make_async_copy(mine, mix_own.at[i], osem.at[sl]),
                remote(other, mix_peer.at[i], pss.at[i], prs.at[i], rg.pt))

    @pl.loop(0, nt)
    def _(i):
        @pl.when(i < gd.steps)
        def _():
            gd.tick(i)

        s = dot(k_ref[...], q3_ref[i], NT) * SCORE_SCALE
        keep = keep_t(kdc_ref[...], kdr_ref[pl.ds(i, 1), :], i, seq)
        pbs = []
        for h in range(nh):
            sh = jnp.where(keep, s[:, h * TILE:(h + 1) * TILE], MASKED)
            m = jnp.max(sh, axis=0, keepdims=True)
            e = jnp.exp(sh - m)
            li = 1.0 / jnp.sum(e, axis=0, keepdims=True)
            st_ref[i, pl.ds(0, 1), pl.ds(h * TILE, TILE)] = m
            st_ref[i, pl.ds(1, 1), pl.ds(h * TILE, TILE)] = li
            pbs.append((e * li).astype(BF16))
        ot = dot(vt[...], jnp.concatenate(pbs, axis=1))
        os = []
        for h in range(nh):
            oh = ot[:, h * TILE:(h + 1) * TILE]
            ot_ref[pl.ds(h * HEAD_DIM, HEAD_DIM), trow(i)] = oh.astype(BF16)
            os.append(oh.T.astype(BF16))
        o = jnp.concatenate(os, axis=1)

        @pl.when(i >= 2)
        def _():
            a, b = outs(i - 2)
            a.wait()
            b.wait_send()
        NC = dm // 4
        for n in range(4):
            stage[i % 2, :, pl.ds(n * NC, NC)] = dot(o, wo_v[:, pl.ds(n * NC, NC)]).astype(BF16)
        a, b = outs(i)
        a.start()
        b.start()

    for i in (nt - 2, nt - 1):
        a, b = outs(i)
        a.wait()
        b.wait_send()
    for i in range(nt):
        outs(i)[1].wait_recv()
    gd.wait_pair()
    ga.drain()
    gd.drain()


def bwd_kernel(tp, kvr, mix_own, mix_peer, x_ref, dy_full, wq, wk, wv, wo, q3_ref, k_ref, v_ref, st_ref, cos_ref, sin_ref, kdc_ref, kdr_ref,
               out_ref, dqkv_ref, dh_own, dh_peer,
               w_all, wo_v, dyt, stage, kt, dk_acc, dv_acc, do3, dqkv_t, wsem, ysem, osem, pss, prs, *rsem):
    rg = Ring(tp)
    rows, dm = x_ref.shape
    seq = rows * tp
    nt = seq // TILE
    np_ = nt // 2
    nh = wq.shape[1] // HEAD_DIM
    dq = wq.shape[1]
    half = TILE // 2

    def final(d, u, val):
        cs = pl.ds(d * sc.W + u * sc.CW, sc.CW)
        out_ref[:, cs] = (x_ref[:, cs].astype(F32) + val).astype(BF16)

    sc = Scatter(rg, mix_own, mix_peer, *rsem, final)
    for cp in sc.loads(0):
        cp.start()
    wcp = weight_copies(rg.me // kvr, wq, wk, wv, wo, w_all, wo_v, wsem)

    def yload(it):
        return pltpu.make_async_copy(dy_full.at[trow(np_ - 1 - it, 2 * TILE), :], dyt.at[it % 2], ysem.at[it % 2])

    yload(0).start()
    for cp in (wcp[3], wcp[0], wcp[1], wcp[2]):
        cp.start()
    rg.barrier()
    for u in range(SUBS):
        sc.tick(0, u)
    kt[...] = k_ref[...].astype(F32).T.astype(BF16)
    dk_acc[...] = jnp.zeros_like(dk_acc)
    dv_acc[...] = jnp.zeros_like(dv_acc)
    for cp in wcp:
        cp.wait()

    def outs(i, sl, j):
        mine = stage.at[sl, pl.ds(pl.multiple_of(j * TILE + rg.k * half, half), half), :]
        other = stage.at[sl, pl.ds(pl.multiple_of(j * TILE + (1 - rg.k) * half, half), half), :]
        return (pltpu.make_async_copy(mine, dh_own.at[i], osem.at[sl, j]),
                remote(other, dh_peer.at[i], pss.at[i], prs.at[i], rg.pt))

    def attn(i, j):
        q3 = q3_ref[i]
        do = do3[j]
        s = dot(k_ref[...], q3, NT) * SCORE_SCALE
        keep = keep_t(kdc_ref[...], kdr_ref[pl.ds(i, 1), :], i, seq)
        dp = dot(v_ref[...], do, NT)
        pbs, dss = [], []
        for h in range(nh):
            hs = slice(h * TILE, (h + 1) * TILE)
            m = st_ref[i, pl.ds(0, 1), pl.ds(h * TILE, TILE)]
            li = st_ref[i, pl.ds(1, 1), pl.ds(h * TILE, TILE)]
            p = jnp.exp(jnp.where(keep, s[:, hs], MASKED) - m) * li
            dph = dp[:, hs].astype(BF16).astype(F32)
            dl = jnp.sum(dph * p, axis=0, keepdims=True)
            dss.append((p * (dph - dl) * SCORE_SCALE).astype(BF16))
            pbs.append(p.astype(BF16))
        pb = jnp.concatenate(pbs, axis=1)
        ds = jnp.concatenate(dss, axis=1)
        dv_acc[...] += dot(pb, do)
        dk_acc[...] += dot(ds, q3)
        dqt = dot(kt[...], ds)
        cos, sin = cos_ref[trow(i), :], sin_ref[trow(i), :]
        jr = pl.ds(j * TILE, TILE)
        for h in range(nh):
            t = dqt[:, h * TILE:(h + 1) * TILE].T.astype(BF16).astype(F32)
            dqkv_t[jr, pl.ds(h * HEAD_DIM, HEAD_DIM)] = rope_t(t, cos, sin).astype(BF16)
        t = dk_acc[trow(i), :].astype(BF16).astype(F32)
        dqkv_t[jr, pl.ds(dq, HEAD_DIM)] = rope_t(t, cos, sin).astype(BF16)
        dqkv_t[jr, pl.ds(dq + HEAD_DIM, HEAD_DIM)] = dv_acc[trow(i), :].astype(BF16)

    @pl.loop(0, np_)
    def _(it):
        ip = np_ - 1 - it
        sl = it % 2
        yload(it).wait()

        @pl.when(it + 1 < np_)
        def _():
            yload(it + 1).start()

        def tick(j, u):
            s = 2 * it + j
            if j == 0:
                @pl.when(s > 0)
                def _():
                    sc.tick(s, u)
            else:
                sc.tick(s, u)

        tick(0, 0)
        do = dot(dyt[sl], wo_v[...], NT).astype(BF16)
        for j in range(2):
            for h in range(nh):
                do3[j, pl.ds(h * TILE, TILE), :] = do[j * TILE:(j + 1) * TILE, h * HEAD_DIM:(h + 1) * HEAD_DIM]
        tick(0, 1)
        attn(2 * ip + 1, 1)
        tick(0, 2)
        attn(2 * ip, 0)
        tick(0, 3)
        dqkv_ref[trow(ip, 2 * TILE), :] = dqkv_t[...]

        @pl.when(it >= 2)
        def _():
            for j in range(2):
                a, b = outs(2 * (ip + 2) + j, sl, j)
                a.wait()
                b.wait_send()
        NC = dm // 4
        for n in range(4):
            ns = pl.ds(n * NC, NC)
            stage[sl, :, ns] = dot(dqkv_t[...], w_all[ns, :], NT).astype(BF16)
            tick(1, n)
        for j in range(2):
            a, b = outs(2 * ip + j, sl, j)
            a.start()
            b.start()

    for it in (np_ - 2, np_ - 1):
        ip = np_ - 1 - it
        for j in range(2):
            a, b = outs(2 * ip + j, it % 2, j)
            a.wait()
            b.wait_send()
    for i in range(nt):
        outs(i, 0, 0)[1].wait_recv()
    sc.drain()


def grad_kernel(tp, dh_own, dh_peer, x_ref, dy_ref, g_ref, h_full, dy_full, dqkv_ref, ot_ref,
                gx_ref, dg_ref, dwq, dwk, dwv, dwo,
                ht, yt, sq, skv, so, peer, dhr, part, slots, tot, hsem, ysem, osem, pss, prs, gss, grs, bss, brs, *rsem):
    rg = Ring(tp)
    rows, dm = x_ref.shape
    nz = rg.nz
    dq = dwq.shape[1]
    CB = dm // nz

    def final(d, u, val):
        dhr[:, pl.ds(d * sc.W + u * sc.CW, sc.CW)] = val.astype(BF16)

    sc = Scatter(rg, dh_own, dh_peer, *rsem, final)
    for cp in sc.loads(0):
        cp.start()

    def col(it):
        return pl.ds(pl.multiple_of(it * CB, CB), CB)

    def hload(it):
        return pltpu.make_async_copy(h_full.at[:, col(it)], ht.at[it % 2], hsem.at[it % 2])

    def yload(it):
        return pltpu.make_async_copy(dy_full.at[:, col(it)], yt.at[it % 2], ysem.at[it % 2])

    hload(0).start()
    yload(0).start()
    rg.barrier_all()

    def to_peer(it):
        return remote(skv.at[it % 2], peer.at[it], pss.at[it], prs.at[it], rg.pt)

    def outs(it):
        sl = it % 2
        return [pltpu.make_async_copy(sq.at[sl], dwq.at[col(it), :], osem.at[sl, 0]),
                pltpu.make_async_copy(so.at[sl], dwo.at[:, col(it)], osem.at[sl, 1])]

    def kv_outs(it):
        return [pltpu.make_async_copy(peer.at[it, :, pl.ds(0, HEAD_DIM)], dwk.at[col(it), :], osem.at[it % 2, 2]),
                pltpu.make_async_copy(peer.at[it, :, pl.ds(HEAD_DIM, HEAD_DIM)], dwv.at[col(it), :], osem.at[it % 2, 3])]

    def pair_sum(it):
        to_peer(it).wait_recv()
        peer[it] = peer[it] + skv[it % 2]
        to_peer(it).wait_send()
        for cp in kv_outs(it):
            cp.start()

    HC = CB // 2

    @pl.loop(0, nz)
    def _(it):
        sl = it % 2
        hload(it).wait()
        yload(it).wait()

        @pl.when(it + 1 < nz)
        def _():
            hload(it + 1).start()
            yload(it + 1).start()

        @pl.when(it >= 2)
        def _():
            for cp in outs(it - 2) + kv_outs(it - 2):
                cp.wait()
        for n in range(2):
            sc.tick(it, 2 * n)
            hs = pl.ds(n * HC, HC)
            dw = dot(ht[sl, :, hs], dqkv_ref[...], TN)
            sq[sl, hs, :] = dw[:, :dq].astype(BF16)
            skv[sl, hs, :] = dw[:, dq:]
            sc.tick(it, 2 * n + 1)
            so[sl, :, hs] = dot(ot_ref[...], yt[sl, :, hs]).astype(BF16)
        to_peer(it).start()
        for cp in outs(it):
            cp.start()

        @pl.when(it >= 1)
        def _():
            pair_sum(it - 1)

    pair_sum(nz - 1)
    RB = 16
    part[...] = jnp.zeros_like(part)

    @pl.loop(0, rows // RB)
    def _(r):
        rr = trow(r, RB)
        xf = x_ref[rr, :].astype(F32)
        inv = lax.rsqrt(jnp.mean(xf * xf, axis=-1, keepdims=True) + NORM_EPS)
        xh = xf * inv
        dh = dhr[rr, :].astype(F32)
        part[...] += jnp.sum(dh * xh, axis=0, keepdims=True)
        a = dh * g_ref[...]
        di = inv * (a - xh * jnp.mean(a * xh, axis=-1, keepdims=True))
        gx_ref[rr, :] = (dy_ref[rr, :].astype(F32) + di).astype(BF16)

    GW = dm // tp

    def gcol(dev):
        return pl.ds(pl.multiple_of(dev * GW, GW), GW)

    def dev(o):
        return lax.rem(rg.me + o, tp)

    def scat(o):
        return remote(part.at[:, gcol(dev(o))], slots.at[o], gss.at[o], grs.at[o], dev(o))

    for o in range(1, tp):
        scat(o).start()
    acc = part[:, gcol(rg.me)]
    for o in range(1, tp):
        scat(o).wait_recv()
        acc = acc + slots[o]
    tot[...] = acc

    def bcast(o):
        return remote(tot, dg_ref.at[:, gcol(rg.me)], bss.at[o], brs.at[o], dev(o))

    def arrive(o):
        src = lax.rem(rg.me + tp - o, tp)
        return remote(tot, dg_ref.at[:, gcol(src)], bss.at[o], brs.at[o], dev(o))

    for o in range(1, tp):
        bcast(o).start()
    dg_ref[:, gcol(rg.me)] = acc
    for o in range(1, tp):
        arrive(o).wait_recv()
    for o in range(1, tp):
        scat(o).wait_send()
        bcast(o).wait_send()
    for it in (nz - 2, nz - 1):
        for cp in outs(it) + kv_outs(it):
            cp.wait()
    sc.drain()


def solution(mesh):
    tp = mesh.shape["tp"]
    nz = tp // 2
    DMA = pltpu.SemaphoreType.DMA

    def device_step(x, dy, pos, gain, wq, wk, wv, wo):
        rows, dm = x.shape
        seq = rows * tp
        nt = seq // TILE
        dq = wq.shape[1]
        nh = dq // HEAD_DIM
        qr = nh * TILE
        wd = dq + 2 * HEAD_DIM
        kvr = tp // (wk.shape[1] // HEAD_DIM)
        expo = jnp.arange(0, HEAD_DIM, 2, dtype=F32) / HEAD_DIM
        frq = jnp.power(ROPE_THETA, -expo)
        frq = jnp.concatenate([frq, frq]).reshape(1, HEAD_DIM)
        g2 = gain.reshape(1, dm)
        posf = pos.astype(F32).reshape(nt, TILE)

        def sds(shape, dt):
            return jax.ShapeDtypeStruct(shape, dt)

        full = sds((seq, dm), BF16)
        blocks = sds((nt, rows, dm), BF16)
        (h_full, dy_full, mix_own, mix_peer, q3, kk, vv, ot, st, cos, sin, kdc, kdr) = pl.pallas_call(
            functools.partial(fwd_kernel, tp, kvr),
            out_shape=[full, full, blocks, blocks, sds((nt, qr, HEAD_DIM), BF16), sds((seq, HEAD_DIM), BF16), sds((seq, HEAD_DIM), BF16),
                       sds((dq, seq), BF16), sds((nt, 2, qr), F32), sds((seq, HEAD_DIM), F32), sds((seq, HEAD_DIM), F32),
                       sds((seq, TILE), F32), sds((nt, TILE), F32)],
            in_specs=[VM, VM, VM, VM, ANY, ANY, ANY, ANY, ANY],
            out_specs=[ANY] * 4 + [VM] * 9,
            scratch_shapes=[pltpu.VMEM((rows, dm), BF16), pltpu.VMEM((dm, wd), BF16), pltpu.VMEM((dq, dm), BF16),
                            pltpu.VMEM((2, TILE, dm), BF16), pltpu.VMEM((2, TILE, dm), BF16), pltpu.VMEM((HEAD_DIM, seq), BF16),
                            DMA((4,)), DMA((2,)), DMA((2,)), DMA((nt,)), DMA((nt,))] + Gather.scratch(tp) + Gather.scratch(tp),
            compiler_params=pltpu.CompilerParams(collective_id=1, has_side_effects=True, vmem_limit_bytes=VMEM_LIMIT),
            name="gather_fwd",
        )(x, g2, posf, frq, dy, wq, wk, wv, wo)

        out, dqkv, dh_own, dh_peer = pl.pallas_call(
            functools.partial(bwd_kernel, tp, kvr),
            out_shape=[sds((rows, dm), BF16), sds((seq, wd), BF16), blocks, blocks],
            in_specs=[ANY, ANY, VM, ANY, ANY, ANY, ANY, ANY] + [VM] * 8,
            out_specs=[VM, VM, ANY, ANY],
            scratch_shapes=[pltpu.VMEM((dm, wd), BF16), pltpu.VMEM((dq, dm), BF16), pltpu.VMEM((2, 2 * TILE, dm), BF16),
                            pltpu.VMEM((2, 2 * TILE, dm), BF16), pltpu.VMEM((HEAD_DIM, seq), BF16), pltpu.VMEM((seq, HEAD_DIM), F32),
                            pltpu.VMEM((seq, HEAD_DIM), F32), pltpu.VMEM((2, qr, HEAD_DIM), BF16), pltpu.VMEM((2 * TILE, wd), BF16),
                            DMA((4,)), DMA((2,)), DMA((2, 2)), DMA((nt,)), DMA((nt,))] + Scatter.scratch(tp, rows, dm),
            compiler_params=pltpu.CompilerParams(collective_id=2, has_side_effects=True, vmem_limit_bytes=VMEM_LIMIT),
            name="scatter_bwd",
        )(mix_own, mix_peer, x, dy_full, wq, wk, wv, wo, q3, kk, vv, st, cos, sin, kdc, kdr)

        CB = dm // nz
        grad_x, d_gain, d_wq, d_wk, d_wv, d_wo = pl.pallas_call(
            functools.partial(grad_kernel, tp),
            out_shape=[sds((rows, dm), BF16), sds((1, dm), F32), sds((dm, dq), BF16), sds((dm, HEAD_DIM), F32), sds((dm, HEAD_DIM), F32),
                       sds((dq, dm), BF16)],
            in_specs=[ANY, ANY, VM, VM, VM, ANY, ANY, VM, VM],
            out_specs=[VM, VM, ANY, ANY, ANY, ANY],
            scratch_shapes=[pltpu.VMEM((2, seq, CB), BF16), pltpu.VMEM((2, seq, CB), BF16), pltpu.VMEM((2, CB, dq), BF16),
                            pltpu.VMEM((2, CB, 2 * HEAD_DIM), F32), pltpu.VMEM((2, dq, CB), BF16), pltpu.VMEM((nz, CB, 2 * HEAD_DIM), F32),
                            pltpu.VMEM((rows, dm), BF16), pltpu.VMEM((1, dm), F32), pltpu.VMEM((tp, 1, dm // tp), F32), pltpu.VMEM((1, dm // tp), F32),
                            DMA((2,)), DMA((2,)), DMA((2, 4)), DMA((nz,)), DMA((nz,)), DMA((tp,)), DMA((tp,)), DMA((tp,)), DMA((tp,))]
            + Scatter.scratch(tp, rows, dm),
            compiler_params=pltpu.CompilerParams(collective_id=3, has_side_effects=True, vmem_limit_bytes=VMEM_LIMIT),
            name="scatter_grads",
        )(dh_own, dh_peer, x, dy, g2, h_full, dy_full, dqkv, ot)
        return out, grad_x, d_wq, d_wk, d_wv, d_wo, d_gain.reshape(dm)

    specs_in = (P(('dp', 'tp'), None), P(('dp', 'tp'), None), P('dp'), P(), P(None, 'tp'), P(), P(), P('tp', None))
    specs_out = (P(('dp', 'tp'), None), P(('dp', 'tp'), None), P('dp', 'tp'), P('dp', 'tp'), P('dp', 'tp'), P(('dp', 'tp'), None), P('dp'))
    return jax.shard_map(device_step, mesh=mesh, in_specs=specs_in, out_specs=specs_out, check_vma=False)
```

```python
import functools
import jax
import jax.numpy as jnp
import numpy as np
from jax import lax
from jax.experimental import pallas as pl
from jax.experimental.pallas import tpu as pltpu
from jax.sharding import PartitionSpec as P

HEAD_DIM = 128
TILE = 128
SUBS = 4
SCORE_SCALE = HEAD_DIM ** -0.5
ROPE_THETA = 1000000.0
NORM_EPS = 1e-05
MASKED = -1e30
MESH = pl.DeviceIdType.MESH
F32 = jnp.float32
BF16 = jnp.bfloat16
ANY = pl.BlockSpec(memory_space=pl.ANY)
VM = pl.BlockSpec(memory_space=pltpu.VMEM)
NT = (((1,), (1,)), ((), ()))
TN = (((0,), (0,)), ((), ()))
VMEM_LIMIT = 63 * 1024 * 1024


def dot(a, b, dims=(((1,), (0,)), ((), ()))):
    return lax.dot_general(a, b, dims, preferred_element_type=F32)


class Ring:
    def __init__(self, tp):
        self.tp = tp
        self.nz = tp // 2
        self.me = lax.axis_index("tp")
        self.c = self.me // 2
        self.k = self.me % 2
        self.up = lax.rem(self.c + 1, self.nz) * 2 + self.k
        self.dn = lax.rem(self.c + self.nz - 1, self.nz) * 2 + self.k
        self.pt = self.c * 2 + 1 - self.k

    def barrier(self):
        bar = pltpu.get_barrier_semaphore()
        for d in (self.up, self.dn, self.pt):
            pl.semaphore_signal(bar, inc=1, device_id={"tp": d}, device_id_type=MESH)
        pl.semaphore_wait(bar, 3)

    def barrier_all(self):
        bar = pltpu.get_barrier_semaphore()
        for o in range(1, self.tp):
            pl.semaphore_signal(bar, inc=1, device_id={"tp": lax.rem(self.me + o, self.tp)}, device_id_type=MESH)
        pl.semaphore_wait(bar, self.tp - 1)

    def chip(self, n):
        return lax.rem(n + 2 * self.nz, self.nz)


def remote(src, dst, ss, rs, dev):
    return pltpu.make_async_remote_copy(src, dst, ss, rs, device_id={"tp": dev}, device_id_type=MESH)


class Gather:
    def __init__(self, rg, src, dst, rows, ss, rs, dss, drs, ls):
        self.rg, self.src, self.dst, self.R = rg, src, dst, rows
        self.ss, self.rs, self.dss, self.drs, self.ls = ss, rs, dss, drs, ls
        self.H = rows // 2
        self.steps = rg.nz - 1

    def rows(self, chip, core, half):
        return pl.ds(pl.multiple_of((self.rg.chip(chip) * 2 + core) * self.R + half * self.H, self.H), self.H)

    def half(self, d, s):
        return s % 2 if d == 0 else 1 - s % 2

    def origin(self, d, s):
        h = (s + 2) // 2
        return self.rg.c - h if d == 0 else self.rg.c + h

    def dev(self, d):
        return self.rg.up if d == 0 else self.rg.dn

    def own(self, d, s):
        h = self.half(d, s)
        return remote(self.src.at[pl.ds(h * self.H, self.H), :], self.dst.at[self.rows(self.rg.c, self.rg.k, h), :],
                      self.ss.at[d, s], self.rs.at[d, s], self.dev(d))

    def recv_rows(self, d, s, core):
        return self.rows(self.origin(d, s), core, self.half(d, s))

    def fwd(self, d, s):
        r = self.recv_rows(d, s - 2, self.rg.k)
        return remote(self.dst.at[r, :], self.dst.at[r, :], self.ss.at[d, s], self.rs.at[d, s], self.dev(d))

    def recv(self, d, s):
        r = self.recv_rows(d, s, self.rg.k)
        return remote(self.dst.at[r, :], self.dst.at[r, :], self.ss.at[d, s], self.rs.at[d, s], self.dev(d))

    def pair(self, i, r):
        return remote(self.dst.at[r, :], self.dst.at[r, :], self.dss.at[i], self.drs.at[i], self.rg.pt)

    def block(self, dev):
        return pl.ds(pl.multiple_of(dev * self.R, self.R), self.R)

    def pair_own(self):
        return remote(self.src, self.dst.at[self.block(self.rg.me), :], self.dss.at[0], self.drs.at[0], self.rg.pt)

    def local(self):
        return pltpu.make_async_copy(self.src, self.dst.at[self.block(self.rg.me), :], self.ls)

    def start_ring(self, s):
        for d in range(2):
            self.own(d, s).start()

    def start_local(self):
        self.local().start()
        self.pair_own().start()

    def tick(self, s, forward=True):
        for d in range(2):
            self.recv(d, s).wait_recv()
            if isinstance(s, int):
                if s + 2 < self.steps:
                    self.fwd(d, s + 2).start()
            else:
                @pl.when(s + 2 < self.steps)
                def _():
                    self.fwd(d, s + 2).start()
            self.pair(1 + 2 * s + d, self.recv_rows(d, s, self.rg.k)).start()

    def wait_pair(self):
        self.local().wait()
        self.pair(0, self.block(self.rg.pt)).wait_recv()
        for s in range(self.steps):
            for d in range(2):
                self.pair(1 + 2 * s + d, self.recv_rows(d, s, 1 - self.rg.k)).wait_recv()

    def drain(self):
        self.pair_own().wait_send()
        for s in range(self.steps):
            for d in range(2):
                self.pair(1 + 2 * s + d, self.recv_rows(d, s, self.rg.k)).wait_send()
                if s < 2:
                    self.own(d, s).wait_send()
                else:
                    self.fwd(d, s).wait_send()

    @staticmethod
    def scratch(tp):
        n = tp // 2 - 1
        dma = pltpu.SemaphoreType.DMA
        return [dma((2, n)), dma((2, n)), dma((1 + 2 * n,)), dma((1 + 2 * n,)), dma]


class Scatter:
    def __init__(self, rg, own, peer, off, pre, psem, buf, ss, rs, final):
        self.rg, self.own, self.peer, self.pre, self.psem = rg, own, peer, pre, psem
        self.buf, self.ss, self.rs, self.final = buf, ss, rs, final
        self.H = own.shape[-1] // 2
        self.W = pre.shape[-1]
        self.off = off
        self.CW = self.W // SUBS

    def blk(self, d, s):
        return self.rg.chip(self.rg.c - 1 - s) if d == 0 else self.rg.chip(self.rg.c + 1 + s)

    def load(self, w, d, s):
        src = (self.own, self.peer)[w].at[self.blk(d, s), :, pl.ds(d * self.H + self.off, self.W)]
        return pltpu.make_async_copy(src, self.pre.at[s % 2, w, d], self.psem.at[s % 2, w, d])

    def start_loads(self, s):
        for w in range(2):
            for d in range(2):
                self.load(w, d, s).start()

    def wait_loads(self, s):
        for w in range(2):
            for d in range(2):
                self.load(w, d, s).wait()

    def send(self, d, u, s):
        return remote(self.buf.at[d, u, s], self.buf.at[d, u, s + 1], self.ss.at[d, u, s], self.rs.at[d, u, s],
                      self.rg.up if d == 0 else self.rg.dn)

    def cols(self, u):
        return pl.ds(u * self.CW if isinstance(u, int) else pl.multiple_of(u * self.CW, self.CW), self.CW)

    def mine(self, d, s, u):
        c = self.cols(u)
        return self.pre[s % 2, 0, d, :, c].astype(F32) + self.pre[s % 2, 1, d, :, c].astype(F32)

    def init(self):
        self.wait_loads(0)
        self.start_loads(1)
        for u in range(SUBS):
            for d in range(2):
                self.buf[d, u, 0] = self.mine(d, 0, u).astype(BF16)
                self.send(d, u, 0).start()

    def tick(self, s, u):
        last = self.rg.nz - 1

        def loads():
            self.wait_loads(s)

            @pl.when(s < last)
            def _():
                self.start_loads(s + 1)

        if isinstance(u, int):
            if u == 0:
                loads()
        else:
            pl.when(u == 0)(loads)
        for d in range(2):
            self.send(d, u, s - 1).wait_recv()

            @pl.when(s < last)
            def _():
                self.buf[d, u, s] = (self.mine(d, s, u) + self.buf[d, u, s].astype(F32)).astype(BF16)
                self.send(d, u, s).start()

            @pl.when(s == last)
            def _():
                self.final(d, u, self.mine(d, s, u) + self.buf[d, u, s].astype(F32))

    def drain(self):
        @pl.loop(0, self.rg.nz - 1)
        def _(s):
            for d in range(2):
                for u in range(SUBS):
                    self.send(d, u, s).wait_send()

    @staticmethod
    def scratch(tp, rows, W):
        nz = tp // 2
        dma = pltpu.SemaphoreType.DMA
        return [pltpu.VMEM((2, 2, 2, rows, W), BF16), dma((2, 2, 2)), pltpu.VMEM((2, SUBS, nz, rows, W // SUBS), BF16),
                dma((2, SUBS, nz - 1)), dma((2, SUBS, nz - 1))]


def weight_copies(kv, wq, wk, wv, wo, w_all, wo_v, sem):
    dq = wq.shape[1]
    kvc = pl.ds(pl.multiple_of(kv * HEAD_DIM, HEAD_DIM), HEAD_DIM)
    return [pltpu.make_async_copy(wq, w_all.at[:, pl.ds(0, dq)], sem.at[0]),
            pltpu.make_async_copy(wk.at[:, kvc], w_all.at[:, pl.ds(dq, HEAD_DIM)], sem.at[1]),
            pltpu.make_async_copy(wv.at[:, kvc], w_all.at[:, pl.ds(dq + HEAD_DIM, HEAD_DIM)], sem.at[2]),
            pltpu.make_async_copy(wo, wo_v, sem.at[3])]


def rope(t, cos, sin):
    return t * cos + pltpu.roll(t, HEAD_DIM // 2, 1) * sin


def rope_t(t, cos, sin):
    return t * cos - pltpu.roll(t, HEAD_DIM // 2, 1) * sin


def to_col(row):
    return jnp.broadcast_to(row, (TILE, TILE)).T


def trow(i, n=TILE):
    return pl.ds(pl.multiple_of(i * n, n), n)


def keep_t(kdc, kdr, i, seq):
    key = lax.broadcasted_iota(jnp.int32, (seq, TILE), 0)
    qry = lax.broadcasted_iota(jnp.int32, (seq, TILE), 1) + i * TILE
    return (key <= qry) & (kdc == kdr)


def first_kernel(tp, kvr, x_ref, g_ref, pos_ref, frq_ref, dy_ref, wq, wk, wv, wo,
                 h_full, dy_full, mix_own, mix_peer, dh_own, dh_peer, ot_ref, dqkv_ref, out_ref,
                 hown, w_all, wo_v, tile, stage, q3_ref, k_ref, v_ref, vt, kt, st_ref, cos_ref, sin_ref, kdc_ref, kdr_ref,
                 dk_acc, dv_acc, do3, dqkv_t, wsem, tsem, msem, mss, mrs, dsem, dss, drs, *sems):
    rg = Ring(tp)
    rows, dm = x_ref.shape
    seq = rows * tp
    nt = seq // TILE
    np_ = nt // 2
    dq = wq.shape[1]
    nh = dq // HEAD_DIM
    half = TILE // 2
    ga = Gather(rg, hown, h_full, rows, *sems[:5])
    gd = Gather(rg, dy_ref, dy_full, rows, *sems[5:10])

    def final(d, u, val):
        xs = pl.ds(pl.multiple_of(d * sc.H + u * sc.CW, sc.CW), sc.CW)
        out_ref[d, :, sc.cols(u)] = (x_ref[:, xs].astype(F32) + val).astype(BF16)

    sc = Scatter(rg, mix_own, mix_peer, 0, *sems[10:], final)
    wcp = weight_copies(rg.me // kvr, wq, wk, wv, wo, w_all, wo_v, wsem)
    for cp in wcp:
        cp.start()
    RB = 16

    @pl.loop(0, rows // RB)
    def _(r):
        xf = x_ref[trow(r, RB), :].astype(F32)
        inv = lax.rsqrt(jnp.mean(xf * xf, axis=-1, keepdims=True) + NORM_EPS)
        hown[trow(r, RB), :] = (xf * inv * g_ref[...]).astype(BF16)

    rg.barrier()
    ga.start_ring(0)
    ga.start_ring(1)
    ga.start_local()
    gd.start_local()
    lane = lax.broadcasted_iota(jnp.int32, (TILE, TILE), 1)
    sgn = jnp.where(lane < HEAD_DIM // 2, -1.0, 1.0).astype(F32)
    kdr_ref[...] = (pos_ref[...] - (lax.broadcasted_iota(jnp.int32, pos_ref.shape, 0) * TILE
                                    + lax.broadcasted_iota(jnp.int32, pos_ref.shape, 1))).astype(F32)

    @pl.loop(0, nt)
    def _(i):
        ang = to_col(pos_ref[pl.ds(i, 1), :].astype(F32)) * frq_ref[...]
        cos_ref[trow(i), :] = jnp.cos(ang)
        sin_ref[trow(i), :] = jnp.sin(ang) * sgn
        kdc_ref[trow(i), :] = to_col(kdr_ref[pl.ds(i, 1), :])

    dk_acc[...] = jnp.zeros_like(dk_acc)
    dv_acc[...] = jnp.zeros_like(dv_acc)
    for s in range(ga.steps):
        ga.tick(s)
        if s >= ga.steps - 2:
            gd.start_ring(s - (ga.steps - 2))
    ga.wait_pair()
    for cp in wcp:
        cp.wait()

    def hload(i):
        return pltpu.make_async_copy(h_full.at[trow(i, 2 * TILE), :], tile.at[i % 2], tsem.at[i % 2])

    hload(0).start()

    @pl.loop(0, np_)
    def _(p):
        hload(p).wait()

        @pl.when(p + 1 < np_)
        def _():
            hload(p + 1).start()

        @pl.when(p == np_ // 2)
        def _():
            gd.tick(0)
        qkv = dot(tile[p % 2], w_all[...])
        for j in range(2):
            i = 2 * p + j
            js = slice(j * TILE, (j + 1) * TILE)
            cos, sin = cos_ref[trow(i), :], sin_ref[trow(i), :]
            for h in range(nh + 1):
                t = qkv[js, h * HEAD_DIM:(h + 1) * HEAD_DIM].astype(BF16).astype(F32)
                t = rope(t, cos, sin)
                if h < nh:
                    q3_ref[i, pl.ds(h * TILE, TILE), :] = t.astype(BF16)
                else:
                    k_ref[trow(i), :] = t.astype(BF16)
                    kt[:, trow(i)] = t.T.astype(BF16)
            v = qkv[js, (nh + 1) * HEAD_DIM:]
            v_ref[trow(i), :] = v.astype(BF16)
            vt[:, trow(i)] = v.T.astype(BF16)

    def half_rows(j, core):
        return pl.ds(pl.multiple_of(j * TILE + core * half, half), half)

    def mix_mine(i):
        return pltpu.make_async_copy(stage.at[i % 2, half_rows(0, rg.k), :], mix_own.at[i], msem.at[i % 2])

    def mix_other(i):
        return remote(stage.at[i % 2, half_rows(0, 1 - rg.k), :], mix_peer.at[i], mss.at[i], mrs.at[i], rg.pt)

    NC = dm // 4

    @pl.loop(0, nt)
    def _(i):
        for n in range(2):
            @pl.when(i == n * np_)
            def _():
                gd.tick(1 + n)

        s = dot(k_ref[...], q3_ref[i], NT) * SCORE_SCALE
        keep = keep_t(kdc_ref[...], kdr_ref[pl.ds(i, 1), :], i, seq)
        pbs = []
        for h in range(nh):
            sh = jnp.where(keep, s[:, h * TILE:(h + 1) * TILE], MASKED)
            m = jnp.max(sh, axis=0, keepdims=True)
            e = jnp.exp(sh - m)
            li = 1.0 / jnp.sum(e, axis=0, keepdims=True)
            st_ref[i, pl.ds(0, 1), pl.ds(h * TILE, TILE)] = m
            st_ref[i, pl.ds(1, 1), pl.ds(h * TILE, TILE)] = li
            pbs.append((e * li).astype(BF16))
        ot = dot(vt[...], jnp.concatenate(pbs, axis=1))
        os = []
        for h in range(nh):
            oh = ot[:, h * TILE:(h + 1) * TILE]
            ot_ref[pl.ds(h * HEAD_DIM, HEAD_DIM), trow(i)] = oh.astype(BF16)
            os.append(oh.T.astype(BF16))
        o = jnp.concatenate(os, axis=1)

        @pl.when(i >= 2)
        def _():
            mix_mine(i - 2).wait()
            mix_other(i - 2).wait_send()
        for n in range(4):
            ns = pl.ds(n * NC, NC)
            stage[i % 2, pl.ds(0, TILE), ns] = dot(o, wo_v[:, ns]).astype(BF16)
        mix_mine(i).start()
        mix_other(i).start()

    for i in (nt - 2, nt - 1):
        mix_mine(i).wait()
        mix_other(i).wait_send()
    for i in range(nt):
        mix_other(i).wait_recv()
    sc.start_loads(0)
    for s in range(3, gd.steps - 2):
        gd.tick(s)
    sc.init()
    for s in range(max(3, gd.steps - 2), gd.steps):
        gd.tick(s)
    gd.wait_pair()

    def yload(it):
        return pltpu.make_async_copy(dy_full.at[trow(np_ - 1 - it, 2 * TILE), :], tile.at[it % 2], tsem.at[it % 2])

    def dh_mine(i, sl, j):
        return pltpu.make_async_copy(stage.at[sl, half_rows(j, rg.k), :], dh_own.at[i], dsem.at[sl, j])

    def dh_other(i, sl, j):
        return remote(stage.at[sl, half_rows(j, 1 - rg.k), :], dh_peer.at[i], dss.at[i], drs.at[i], rg.pt)

    def attn(i, j):
        q3 = q3_ref[i]
        do = do3[j]
        s = dot(k_ref[...], q3, NT) * SCORE_SCALE
        keep = keep_t(kdc_ref[...], kdr_ref[pl.ds(i, 1), :], i, seq)
        dp = dot(v_ref[...], do, NT)
        pbs, dss_ = [], []
        for h in range(nh):
            hs = slice(h * TILE, (h + 1) * TILE)
            m = st_ref[i, pl.ds(0, 1), pl.ds(h * TILE, TILE)]
            li = st_ref[i, pl.ds(1, 1), pl.ds(h * TILE, TILE)]
            p = jnp.exp(jnp.where(keep, s[:, hs], MASKED) - m) * li
            dph = dp[:, hs].astype(BF16).astype(F32)
            dl = jnp.sum(dph * p, axis=0, keepdims=True)
            dss_.append((p * (dph - dl) * SCORE_SCALE).astype(BF16))
            pbs.append(p.astype(BF16))
        pb = jnp.concatenate(pbs, axis=1)
        ds = jnp.concatenate(dss_, axis=1)
        dv_acc[...] += dot(pb, do)
        dk_acc[...] += dot(ds, q3)
        dqt = dot(kt[...], ds)
        cos, sin = cos_ref[trow(i), :], sin_ref[trow(i), :]
        jr = pl.ds(j * TILE, TILE)
        for h in range(nh):
            t = dqt[:, h * TILE:(h + 1) * TILE].T.astype(BF16).astype(F32)
            dqkv_t[jr, pl.ds(h * HEAD_DIM, HEAD_DIM)] = rope_t(t, cos, sin).astype(BF16)
        t = dk_acc[trow(i), :].astype(BF16).astype(F32)
        dqkv_t[jr, pl.ds(dq, HEAD_DIM)] = rope_t(t, cos, sin).astype(BF16)
        dqkv_t[jr, pl.ds(dq + HEAD_DIM, HEAD_DIM)] = dv_acc[trow(i), :].astype(BF16)

    yload(0).start()
    per = -(-SUBS * (rg.nz - 1) // np_)

    @pl.loop(0, np_)
    def _(it):
        ip = np_ - 1 - it
        sl = it % 2
        yload(it).wait()

        @pl.when(it + 1 < np_)
        def _():
            yload(it + 1).start()

        def tick(n):
            at = per * it + n
            sc.tick(1 + at // SUBS, at % SUBS)

        do = dot(tile[sl], wo_v[...], NT).astype(BF16)
        for j in range(2):
            for h in range(nh):
                do3[j, pl.ds(h * TILE, TILE), :] = do[j * TILE:(j + 1) * TILE, h * HEAD_DIM:(h + 1) * HEAD_DIM]
        tick(0)
        attn(2 * ip + 1, 1)
        tick(1)
        attn(2 * ip, 0)
        tick(2)
        dqkv_ref[trow(ip, 2 * TILE), :] = dqkv_t[...]

        @pl.when(it >= 2)
        def _():
            for j in range(2):
                dh_mine(2 * (ip + 2) + j, sl, j).wait()
                dh_other(2 * (ip + 2) + j, sl, j).wait_send()
        for n in range(4):
            ns = pl.ds(n * NC, NC)
            stage[sl, :, ns] = dot(dqkv_t[...], w_all[ns, :], NT).astype(BF16)
            if n == 3:
                for j in range(2):
                    dh_mine(2 * ip + j, sl, j).start()
                    dh_other(2 * ip + j, sl, j).start()
            tick(3 + n)

    for it in (np_ - 2, np_ - 1):
        ip = np_ - 1 - it
        for j in range(2):
            dh_mine(2 * ip + j, it % 2, j).wait()
            dh_other(2 * ip + j, it % 2, j).wait_send()
    for i in range(nt):
        dh_other(i, 0, 0).wait_recv()
    sc.drain()
    ga.drain()
    gd.drain()


def second_kernel(tp, dh_own, dh_peer, mix_own, mix_peer, part1_ref, x_ref, dy_ref, g_ref, h_full, dy_full, dqkv_ref, ot_ref,
                  out_ref, gx_ref, dg_ref, dwq, dwk, dwv, dwo,
                  ht, yt, skv, peer, dhr, part, slots, tot, hsem, ysem, pss, prs, gss, grs, bss, brs, *rsem):
    rg = Ring(tp)
    rows, dm = x_ref.shape
    nz = rg.nz
    dq = dwq.shape[1]
    CB = dm // nz
    LAG = 5
    done = part1_ref.shape[-1]

    def final_a(d, u, val):
        dhr[:, pl.ds(d * sa.H + u * sa.CW, sa.CW)] = val.astype(BF16)

    def final_b(d, u, val):
        cs = pl.ds(d * sb.H + sb.off + u * sb.CW, sb.CW)
        out_ref[:, cs] = (x_ref[:, cs].astype(F32) + val).astype(BF16)

    sa = Scatter(rg, dh_own, dh_peer, 0, *rsem[:5], final_a)
    sb = Scatter(rg, mix_own, mix_peer, done, *rsem[5:], final_b)
    sa.start_loads(0)
    sb.start_loads(0)

    def col(it, n=None):
        return pl.ds(pl.multiple_of(it * CB, CB), CB)

    def hload(it):
        return pltpu.make_async_copy(h_full.at[:, col(it)], ht.at[it % 2], hsem.at[it % 2])

    def yload(it):
        return pltpu.make_async_copy(dy_full.at[:, col(it)], yt.at[it % 2], ysem.at[it % 2])

    hload(0).start()
    yload(0).start()
    rg.barrier_all()
    sa.init()
    for d in range(2):
        out_ref[:, pl.ds(d * sb.H, done)] = part1_ref[d]

    def to_peer(it):
        return remote(skv.at[it % 2], peer.at[it], pss.at[it], prs.at[it], rg.pt)

    def pair_sum(it):
        to_peer(it).wait_recv()
        both = peer[it] + skv[it % 2]
        dwk[col(it), :] = both[:, :HEAD_DIM]
        dwv[col(it), :] = both[:, HEAD_DIM:]
        to_peer(it).wait_send()

    HC = CB // 2

    @pl.loop(0, nz)
    def _(it):
        sl = it % 2
        hload(it).wait()
        yload(it).wait()

        @pl.when(it + 1 < nz)
        def _():
            hload(it + 1).start()
            yload(it + 1).start()

        @pl.when(it == LAG)
        def _():
            sb.init()

        def tick(u):
            @pl.when(it > 0)
            def _():
                sa.tick(it, u)

            @pl.when(it > LAG)
            def _():
                sb.tick(it - LAG, u)

        for n in range(2):
            tick(2 * n)
            hs = pl.ds(n * HC, HC)
            at = pl.ds(pl.multiple_of(it * CB + n * HC, HC), HC)
            dw = dot(ht[sl, :, hs], dqkv_ref[...], TN)
            dwq[at, :] = dw[:, :dq].astype(BF16)
            skv[sl, hs, :] = dw[:, dq:]
            tick(2 * n + 1)
            dwo[:, at] = dot(ot_ref[...], yt[sl, :, hs]).astype(BF16)
        to_peer(it).start()

        @pl.when(it >= 1)
        def _():
            pair_sum(it - 1)

    for u in range(SUBS):
        sb.tick(nz - LAG, u)
    RB = 16
    part[...] = jnp.zeros_like(part)

    @pl.loop(0, rows // RB)
    def _(r):
        rr = trow(r, RB)
        xf = x_ref[rr, :].astype(F32)
        inv = lax.rsqrt(jnp.mean(xf * xf, axis=-1, keepdims=True) + NORM_EPS)
        xh = xf * inv
        dh = dhr[rr, :].astype(F32)
        part[...] += jnp.sum(dh * xh, axis=0, keepdims=True)
        a = dh * g_ref[...]
        di = inv * (a - xh * jnp.mean(a * xh, axis=-1, keepdims=True))
        gx_ref[rr, :] = (dy_ref[rr, :].astype(F32) + di).astype(BF16)

    GW = dm // tp

    def gcol(dev):
        return pl.ds(pl.multiple_of(dev * GW, GW), GW)

    def dev(o):
        return lax.rem(rg.me + o, tp)

    def scat(o):
        return remote(part.at[:, gcol(dev(o))], slots.at[o], gss.at[o], grs.at[o], dev(o))

    for o in range(1, tp):
        scat(o).start()
    pair_sum(nz - 1)
    rest = list(range(nz - LAG + 1, nz))
    for s in rest[:2]:
        for u in range(SUBS):
            sb.tick(s, u)
    acc = part[:, gcol(rg.me)]
    for o in range(1, tp):
        scat(o).wait_recv()
        acc = acc + slots[o]
    tot[...] = acc

    def bcast(o):
        return remote(tot, dg_ref.at[:, gcol(rg.me)], bss.at[o], brs.at[o], dev(o))

    def arrive(o):
        src = lax.rem(rg.me + tp - o, tp)
        return remote(tot, dg_ref.at[:, gcol(src)], bss.at[o], brs.at[o], dev(o))

    for o in range(1, tp):
        bcast(o).start()
    dg_ref[:, gcol(rg.me)] = acc
    for s in rest[2:]:
        for u in range(SUBS):
            sb.tick(s, u)
    for o in range(1, tp):
        arrive(o).wait_recv()
    for o in range(1, tp):
        scat(o).wait_send()
        bcast(o).wait_send()
    sa.drain()
    sb.drain()


def solution(mesh):
    tp = mesh.shape["tp"]
    nz = tp // 2
    DMA = pltpu.SemaphoreType.DMA

    def device_step(x, dy, pos, gain, wq, wk, wv, wo):
        rows, dm = x.shape
        seq = rows * tp
        nt = seq // TILE
        dq = wq.shape[1]
        nh = dq // HEAD_DIM
        qr = nh * TILE
        wd = dq + 2 * HEAD_DIM
        kvr = tp // (wk.shape[1] // HEAD_DIM)
        expo = np.arange(0, HEAD_DIM, 2, dtype=np.float64) / HEAD_DIM
        frq = (ROPE_THETA ** -expo).astype(np.float32)
        frq = jnp.asarray(np.concatenate([frq, frq]).reshape(1, HEAD_DIM))
        g2 = gain.reshape(1, dm)
        pos2 = pos.reshape(nt, TILE)

        def sds(shape, dt):
            return jax.ShapeDtypeStruct(shape, dt)

        V = pltpu.VMEM
        full = sds((seq, dm), BF16)
        blocks = sds((nt, rows, dm), BF16)
        W1 = dm // 3
        W2 = dm // 2 - W1
        h_full, dy_full, mix_own, mix_peer, dh_own, dh_peer, ot, dqkv, part1 = pl.pallas_call(
            functools.partial(first_kernel, tp, kvr),
            out_shape=[full, full, blocks, blocks, blocks, blocks, sds((dq, seq), BF16), sds((seq, wd), BF16), sds((2, rows, W1), BF16)],
            in_specs=[VM, VM, VM, VM, ANY, ANY, ANY, ANY, ANY],
            out_specs=[ANY] * 6 + [VM] * 3,
            scratch_shapes=[V((rows, dm), BF16), V((dm, wd), BF16), V((dq, dm), BF16), V((2, 2 * TILE, dm), BF16), V((2, 2 * TILE, dm), BF16),
                            V((nt, qr, HEAD_DIM), BF16), V((seq, HEAD_DIM), BF16), V((seq, HEAD_DIM), BF16), V((HEAD_DIM, seq), BF16),
                            V((HEAD_DIM, seq), BF16), V((nt, 2, qr), F32), V((seq, HEAD_DIM), F32), V((seq, HEAD_DIM), F32), V((seq, TILE), F32),
                            V((nt, TILE), F32), V((seq, HEAD_DIM), F32), V((seq, HEAD_DIM), F32), V((2, qr, HEAD_DIM), BF16),
                            V((2 * TILE, wd), BF16), DMA((4,)), DMA((2,)), DMA((2,)), DMA((nt,)), DMA((nt,)), DMA((2, 2)), DMA((nt,)), DMA((nt,))]
            + Gather.scratch(tp) + Gather.scratch(tp) + Scatter.scratch(tp, rows, W1),
            compiler_params=pltpu.CompilerParams(collective_id=1, has_side_effects=True, vmem_limit_bytes=VMEM_LIMIT),
            name="gather_attend_scatter",
        )(x, g2, pos2, frq, dy, wq, wk, wv, wo)

        CB = dm // nz
        out, grad_x, d_gain, d_wq, d_wk, d_wv, d_wo = pl.pallas_call(
            functools.partial(second_kernel, tp),
            out_shape=[sds((rows, dm), BF16), sds((rows, dm), BF16), sds((1, dm), F32), V((dm, dq), BF16), V((dm, HEAD_DIM), F32),
                       V((dm, HEAD_DIM), F32), V((dq, dm), BF16)],
            in_specs=[ANY, ANY, ANY, ANY, VM, VM, VM, VM, ANY, ANY, VM, VM],
            out_specs=[VM] * 7,
            scratch_shapes=[V((2, seq, CB), BF16), V((2, seq, CB), BF16), V((2, CB, 2 * HEAD_DIM), F32), V((nz, CB, 2 * HEAD_DIM), F32),
                            V((rows, dm), BF16), V((1, dm), F32), V((tp, 1, dm // tp), F32), V((1, dm // tp), F32),
                            DMA((2,)), DMA((2,)), DMA((nz,)), DMA((nz,)), DMA((tp,)), DMA((tp,)), DMA((tp,)), DMA((tp,))]
            + Scatter.scratch(tp, rows, dm // 2) + Scatter.scratch(tp, rows, W2),
            compiler_params=pltpu.CompilerParams(collective_id=2, has_side_effects=True, vmem_limit_bytes=40 * 1024 * 1024),
            name="scatter_grads",
        )(dh_own, dh_peer, mix_own, mix_peer, part1, x, dy, g2, h_full, dy_full, dqkv, ot)
        return out, grad_x, d_wq, d_wk, d_wv, d_wo, d_gain.reshape(dm)

    specs_in = (P(('dp', 'tp'), None), P(('dp', 'tp'), None), P('dp'), P(), P(None, 'tp'), P(), P(), P('tp', None))
    specs_out = (P(('dp', 'tp'), None), P(('dp', 'tp'), None), P('dp', 'tp'), P('dp', 'tp'), P('dp', 'tp'), P(('dp', 'tp'), None), P('dp'))
    return jax.shard_map(device_step, mesh=mesh, in_specs=specs_in, out_specs=specs_out, check_vma=False)
```

```python
import functools
import jax
import jax.numpy as jnp
import numpy as np
from jax import lax
from jax.experimental import pallas as pl
from jax.experimental.pallas import tpu as pltpu
from jax.sharding import PartitionSpec as P

HEAD_DIM = 128
TILE = 128
SUBS = 4
SCORE_SCALE = HEAD_DIM ** -0.5
ROPE_THETA = 1000000.0
NORM_EPS = 1e-05
MASKED = -1e30
MESH = pl.DeviceIdType.MESH
F32 = jnp.float32
BF16 = jnp.bfloat16
ANY = pl.BlockSpec(memory_space=pl.ANY)
VM = pl.BlockSpec(memory_space=pltpu.VMEM)
NT = (((1,), (1,)), ((), ()))
TN = (((0,), (0,)), ((), ()))
VMEM_LIMIT = 63 * 1024 * 1024


def dot(a, b, dims=(((1,), (0,)), ((), ()))):
    return lax.dot_general(a, b, dims, preferred_element_type=F32)


class Ring:
    def __init__(self, tp):
        self.tp = tp
        self.nz = tp // 2
        self.me = lax.axis_index("tp")
        self.c = self.me // 2
        self.k = self.me % 2
        self.up = lax.rem(self.c + 1, self.nz) * 2 + self.k
        self.dn = lax.rem(self.c + self.nz - 1, self.nz) * 2 + self.k
        self.pt = self.c * 2 + 1 - self.k

    def greet(self, devs):
        bar = pltpu.get_barrier_semaphore()
        for d in devs:
            pl.semaphore_signal(bar, inc=1, device_id={"tp": d}, device_id_type=MESH)

    def greet_near(self):
        self.greet((self.up, self.dn, self.pt))

    def greet_all(self):
        self.greet([lax.rem(self.me + o, self.tp) for o in range(1, self.tp)])

    def met(self, count):
        pl.semaphore_wait(pltpu.get_barrier_semaphore(), count)

    def chip(self, n):
        return lax.rem(n + 2 * self.nz, self.nz)


def remote(src, dst, ss, rs, dev):
    return pltpu.make_async_remote_copy(src, dst, ss, rs, device_id={"tp": dev}, device_id_type=MESH)


class Gather:
    def __init__(self, rg, src, dst, rows, ss, rs, dss, drs, ls):
        self.rg, self.src, self.dst, self.R = rg, src, dst, rows
        self.ss, self.rs, self.dss, self.drs, self.ls = ss, rs, dss, drs, ls
        self.H = rows // 2
        self.steps = rg.nz - 1

    def rows(self, chip, core, half):
        return pl.ds(pl.multiple_of((self.rg.chip(chip) * 2 + core) * self.R + half * self.H, self.H), self.H)

    def half(self, d, s):
        return s % 2 if d == 0 else 1 - s % 2

    def origin(self, d, s):
        h = (s + 2) // 2
        return self.rg.c - h if d == 0 else self.rg.c + h

    def dev(self, d):
        return self.rg.up if d == 0 else self.rg.dn

    def own(self, d, s):
        h = self.half(d, s)
        return remote(self.src.at[pl.ds(h * self.H, self.H), :], self.dst.at[self.rows(self.rg.c, self.rg.k, h), :],
                      self.ss.at[d, s], self.rs.at[d, s], self.dev(d))

    def recv_rows(self, d, s, core):
        return self.rows(self.origin(d, s), core, self.half(d, s))

    def fwd(self, d, s):
        r = self.recv_rows(d, s - 2, self.rg.k)
        return remote(self.dst.at[r, :], self.dst.at[r, :], self.ss.at[d, s], self.rs.at[d, s], self.dev(d))

    def recv(self, d, s):
        r = self.recv_rows(d, s, self.rg.k)
        return remote(self.dst.at[r, :], self.dst.at[r, :], self.ss.at[d, s], self.rs.at[d, s], self.dev(d))

    def pair(self, i, r):
        return remote(self.dst.at[r, :], self.dst.at[r, :], self.dss.at[i], self.drs.at[i], self.rg.pt)

    def block(self, dev):
        return pl.ds(pl.multiple_of(dev * self.R, self.R), self.R)

    def pair_own(self):
        return remote(self.src, self.dst.at[self.block(self.rg.me), :], self.dss.at[0], self.drs.at[0], self.rg.pt)

    def local(self):
        return pltpu.make_async_copy(self.src, self.dst.at[self.block(self.rg.me), :], self.ls)

    def start_ring(self, s):
        for d in range(2):
            self.own(d, s).start()

    def start_local(self):
        self.local().start()
        self.pair_own().start()

    def tick(self, s, forward=True):
        for d in range(2):
            self.recv(d, s).wait_recv()
            if isinstance(s, int):
                if s + 2 < self.steps:
                    self.fwd(d, s + 2).start()
            else:
                @pl.when(s + 2 < self.steps)
                def _():
                    self.fwd(d, s + 2).start()
            self.pair(1 + 2 * s + d, self.recv_rows(d, s, self.rg.k)).start()

    def wait_pair(self):
        self.local().wait()
        self.pair(0, self.block(self.rg.pt)).wait_recv()
        for s in range(self.steps):
            for d in range(2):
                self.pair(1 + 2 * s + d, self.recv_rows(d, s, 1 - self.rg.k)).wait_recv()

    def drain(self):
        self.pair_own().wait_send()
        for s in range(self.steps):
            for d in range(2):
                self.pair(1 + 2 * s + d, self.recv_rows(d, s, self.rg.k)).wait_send()
                if s < 2:
                    self.own(d, s).wait_send()
                else:
                    self.fwd(d, s).wait_send()

    @staticmethod
    def scratch(tp):
        n = tp // 2 - 1
        dma = pltpu.SemaphoreType.DMA
        return [dma((2, n)), dma((2, n)), dma((1 + 2 * n,)), dma((1 + 2 * n,)), dma]


class Scatter:
    def __init__(self, rg, own, peer, off, pre, psem, buf, ss, rs, final):
        self.rg, self.own, self.peer, self.pre, self.psem = rg, own, peer, pre, psem
        self.buf, self.ss, self.rs, self.final = buf, ss, rs, final
        self.H = own.shape[-1] // 2
        self.W = pre.shape[-1]
        self.off = off
        self.CW = self.W // SUBS

    def blk(self, d, s):
        return self.rg.chip(self.rg.c - 1 - s) if d == 0 else self.rg.chip(self.rg.c + 1 + s)

    def load(self, w, d, s):
        src = (self.own, self.peer)[w].at[self.blk(d, s), :, pl.ds(d * self.H + self.off, self.W)]
        return pltpu.make_async_copy(src, self.pre.at[s % 2, w, d], self.psem.at[s % 2, w, d])

    def start_loads(self, s):
        for w in range(2):
            for d in range(2):
                self.load(w, d, s).start()

    def wait_loads(self, s):
        for w in range(2):
            for d in range(2):
                self.load(w, d, s).wait()

    def send(self, d, u, s):
        return remote(self.buf.at[d, u, s], self.buf.at[d, u, s + 1], self.ss.at[d, u, s], self.rs.at[d, u, s],
                      self.rg.up if d == 0 else self.rg.dn)

    def cols(self, u):
        return pl.ds(u * self.CW if isinstance(u, int) else pl.multiple_of(u * self.CW, self.CW), self.CW)

    def mine(self, d, s, u):
        c = self.cols(u)
        return self.pre[s % 2, 0, d, :, c].astype(F32) + self.pre[s % 2, 1, d, :, c].astype(F32)

    def init(self):
        self.wait_loads(0)
        self.start_loads(1)
        for u in range(SUBS):
            for d in range(2):
                self.buf[d, u, 0] = self.mine(d, 0, u).astype(BF16)
                self.send(d, u, 0).start()

    def tick(self, s, u):
        last = self.rg.nz - 1

        def loads():
            self.wait_loads(s)

            @pl.when(s < last)
            def _():
                self.start_loads(s + 1)

        if isinstance(u, int):
            if u == 0:
                loads()
        else:
            pl.when(u == 0)(loads)
        for d in range(2):
            self.send(d, u, s - 1).wait_recv()

            @pl.when(s < last)
            def _():
                self.buf[d, u, s] = (self.mine(d, s, u) + self.buf[d, u, s].astype(F32)).astype(BF16)
                self.send(d, u, s).start()

            @pl.when(s == last)
            def _():
                self.final(d, u, self.mine(d, s, u) + self.buf[d, u, s].astype(F32))

    def drain(self, lo, hi):
        @pl.loop(lo, hi)
        def _(s):
            for d in range(2):
                for u in range(SUBS):
                    self.send(d, u, s).wait_send()

    @staticmethod
    def scratch(tp, rows, W):
        nz = tp // 2
        dma = pltpu.SemaphoreType.DMA
        return [pltpu.VMEM((2, 2, 2, rows, W), BF16), dma((2, 2, 2)), pltpu.VMEM((2, SUBS, nz, rows, W // SUBS), BF16),
                dma((2, SUBS, nz - 1)), dma((2, SUBS, nz - 1))]


def weight_copies(kv, wq, wk, wv, wo, w_all, wo_v, sem):
    dq = wq.shape[1]
    kvc = pl.ds(pl.multiple_of(kv * HEAD_DIM, HEAD_DIM), HEAD_DIM)
    return [pltpu.make_async_copy(wq, w_all.at[:, pl.ds(0, dq)], sem.at[0]),
            pltpu.make_async_copy(wk.at[:, kvc], w_all.at[:, pl.ds(dq, HEAD_DIM)], sem.at[1]),
            pltpu.make_async_copy(wv.at[:, kvc], w_all.at[:, pl.ds(dq + HEAD_DIM, HEAD_DIM)], sem.at[2]),
            pltpu.make_async_copy(wo, wo_v, sem.at[3])]


def rope(t, cos, sin):
    return t * cos + pltpu.roll(t, HEAD_DIM // 2, 1) * sin


def rope_t(t, cos, sin):
    return t * cos - pltpu.roll(t, HEAD_DIM // 2, 1) * sin


def to_col(row):
    return jnp.broadcast_to(row, (TILE, TILE)).T


def trow(i, n=TILE):
    return pl.ds(pl.multiple_of(i * n, n), n)


def keep_t(kdc, kdr, i, seq):
    key = lax.broadcasted_iota(jnp.int32, (seq, TILE), 0)
    qry = lax.broadcasted_iota(jnp.int32, (seq, TILE), 1) + i * TILE
    return (key <= qry) & (kdc == kdr)


def first_kernel(tp, kvr, x_ref, g_ref, pos_ref, frq_ref, dy_ref, wq, wk, wv, wo,
                 h_full, dy_full, mix_own, mix_peer, dh_own, dh_peer, ot_ref, dqkv_ref, out_ref,
                 hown, w_all, wo_v, tile, stage, q3_ref, k_ref, v_ref, vt, kt, st_ref, cos_ref, sin_ref, kdc_ref, kdr_ref,
                 dk_acc, dv_acc, do3, dqkv_t, wsem, tsem, msem, mss, mrs, dsem, dss, drs, *sems):
    rg = Ring(tp)
    rows, dm = x_ref.shape
    seq = rows * tp
    nt = seq // TILE
    np_ = nt // 2
    dq = wq.shape[1]
    nh = dq // HEAD_DIM
    half = TILE // 2
    ga = Gather(rg, hown, h_full, rows, *sems[:5])
    gd = Gather(rg, dy_ref, dy_full, rows, *sems[5:10])

    def final(d, u, val):
        xs = pl.ds(pl.multiple_of(d * sc.H + u * sc.CW, sc.CW), sc.CW)
        out_ref[d, :, sc.cols(u)] = (x_ref[:, xs].astype(F32) + val).astype(BF16)

    sc = Scatter(rg, mix_own, mix_peer, 0, *sems[10:], final)
    rg.greet_near()
    wcp = weight_copies(rg.me // kvr, wq, wk, wv, wo, w_all, wo_v, wsem)
    for cp in wcp:
        cp.start()
    RB = 16

    @pl.loop(0, rows // RB)
    def _(r):
        xf = x_ref[trow(r, RB), :].astype(F32)
        inv = lax.rsqrt(jnp.mean(xf * xf, axis=-1, keepdims=True) + NORM_EPS)
        hown[trow(r, RB), :] = (xf * inv * g_ref[...]).astype(BF16)

    rg.met(3)
    ga.start_ring(0)
    ga.start_ring(1)
    ga.start_local()
    gd.start_local()
    lane = lax.broadcasted_iota(jnp.int32, (TILE, TILE), 1)
    sgn = jnp.where(lane < HEAD_DIM // 2, -1.0, 1.0).astype(F32)
    kdr_ref[...] = (pos_ref[...] - (lax.broadcasted_iota(jnp.int32, pos_ref.shape, 0) * TILE
                                    + lax.broadcasted_iota(jnp.int32, pos_ref.shape, 1))).astype(F32)

    @pl.loop(0, nt)
    def _(i):
        ang = to_col(pos_ref[pl.ds(i, 1), :].astype(F32)) * frq_ref[...]
        cos_ref[trow(i), :] = jnp.cos(ang)
        sin_ref[trow(i), :] = jnp.sin(ang) * sgn
        kdc_ref[trow(i), :] = to_col(kdr_ref[pl.ds(i, 1), :])

    dk_acc[...] = jnp.zeros_like(dk_acc)
    dv_acc[...] = jnp.zeros_like(dv_acc)
    for s in range(ga.steps):
        ga.tick(s)
        if s >= ga.steps - 2:
            gd.start_ring(s - (ga.steps - 2))
    ga.wait_pair()
    for cp in wcp:
        cp.wait()

    def hload(i):
        return pltpu.make_async_copy(h_full.at[trow(i, 2 * TILE), :], tile.at[i % 2], tsem.at[i % 2])

    hload(0).start()

    @pl.loop(0, np_)
    def _(p):
        hload(p).wait()

        @pl.when(p + 1 < np_)
        def _():
            hload(p + 1).start()

        @pl.when(p == np_ // 2)
        def _():
            gd.tick(0)
        qkv = dot(tile[p % 2], w_all[...])
        for j in range(2):
            i = 2 * p + j
            js = slice(j * TILE, (j + 1) * TILE)
            cos, sin = cos_ref[trow(i), :], sin_ref[trow(i), :]
            for h in range(nh + 1):
                t = qkv[js, h * HEAD_DIM:(h + 1) * HEAD_DIM].astype(BF16).astype(F32)
                t = rope(t, cos, sin)
                if h < nh:
                    q3_ref[i, pl.ds(h * TILE, TILE), :] = t.astype(BF16)
                else:
                    k_ref[trow(i), :] = t.astype(BF16)
                    kt[:, trow(i)] = t.T.astype(BF16)
            v = qkv[js, (nh + 1) * HEAD_DIM:]
            v_ref[trow(i), :] = v.astype(BF16)
            vt[:, trow(i)] = v.T.astype(BF16)

    def half_rows(j, core):
        return pl.ds(pl.multiple_of(j * TILE + core * half, half), half)

    def mix_mine(i):
        return pltpu.make_async_copy(stage.at[i % 2, half_rows(0, rg.k), :], mix_own.at[i], msem.at[i % 2])

    def mix_other(i):
        return remote(stage.at[i % 2, half_rows(0, 1 - rg.k), :], mix_peer.at[i], mss.at[i], mrs.at[i], rg.pt)

    NC = dm // 4

    @pl.loop(0, nt)
    def _(i):
        for n in range(2):
            @pl.when(i == n * np_)
            def _():
                gd.tick(1 + n)

        s = dot(k_ref[...], q3_ref[i], NT) * SCORE_SCALE
        keep = keep_t(kdc_ref[...], kdr_ref[pl.ds(i, 1), :], i, seq)
        pbs = []
        for h in range(nh):
            sh = jnp.where(keep, s[:, h * TILE:(h + 1) * TILE], MASKED)
            m = jnp.max(sh, axis=0, keepdims=True)
            e = jnp.exp(sh - m)
            li = 1.0 / jnp.sum(e, axis=0, keepdims=True)
            st_ref[i, pl.ds(0, 1), pl.ds(h * TILE, TILE)] = m
            st_ref[i, pl.ds(1, 1), pl.ds(h * TILE, TILE)] = li
            pbs.append((e * li).astype(BF16))
        ot = dot(vt[...], jnp.concatenate(pbs, axis=1))
        os = []
        for h in range(nh):
            oh = ot[:, h * TILE:(h + 1) * TILE]
            ot_ref[pl.ds(h * HEAD_DIM, HEAD_DIM), trow(i)] = oh.astype(BF16)
            os.append(oh.T.astype(BF16))
        o = jnp.concatenate(os, axis=1)

        @pl.when(i >= 2)
        def _():
            mix_mine(i - 2).wait()
            mix_other(i - 2).wait_send()
        for n in range(4):
            ns = pl.ds(n * NC, NC)
            stage[i % 2, pl.ds(0, TILE), ns] = dot(o, wo_v[:, ns]).astype(BF16)
        mix_mine(i).start()
        mix_other(i).start()

    for i in (nt - 2, nt - 1):
        mix_mine(i).wait()
        mix_other(i).wait_send()
    for i in range(nt):
        mix_other(i).wait_recv()
    sc.start_loads(0)
    for s in range(3, gd.steps - 2):
        gd.tick(s)
    sc.init()
    ga.drain()
    for s in range(max(3, gd.steps - 2), gd.steps):
        gd.tick(s)
    gd.wait_pair()

    def yload(it):
        return pltpu.make_async_copy(dy_full.at[trow(np_ - 1 - it, 2 * TILE), :], tile.at[it % 2], tsem.at[it % 2])

    def dh_mine(i, sl, j, n):
        ns = pl.ds(n * NC, NC)
        return pltpu.make_async_copy(stage.at[sl, half_rows(j, rg.k), ns], dh_own.at[i, :, ns], dsem.at[sl, j, n])

    def dh_other(i, sl, j, n):
        ns = pl.ds(n * NC, NC)
        return remote(stage.at[sl, half_rows(j, 1 - rg.k), ns], dh_peer.at[i, :, ns], dss.at[i, n], drs.at[i, n], rg.pt)

    def attn(i, j):
        q3 = q3_ref[i]
        do = do3[j]
        s = dot(k_ref[...], q3, NT) * SCORE_SCALE
        keep = keep_t(kdc_ref[...], kdr_ref[pl.ds(i, 1), :], i, seq)
        dp = dot(v_ref[...], do, NT)
        pbs, dss_ = [], []
        for h in range(nh):
            hs = slice(h * TILE, (h + 1) * TILE)
            m = st_ref[i, pl.ds(0, 1), pl.ds(h * TILE, TILE)]
            li = st_ref[i, pl.ds(1, 1), pl.ds(h * TILE, TILE)]
            p = jnp.exp(jnp.where(keep, s[:, hs], MASKED) - m) * li
            dph = dp[:, hs].astype(BF16).astype(F32)
            dl = jnp.sum(dph * p, axis=0, keepdims=True)
            dss_.append((p * (dph - dl) * SCORE_SCALE).astype(BF16))
            pbs.append(p.astype(BF16))
        pb = jnp.concatenate(pbs, axis=1)
        ds = jnp.concatenate(dss_, axis=1)
        dv_acc[...] += dot(pb, do)
        dk_acc[...] += dot(ds, q3)
        dqt = dot(kt[...], ds)
        cos, sin = cos_ref[trow(i), :], sin_ref[trow(i), :]
        jr = pl.ds(j * TILE, TILE)
        for h in range(nh):
            t = dqt[:, h * TILE:(h + 1) * TILE].T.astype(BF16).astype(F32)
            dqkv_t[jr, pl.ds(h * HEAD_DIM, HEAD_DIM)] = rope_t(t, cos, sin).astype(BF16)
        t = dk_acc[trow(i), :].astype(BF16).astype(F32)
        dqkv_t[jr, pl.ds(dq, HEAD_DIM)] = rope_t(t, cos, sin).astype(BF16)
        dqkv_t[jr, pl.ds(dq + HEAD_DIM, HEAD_DIM)] = dv_acc[trow(i), :].astype(BF16)

    yload(0).start()
    per = -(-SUBS * (rg.nz - 1) // np_)

    @pl.loop(0, np_)
    def _(it):
        ip = np_ - 1 - it
        sl = it % 2
        yload(it).wait()

        @pl.when(it + 1 < np_)
        def _():
            yload(it + 1).start()

        def tick(n):
            at = per * it + n
            sc.tick(1 + at // SUBS, at % SUBS)

        do = dot(tile[sl], wo_v[...], NT).astype(BF16)
        for j in range(2):
            for h in range(nh):
                do3[j, pl.ds(h * TILE, TILE), :] = do[j * TILE:(j + 1) * TILE, h * HEAD_DIM:(h + 1) * HEAD_DIM]
        tick(0)
        attn(2 * ip + 1, 1)
        tick(1)
        attn(2 * ip, 0)
        tick(2)
        dqkv_ref[trow(ip, 2 * TILE), :] = dqkv_t[...]

        for n in range(4):
            @pl.when(it >= 2)
            def _():
                for j in range(2):
                    dh_mine(2 * (ip + 2) + j, sl, j, n).wait()
                    dh_other(2 * (ip + 2) + j, sl, j, n).wait_send()
            ns = pl.ds(n * NC, NC)
            stage[sl, :, ns] = dot(dqkv_t[...], w_all[ns, :], NT).astype(BF16)
            for j in range(2):
                dh_mine(2 * ip + j, sl, j, n).start()
                dh_other(2 * ip + j, sl, j, n).start()
            tick(3 + n)

    gd.drain()
    sc.drain(0, rg.nz - 1)
    for it in (np_ - 2, np_ - 1):
        ip = np_ - 1 - it
        for j in range(2):
            for n in range(4):
                dh_mine(2 * ip + j, it % 2, j, n).wait()
                dh_other(2 * ip + j, it % 2, j, n).wait_send()

    @pl.loop(0, nt)
    def _(i):
        for n in range(4):
            dh_other(i, 0, 0, n).wait_recv()


def second_kernel(tp, dh_own, dh_peer, mix_own, mix_peer, part1_ref, x_hbm, dy_hbm, g_ref, h_full, dy_full, dqkv_ref, ot_ref,
                  out_ref, gx_ref, dg_ref, dwq, dwk, dwv, dwo,
                  x_ref, dy_ref, xsem, ht, yt, skv, peer, dhr, part, slots, tot, hsem, ysem, pss, prs, gss, grs, bss, brs, *rsem):
    rg = Ring(tp)
    rg.greet_all()
    rows, dm = x_ref.shape
    nz = rg.nz
    dq = dwq.shape[1]
    CB = dm // nz
    LAG = 5
    done = part1_ref.shape[-1]

    def final_a(d, u, val):
        dhr[:, pl.ds(d * sa.H + u * sa.CW, sa.CW)] = val.astype(BF16)

    def final_b(d, u, val):
        cs = pl.ds(d * sb.H + sb.off + u * sb.CW, sb.CW)
        out_ref[:, cs] = (x_ref[:, cs].astype(F32) + val).astype(BF16)

    sa = Scatter(rg, dh_own, dh_peer, 0, *rsem[:5], final_a)
    sb = Scatter(rg, mix_own, mix_peer, done, *rsem[5:], final_b)
    sa.start_loads(0)
    sb.start_loads(0)

    def col(it, n=None):
        return pl.ds(pl.multiple_of(it * CB, CB), CB)

    def hload(it):
        return pltpu.make_async_copy(h_full.at[:, col(it)], ht.at[it % 2], hsem.at[it % 2])

    def yload(it):
        return pltpu.make_async_copy(dy_full.at[:, col(it)], yt.at[it % 2], ysem.at[it % 2])

    hload(0).start()
    yload(0).start()
    xcp = [pltpu.make_async_copy(x_hbm, x_ref, xsem.at[0]), pltpu.make_async_copy(dy_hbm, dy_ref, xsem.at[1])]
    for cp in xcp:
        cp.start()
    rg.met(tp - 1)
    sa.init()
    for cp in xcp:
        cp.wait()
    for d in range(2):
        out_ref[:, pl.ds(d * sb.H, done)] = part1_ref[d]

    def to_peer(it):
        return remote(skv.at[it % 2], peer.at[it], pss.at[it], prs.at[it], rg.pt)

    def pair_sum(it):
        to_peer(it).wait_recv()
        both = peer[it] + skv[it % 2]
        dwk[col(it), :] = both[:, :HEAD_DIM]
        dwv[col(it), :] = both[:, HEAD_DIM:]
        to_peer(it).wait_send()

    HC = CB // 2

    @pl.loop(0, nz)
    def _(it):
        sl = it % 2
        hload(it).wait()
        yload(it).wait()

        @pl.when(it + 1 < nz)
        def _():
            hload(it + 1).start()
            yload(it + 1).start()

        @pl.when(it == LAG)
        def _():
            sb.init()

        def tick(u):
            @pl.when(it > 0)
            def _():
                sa.tick(it, u)

            @pl.when(it > LAG)
            def _():
                sb.tick(it - LAG, u)

        for n in range(2):
            tick(2 * n)
            hs = pl.ds(n * HC, HC)
            at = pl.ds(pl.multiple_of(it * CB + n * HC, HC), HC)
            dw = dot(ht[sl, :, hs], dqkv_ref[...], TN)
            dwq[at, :] = dw[:, :dq].astype(BF16)
            skv[sl, hs, :] = dw[:, dq:]
            tick(2 * n + 1)
            dwo[:, at] = dot(ot_ref[...], yt[sl, :, hs]).astype(BF16)
        to_peer(it).start()

        @pl.when(it >= 1)
        def _():
            pair_sum(it - 1)

    for u in range(SUBS):
        sb.tick(nz - LAG, u)
    RB = 16
    part[...] = jnp.zeros_like(part)

    @pl.loop(0, rows // RB)
    def _(r):
        rr = trow(r, RB)
        xf = x_ref[rr, :].astype(F32)
        inv = lax.rsqrt(jnp.mean(xf * xf, axis=-1, keepdims=True) + NORM_EPS)
        xh = xf * inv
        dh = dhr[rr, :].astype(F32)
        part[...] += jnp.sum(dh * xh, axis=0, keepdims=True)
        a = dh * g_ref[...]
        di = inv * (a - xh * jnp.mean(a * xh, axis=-1, keepdims=True))
        gx_ref[rr, :] = (dy_ref[rr, :].astype(F32) + di).astype(BF16)

    GW = dm // tp

    def gcol(dev):
        return pl.ds(pl.multiple_of(dev * GW, GW), GW)

    def dev(o):
        return lax.rem(rg.me + o, tp)

    def scat(o):
        return remote(part.at[:, gcol(dev(o))], slots.at[o], gss.at[o], grs.at[o], dev(o))

    for o in range(1, tp):
        scat(o).start()
    pair_sum(nz - 1)
    rest = list(range(nz - LAG + 1, nz))
    for s in rest[:2]:
        for u in range(SUBS):
            sb.tick(s, u)
    acc = part[:, gcol(rg.me)]
    for o in range(1, tp):
        scat(o).wait_recv()
        acc = acc + slots[o]
    tot[...] = acc

    def bcast(o):
        return remote(tot, dg_ref.at[:, gcol(rg.me)], bss.at[o], brs.at[o], dev(o))

    def arrive(o):
        src = lax.rem(rg.me + tp - o, tp)
        return remote(tot, dg_ref.at[:, gcol(src)], bss.at[o], brs.at[o], dev(o))

    for o in range(1, tp):
        bcast(o).start()
    dg_ref[:, gcol(rg.me)] = acc
    sa.drain(0, nz - 1)
    sb.drain(0, nz - 3)
    for o in range(1, tp):
        scat(o).wait_send()
    for s in rest[2:]:
        for u in range(SUBS):
            sb.tick(s, u)
    for o in range(1, tp):
        arrive(o).wait_recv()
    for o in range(1, tp):
        bcast(o).wait_send()
    sb.drain(nz - 3, nz - 1)


def write_kernel(n, *refs):
    sem = refs[-1]
    cps = [pltpu.make_async_copy(refs[i], refs[n + i], sem.at[i]) for i in range(n)]
    for cp in cps:
        cp.start()
    for cp in cps:
        cp.wait()


def solution(mesh):
    tp = mesh.shape["tp"]
    nz = tp // 2
    DMA = pltpu.SemaphoreType.DMA

    def device_step(x, dy, pos, gain, wq, wk, wv, wo):
        rows, dm = x.shape
        seq = rows * tp
        nt = seq // TILE
        dq = wq.shape[1]
        nh = dq // HEAD_DIM
        qr = nh * TILE
        wd = dq + 2 * HEAD_DIM
        kvr = tp // (wk.shape[1] // HEAD_DIM)
        expo = np.arange(0, HEAD_DIM, 2, dtype=np.float64) / HEAD_DIM
        frq = (ROPE_THETA ** -expo).astype(np.float32)
        frq = jnp.asarray(np.concatenate([frq, frq]).reshape(1, HEAD_DIM))
        g2 = gain.reshape(1, dm)
        pos2 = pos.reshape(nt, TILE)

        def sds(shape, dt):
            return jax.ShapeDtypeStruct(shape, dt)

        V = pltpu.VMEM
        full = sds((seq, dm), BF16)
        blocks = sds((nt, rows, dm), BF16)
        W1 = dm // 3
        W2 = dm // 2 - W1
        h_full, dy_full, mix_own, mix_peer, dh_own, dh_peer, ot, dqkv, part1 = pl.pallas_call(
            functools.partial(first_kernel, tp, kvr),
            out_shape=[full, full, blocks, blocks, blocks, blocks, V((dq, seq), BF16), V((seq, wd), BF16), V((2, rows, W1), BF16)],
            in_specs=[VM, VM, VM, VM, ANY, ANY, ANY, ANY, ANY],
            out_specs=[ANY] * 6 + [VM] * 3,
            scratch_shapes=[V((rows, dm), BF16), V((dm, wd), BF16), V((dq, dm), BF16), V((2, 2 * TILE, dm), BF16), V((2, 2 * TILE, dm), BF16),
                            V((nt, qr, HEAD_DIM), BF16), V((seq, HEAD_DIM), BF16), V((seq, HEAD_DIM), BF16), V((HEAD_DIM, seq), BF16),
                            V((HEAD_DIM, seq), BF16), V((nt, 2, qr), F32), V((seq, HEAD_DIM), F32), V((seq, HEAD_DIM), F32), V((seq, TILE), F32),
                            V((nt, TILE), F32), V((seq, HEAD_DIM), F32), V((seq, HEAD_DIM), F32), V((2, qr, HEAD_DIM), BF16),
                            V((2 * TILE, wd), BF16), DMA((4,)), DMA((2,)), DMA((2,)), DMA((nt,)), DMA((nt,)), DMA((2, 2, 4)), DMA((nt, 4)), DMA((nt, 4))]
            + Gather.scratch(tp) + Gather.scratch(tp) + Scatter.scratch(tp, rows, W1),
            compiler_params=pltpu.CompilerParams(collective_id=1, has_side_effects=True, vmem_limit_bytes=58 * 1024 * 1024),
            name="gather_attend_scatter",
        )(x, g2, pos2, frq, dy, wq, wk, wv, wo)

        ot, dqkv, part1 = (pltpu.with_memory_space_constraint(a, pltpu.VMEM) for a in (ot, dqkv, part1))
        CB = dm // nz
        res = pl.pallas_call(
            functools.partial(second_kernel, tp),
            out_shape=[V((rows, dm), BF16), V((rows, dm), BF16), V((1, dm), F32), V((dm, dq), BF16), V((dm, HEAD_DIM), F32),
                       V((dm, HEAD_DIM), F32), V((dq, dm), BF16)],
            in_specs=[ANY, ANY, ANY, ANY, VM, ANY, ANY, VM, ANY, ANY, VM, VM],
            out_specs=[VM] * 7,
            scratch_shapes=[V((rows, dm), BF16), V((rows, dm), BF16), DMA((2,)), V((2, seq, CB), BF16), V((2, seq, CB), BF16), V((2, CB, 2 * HEAD_DIM), F32), V((nz, CB, 2 * HEAD_DIM), F32),
                            V((rows, dm), BF16), V((1, dm), F32), V((tp, 1, dm // tp), F32), V((1, dm // tp), F32),
                            DMA((2,)), DMA((2,)), DMA((nz,)), DMA((nz,)), DMA((tp,)), DMA((tp,)), DMA((tp,)), DMA((tp,))]
            + Scatter.scratch(tp, rows, dm // 2) + Scatter.scratch(tp, rows, W2),
            compiler_params=pltpu.CompilerParams(collective_id=2, has_side_effects=True, vmem_limit_bytes=40 * 1024 * 1024),
            name="scatter_grads",
        )(dh_own, dh_peer, mix_own, mix_peer, part1, x, dy, g2, h_full, dy_full, dqkv, ot)
        out, grad_x, d_gain, d_wq, d_wk, d_wv, d_wo = pl.pallas_call(
            functools.partial(write_kernel, len(res)),
            out_shape=[sds(r.shape, r.dtype) for r in res],
            in_specs=[VM] * len(res),
            out_specs=[ANY] * len(res),
            scratch_shapes=[DMA((len(res),))],
            compiler_params=pltpu.CompilerParams(vmem_limit_bytes=1024 * 1024),
            name="write_results",
        )(*res)
        return out, grad_x, d_wq, d_wk, d_wv, d_wo, d_gain.reshape(dm)

    specs_in = (P(('dp', 'tp'), None), P(('dp', 'tp'), None), P('dp'), P(), P(None, 'tp'), P(), P(), P('tp', None))
    specs_out = (P(('dp', 'tp'), None), P(('dp', 'tp'), None), P('dp', 'tp'), P('dp', 'tp'), P('dp', 'tp'), P(('dp', 'tp'), None), P('dp'))
    return jax.shard_map(device_step, mesh=mesh, in_specs=specs_in, out_specs=specs_out, check_vma=False)
```

```python
import functools
import jax
import jax.numpy as jnp
import numpy as np
from jax import lax
from jax.experimental import pallas as pl
from jax.experimental.pallas import tpu as pltpu
from jax.sharding import PartitionSpec as P

HEAD_DIM = 128
TILE = 128
SUBS = 4
SCORE_SCALE = HEAD_DIM ** -0.5
ROPE_THETA = 1000000.0
NORM_EPS = 1e-05
MASKED = -1e30
MESH = pl.DeviceIdType.MESH
F32 = jnp.float32
BF16 = jnp.bfloat16
ANY = pl.BlockSpec(memory_space=pl.ANY)
VM = pl.BlockSpec(memory_space=pltpu.VMEM)
NT = (((1,), (1,)), ((), ()))
TN = (((0,), (0,)), ((), ()))
VMEM_LIMIT = 63 * 1024 * 1024


def dot(a, b, dims=(((1,), (0,)), ((), ()))):
    return lax.dot_general(a, b, dims, preferred_element_type=F32)


class Ring:
    def __init__(self, tp):
        self.tp = tp
        self.nz = tp // 2
        self.me = lax.axis_index("tp")
        self.c = self.me // 2
        self.k = self.me % 2
        self.up = lax.rem(self.c + 1, self.nz) * 2 + self.k
        self.dn = lax.rem(self.c + self.nz - 1, self.nz) * 2 + self.k
        self.pt = self.c * 2 + 1 - self.k

    def greet(self, devs):
        bar = pltpu.get_barrier_semaphore()
        for d in devs:
            pl.semaphore_signal(bar, inc=1, device_id={"tp": d}, device_id_type=MESH)

    def greet_near(self):
        self.greet((self.up, self.dn, self.pt))

    def greet_all(self):
        self.greet([lax.rem(self.me + o, self.tp) for o in range(1, self.tp)])

    def met(self, count):
        pl.semaphore_wait(pltpu.get_barrier_semaphore(), count)

    def chip(self, n):
        return lax.rem(n + 2 * self.nz, self.nz)


def remote(src, dst, ss, rs, dev):
    return pltpu.make_async_remote_copy(src, dst, ss, rs, device_id={"tp": dev}, device_id_type=MESH)


def wait_bytes(ref, sem):
    pltpu.make_async_copy(ref, ref, sem).wait()


class Gather:
    def __init__(self, rg, src, dst, rows, ss, rs, drs, ls):
        self.rg, self.src, self.dst, self.R = rg, src, dst, rows
        self.ss, self.rs, self.drs, self.ls = ss, rs, drs, ls
        self.H = rows // 2
        self.steps = rg.nz - 1

    def rows(self, chip, core, half):
        return pl.ds(pl.multiple_of((self.rg.chip(chip) * 2 + core) * self.R + half * self.H, self.H), self.H)

    def half(self, d, s):
        return s % 2 if d == 0 else 1 - s % 2

    def origin(self, d, s):
        h = (s + 2) // 2
        return self.rg.c - h if d == 0 else self.rg.c + h

    def dev(self, d):
        return self.rg.up if d == 0 else self.rg.dn

    def own(self, d, s):
        h = self.half(d, s)
        return remote(self.src.at[pl.ds(h * self.H, self.H), :], self.dst.at[self.rows(self.rg.c, self.rg.k, h), :],
                      self.ss, self.rs.at[d, s], self.dev(d))

    def recv_rows(self, d, s, core):
        return self.rows(self.origin(d, s), core, self.half(d, s))

    def fwd(self, d, s):
        r = self.recv_rows(d, s - 2, self.rg.k)
        return remote(self.dst.at[r, :], self.dst.at[r, :], self.ss, self.rs.at[d, s], self.dev(d))

    def recv(self, d, s):
        r = self.recv_rows(d, s, self.rg.k)
        return remote(self.dst.at[r, :], self.dst.at[r, :], self.ss, self.rs.at[d, s], self.dev(d))

    def pair(self, d, s):
        r = self.recv_rows(d, s, self.rg.k)
        return remote(self.dst.at[r, :], self.dst.at[r, :], self.ss, self.drs.at[s // 2], self.rg.pt)

    def block(self, dev):
        return pl.ds(pl.multiple_of(dev * self.R, self.R), self.R)

    def pair_own(self):
        return remote(self.src, self.dst.at[self.block(self.rg.me), :], self.ss, self.drs.at[0], self.rg.pt)

    def local(self):
        return pltpu.make_async_copy(self.src, self.dst.at[self.block(self.rg.me), :], self.ls)

    def start_ring(self, s):
        for d in range(2):
            self.own(d, s).start()

    def start_local(self):
        self.local().start()
        self.pair_own().start()

    def tick(self, s):
        for d in range(2):
            self.recv(d, s).wait_recv()
            if s + 2 < self.steps:
                self.fwd(d, s + 2).start()
            self.pair(d, s).start()

    def wait_pair(self, g):
        n = 2 * self.H * min(2, self.steps - 2 * g)
        if g == 0:
            self.local().wait()
            n += self.R
        wait_bytes(self.dst.at[pl.ds(0, n), :], self.drs.at[g])

    def groups(self):
        return (self.steps + 1) // 2

    def drain(self):
        wait_bytes(self.dst.at[pl.ds(0, self.R + 4 * self.H * self.steps), :], self.ss)

    @staticmethod
    def scratch(tp):
        n = tp // 2 - 1
        dma = pltpu.SemaphoreType.DMA
        return [dma, dma((2, n)), dma(((n + 1) // 2,)), dma]


class Scatter:
    def __init__(self, rg, own, peer, off, pre, psem, buf, ss, rs, final):
        self.rg, self.own, self.peer, self.pre, self.psem = rg, own, peer, pre, psem
        self.buf, self.ss, self.rs, self.final = buf, ss, rs, final
        self.H = own.shape[-1] // 2
        self.W = pre.shape[-1]
        self.off = off
        self.CW = self.W // SUBS

    def blk(self, d, s):
        return self.rg.chip(self.rg.c - 1 - s) if d == 0 else self.rg.chip(self.rg.c + 1 + s)

    def load(self, w, d, s):
        src = (self.own, self.peer)[w].at[self.blk(d, s), :, pl.ds(d * self.H + self.off, self.W)]
        return pltpu.make_async_copy(src, self.pre.at[s % 2, w, d], self.psem.at[s % 2, w, d])

    def start_loads(self, s):
        for w in range(2):
            for d in range(2):
                self.load(w, d, s).start()

    def wait_loads(self, s):
        for w in range(2):
            for d in range(2):
                self.load(w, d, s).wait()

    def send(self, d, u, s):
        return remote(self.buf.at[d, u, s], self.buf.at[d, u, s + 1], self.ss, self.rs.at[d, u, s],
                      self.rg.up if d == 0 else self.rg.dn)

    def cols(self, u):
        return pl.ds(u * self.CW if isinstance(u, int) else pl.multiple_of(u * self.CW, self.CW), self.CW)

    def mine(self, d, s, u):
        c = self.cols(u)
        return self.pre[s % 2, 0, d, :, c].astype(F32) + self.pre[s % 2, 1, d, :, c].astype(F32)

    def init(self):
        self.wait_loads(0)
        self.start_loads(1)
        for u in range(SUBS):
            for d in range(2):
                self.buf[d, u, 0] = self.mine(d, 0, u).astype(BF16)
                self.send(d, u, 0).start()

    def tick(self, s, u):
        last = self.rg.nz - 1

        def loads():
            self.wait_loads(s)

            @pl.when(s < last)
            def _():
                self.start_loads(s + 1)

        if isinstance(u, int):
            if u == 0:
                loads()
        else:
            pl.when(u == 0)(loads)
        for d in range(2):
            self.send(d, u, s - 1).wait_recv()

            @pl.when(s < last)
            def _():
                self.buf[d, u, s] = (self.mine(d, s, u) + self.buf[d, u, s].astype(F32)).astype(BF16)
                self.send(d, u, s).start()

            @pl.when(s == last)
            def _():
                self.final(d, u, self.mine(d, s, u) + self.buf[d, u, s].astype(F32))

    def drain(self):
        wait_bytes(self.buf.at[:, :, pl.ds(0, self.rg.nz - 1)], self.ss)

    @staticmethod
    def scratch(tp, rows, W):
        nz = tp // 2
        dma = pltpu.SemaphoreType.DMA
        return [pltpu.VMEM((2, 2, 2, rows, W), BF16), dma((2, 2, 2)), pltpu.VMEM((2, SUBS, nz, rows, W // SUBS), BF16),
                dma, dma((2, SUBS, nz - 1))]


def weight_copies(kv, wq, wk, wv, wo, w_all, wo_v, sem):
    dq = wq.shape[1]
    kvc = pl.ds(pl.multiple_of(kv * HEAD_DIM, HEAD_DIM), HEAD_DIM)
    return [pltpu.make_async_copy(wq, w_all.at[:, pl.ds(0, dq)], sem.at[0]),
            pltpu.make_async_copy(wk.at[:, kvc], w_all.at[:, pl.ds(dq, HEAD_DIM)], sem.at[1]),
            pltpu.make_async_copy(wv.at[:, kvc], w_all.at[:, pl.ds(dq + HEAD_DIM, HEAD_DIM)], sem.at[2]),
            pltpu.make_async_copy(wo, wo_v, sem.at[3])]


def rope(t, cos, sin):
    return t * cos + pltpu.roll(t, HEAD_DIM // 2, 1) * sin


def rope_t(t, cos, sin):
    return t * cos - pltpu.roll(t, HEAD_DIM // 2, 1) * sin


def to_col(row):
    return jnp.broadcast_to(row, (TILE, TILE)).T


def trow(i, n=TILE):
    return pl.ds(pl.multiple_of(i * n, n), n)


def keep_t(kdc, kdr, i, seq):
    key = lax.broadcasted_iota(jnp.int32, (seq, TILE), 0)
    qry = lax.broadcasted_iota(jnp.int32, (seq, TILE), 1) + i * TILE
    return (key <= qry) & (kdc == kdr)


def first_kernel(tp, kvr, x_hbm, g_ref, pos_ref, frq_ref, dy_ref, wq, wk, wv, wo,
                 h_full, dy_full, mix_own, mix_peer, dh_own, dh_peer, ot_ref, dqkv_ref, out_ref,
                 x_ref, hown, w_all, wo_v, tile, stage, q3_ref, k_ref, v_ref, vt, kt, st_ref, cos_ref, sin_ref, kdc_ref, kdr_ref,
                 dk_acc, dv_acc, do3, dqkv_t, xsem, wsem, tsem, ysem, msem, mss, mrs, dsem, dss, drs, *sems):
    rg = Ring(tp)
    rg.greet_near()
    xcp = pltpu.make_async_copy(x_hbm, x_ref, xsem)
    xcp.start()
    rows, dm = x_ref.shape
    seq = rows * tp
    nt = seq // TILE
    np_ = nt // 2
    dq = wq.shape[1]
    nh = dq // HEAD_DIM
    half = TILE // 2
    ga = Gather(rg, hown, h_full, rows, *sems[:4])
    gd = Gather(rg, dy_ref, dy_full, rows, *sems[4:8])

    def final(d, u, val):
        xs = pl.ds(pl.multiple_of(d * sc.H + u * sc.CW, sc.CW), sc.CW)
        out_ref[d, :, sc.cols(u)] = (x_ref[:, xs].astype(F32) + val).astype(BF16)

    sc = Scatter(rg, mix_own, mix_peer, 0, *sems[8:], final)
    wcp = weight_copies(rg.me // kvr, wq, wk, wv, wo, w_all, wo_v, wsem)
    for cp in wcp:
        cp.start()
    RB = 16
    xcp.wait()

    @pl.loop(0, rows // RB)
    def _(r):
        xf = x_ref[trow(r, RB), :].astype(F32)
        inv = lax.rsqrt(jnp.mean(xf * xf, axis=-1, keepdims=True) + NORM_EPS)
        hown[trow(r, RB), :] = (xf * inv * g_ref[...]).astype(BF16)

    rg.met(3)
    ga.start_ring(0)
    ga.start_ring(1)
    ga.start_local()
    gd.start_local()
    lane = lax.broadcasted_iota(jnp.int32, (TILE, TILE), 1)
    sgn = jnp.where(lane < HEAD_DIM // 2, -1.0, 1.0).astype(F32)
    kdr_ref[...] = (pos_ref[...] - (lax.broadcasted_iota(jnp.int32, pos_ref.shape, 0) * TILE
                                    + lax.broadcasted_iota(jnp.int32, pos_ref.shape, 1))).astype(F32)

    @pl.loop(0, nt)
    def _(i):
        ang = to_col(pos_ref[pl.ds(i, 1), :].astype(F32)) * frq_ref[...]
        cos_ref[trow(i), :] = jnp.cos(ang)
        sin_ref[trow(i), :] = jnp.sin(ang) * sgn
        kdc_ref[trow(i), :] = to_col(kdr_ref[pl.ds(i, 1), :])

    dk_acc[...] = jnp.zeros_like(dk_acc)
    dv_acc[...] = jnp.zeros_like(dv_acc)
    for s in range(ga.steps):
        ga.tick(s)
        if s >= ga.steps - 2:
            gd.start_ring(s - (ga.steps - 2))
    for n in range(ga.groups()):
        ga.wait_pair(n)
    for cp in wcp:
        cp.wait()

    def hload(i):
        return pltpu.make_async_copy(h_full.at[trow(i, 2 * TILE), :], tile.at[i % 2], tsem.at[i % 2])

    hload(0).start()

    @pl.loop(0, np_)
    def _(p):
        hload(p).wait()

        @pl.when(p + 1 < np_)
        def _():
            hload(p + 1).start()

        @pl.when(p == np_ // 2)
        def _():
            gd.tick(0)
        qkv = dot(tile[p % 2], w_all[...])
        for j in range(2):
            i = 2 * p + j
            js = slice(j * TILE, (j + 1) * TILE)
            cos, sin = cos_ref[trow(i), :], sin_ref[trow(i), :]
            for h in range(nh + 1):
                t = qkv[js, h * HEAD_DIM:(h + 1) * HEAD_DIM].astype(BF16).astype(F32)
                t = rope(t, cos, sin)
                if h < nh:
                    q3_ref[i, pl.ds(h * TILE, TILE), :] = t.astype(BF16)
                else:
                    k_ref[trow(i), :] = t.astype(BF16)
                    kt[:, trow(i)] = t.T.astype(BF16)
            v = qkv[js, (nh + 1) * HEAD_DIM:]
            v_ref[trow(i), :] = v.astype(BF16)
            vt[:, trow(i)] = v.T.astype(BF16)

    def half_rows(j, core):
        return pl.ds(pl.multiple_of(j * TILE + core * half, half), half)

    def mix_mine(i):
        return pltpu.make_async_copy(stage.at[i % 2, half_rows(0, rg.k), :], mix_own.at[i], msem.at[i % 2])

    def mix_other(i):
        return remote(stage.at[i % 2, half_rows(0, 1 - rg.k), :], mix_peer.at[i], mss.at[i % 2], mrs, rg.pt)

    NC = dm // 4

    @pl.loop(0, nt)
    def _(i):
        for n in range(2):
            @pl.when(i == n * np_)
            def _():
                gd.tick(1 + n)

        s = dot(k_ref[...], q3_ref[i], NT) * SCORE_SCALE
        keep = keep_t(kdc_ref[...], kdr_ref[pl.ds(i, 1), :], i, seq)
        pbs = []
        for h in range(nh):
            sh = jnp.where(keep, s[:, h * TILE:(h + 1) * TILE], MASKED)
            m = jnp.max(sh, axis=0, keepdims=True)
            e = jnp.exp(sh - m)
            li = 1.0 / jnp.sum(e, axis=0, keepdims=True)
            st_ref[i, pl.ds(0, 1), pl.ds(h * TILE, TILE)] = m
            st_ref[i, pl.ds(1, 1), pl.ds(h * TILE, TILE)] = li
            pbs.append((e * li).astype(BF16))
        ot = dot(vt[...], jnp.concatenate(pbs, axis=1))
        os = []
        for h in range(nh):
            oh = ot[:, h * TILE:(h + 1) * TILE]
            ot_ref[pl.ds(h * HEAD_DIM, HEAD_DIM), trow(i)] = oh.astype(BF16)
            os.append(oh.T.astype(BF16))
        o = jnp.concatenate(os, axis=1)

        @pl.when(i >= 2)
        def _():
            mix_mine(i - 2).wait()
            mix_other(i - 2).wait_send()
        for n in range(4):
            ns = pl.ds(n * NC, NC)
            stage[i % 2, pl.ds(0, TILE), ns] = dot(o, wo_v[:, ns]).astype(BF16)
        mix_mine(i).start()
        mix_other(i).start()

    for i in (nt - 2, nt - 1):
        mix_mine(i).wait()
        mix_other(i).wait_send()
    wait_bytes(mix_peer, mrs)
    sc.start_loads(0)

    def yload(chip, sl, j):
        return pltpu.make_async_copy(dy_full.at[trow(rg.chip(chip)), :], tile.at[sl, pl.ds(j * TILE, TILE), :], ysem.at[sl, j])

    def pair_of(g):
        return (rg.c + g + 1, rg.c - g - 1) if g + 1 < np_ else (rg.c + np_, rg.c)

    def start_y(g, js=(0, 1)):
        for j in js:
            yload(pair_of(g)[j], g % 2, j).start()

    def d_o(g):
        for j in range(2):
            yload(pair_of(g)[j], g % 2, j).wait()
        do = dot(tile[g % 2], wo_v[...], NT).astype(BF16)
        for j in range(2):
            t = rg.chip(pair_of(g)[j])
            for h in range(nh):
                do3[t, pl.ds(h * TILE, TILE), :] = do[j * TILE:(j + 1) * TILE, h * HEAD_DIM:(h + 1) * HEAD_DIM]

    gd.tick(3)
    gd.wait_pair(0)
    gd.wait_pair(1)
    start_y(0)
    start_y(1)
    gd.tick(4)
    sc.init()
    ga.drain()
    d_o(0)
    d_o(1)
    start_y(3, (1,))
    gd.tick(5)
    gd.wait_pair(2)
    start_y(2)
    d_o(2)
    gd.tick(6)
    gd.wait_pair(3)
    start_y(3, (0,))
    d_o(3)

    def dh_mine(i, sl, j, n):
        ns = pl.ds(n * NC, NC)
        return pltpu.make_async_copy(stage.at[sl, half_rows(j, rg.k), ns], dh_own.at[i, :, ns], dsem.at[sl, j, n])

    def dh_other(i, sl, j, n):
        ns = pl.ds(n * NC, NC)
        return remote(stage.at[sl, half_rows(j, 1 - rg.k), ns], dh_peer.at[i, :, ns], dss.at[sl, j, n], drs, rg.pt)

    def attn(i, j):
        q3 = q3_ref[i]
        do = do3[i]
        s = dot(k_ref[...], q3, NT) * SCORE_SCALE
        keep = keep_t(kdc_ref[...], kdr_ref[pl.ds(i, 1), :], i, seq)
        dp = dot(v_ref[...], do, NT)
        pbs, dss_ = [], []
        for h in range(nh):
            hs = slice(h * TILE, (h + 1) * TILE)
            m = st_ref[i, pl.ds(0, 1), pl.ds(h * TILE, TILE)]
            li = st_ref[i, pl.ds(1, 1), pl.ds(h * TILE, TILE)]
            p = jnp.exp(jnp.where(keep, s[:, hs], MASKED) - m) * li
            dph = dp[:, hs].astype(BF16).astype(F32)
            dl = jnp.sum(dph * p, axis=0, keepdims=True)
            dss_.append((p * (dph - dl) * SCORE_SCALE).astype(BF16))
            pbs.append(p.astype(BF16))
        pb = jnp.concatenate(pbs, axis=1)
        ds = jnp.concatenate(dss_, axis=1)
        dv_acc[...] += dot(pb, do)
        dk_acc[...] += dot(ds, q3)
        dqt = dot(kt[...], ds)
        cos, sin = cos_ref[trow(i), :], sin_ref[trow(i), :]
        jr = pl.ds(j * TILE, TILE)
        for h in range(nh):
            t = dqt[:, h * TILE:(h + 1) * TILE].T.astype(BF16).astype(F32)
            dqkv_t[jr, pl.ds(h * HEAD_DIM, HEAD_DIM)] = rope_t(t, cos, sin).astype(BF16)
        t = dk_acc[trow(i), :].astype(BF16).astype(F32)
        dqkv_t[jr, pl.ds(dq, HEAD_DIM)] = rope_t(t, cos, sin).astype(BF16)
        dqkv_t[jr, pl.ds(dq + HEAD_DIM, HEAD_DIM)] = dv_acc[trow(i), :].astype(BF16)

    per = -(-SUBS * (rg.nz - 1) // np_)

    @pl.loop(0, np_)
    def _(it):
        ip = np_ - 1 - it
        sl = it % 2

        def tick(n):
            at = per * it + n
            sc.tick(1 + at // SUBS, at % SUBS)

        tick(0)
        attn(2 * ip + 1, 1)
        tick(1)
        attn(2 * ip, 0)
        tick(2)
        dqkv_ref[trow(ip, 2 * TILE), :] = dqkv_t[...]

        for n in range(4):
            @pl.when(it >= 2)
            def _():
                for j in range(2):
                    dh_mine(2 * (ip + 2) + j, sl, j, n).wait()
                    dh_other(2 * (ip + 2) + j, sl, j, n).wait_send()
            ns = pl.ds(n * NC, NC)
            stage[sl, :, ns] = dot(dqkv_t[...], w_all[ns, :], NT).astype(BF16)
            for j in range(2):
                dh_mine(2 * ip + j, sl, j, n).start()
                dh_other(2 * ip + j, sl, j, n).start()
            tick(3 + n)

    gd.drain()
    sc.drain()
    for it in (np_ - 2, np_ - 1):
        ip = np_ - 1 - it
        for j in range(2):
            for n in range(4):
                dh_mine(2 * ip + j, it % 2, j, n).wait()
                dh_other(2 * ip + j, it % 2, j, n).wait_send()

    wait_bytes(dh_peer, drs)


def second_kernel(tp, dh_own, dh_peer, mix_own, mix_peer, part1_ref, x_hbm, dy_hbm, g_ref, h_full, dy_full, dqkv_ref, ot_ref,
                  out_ref, gx_ref, dg_ref, dwq, dwk, dwv, dwo,
                  x_ref, dy_ref, xsem, ht, yt, skv, peer, dhr, part, slots, tot, hsem, ysem, pss, prs, gss, grs, bss, brs, *rsem):
    rg = Ring(tp)
    rg.greet_all()
    rows, dm = x_ref.shape
    nz = rg.nz
    dq = dwq.shape[1]
    CB = dm // nz
    LAG = 4
    done = part1_ref.shape[-1]

    def final_a(d, u, val):
        dhr[:, pl.ds(d * sa.H + u * sa.CW, sa.CW)] = val.astype(BF16)

    def final_b(d, u, val):
        cs = pl.ds(d * sb.H + sb.off + u * sb.CW, sb.CW)
        out_ref[:, cs] = (x_ref[:, cs].astype(F32) + val).astype(BF16)

    sa = Scatter(rg, dh_own, dh_peer, 0, *rsem[:5], final_a)
    sb = Scatter(rg, mix_own, mix_peer, done, *rsem[5:], final_b)
    sa.start_loads(0)
    sb.start_loads(0)

    def col(it, n=None):
        return pl.ds(pl.multiple_of(it * CB, CB), CB)

    def hload(it):
        return pltpu.make_async_copy(h_full.at[:, col(it)], ht.at[it % 2], hsem.at[it % 2])

    def yload(it):
        return pltpu.make_async_copy(dy_full.at[:, col(it)], yt.at[it % 2], ysem.at[it % 2])

    hload(0).start()
    yload(0).start()
    xcp = [pltpu.make_async_copy(x_hbm, x_ref, xsem.at[0]), pltpu.make_async_copy(dy_hbm, dy_ref, xsem.at[1])]
    for cp in xcp:
        cp.start()
    rg.met(tp - 1)
    sa.init()
    for cp in xcp:
        cp.wait()
    for d in range(2):
        out_ref[:, pl.ds(d * sb.H, done)] = part1_ref[d]

    def to_peer(it):
        return remote(skv.at[it % 2], peer.at[it], pss.at[it % 2], prs.at[it], rg.pt)

    def pair_sum(it):
        to_peer(it).wait_recv()
        both = peer[it] + skv[it % 2]
        dwk[col(it), :] = both[:, :HEAD_DIM]
        dwv[col(it), :] = both[:, HEAD_DIM:]
        to_peer(it).wait_send()

    HC = CB // 2

    @pl.loop(0, nz)
    def _(it):
        sl = it % 2
        hload(it).wait()
        yload(it).wait()

        @pl.when(it + 1 < nz)
        def _():
            hload(it + 1).start()
            yload(it + 1).start()

        @pl.when(it == LAG)
        def _():
            sb.init()

        def tick(u):
            @pl.when(it > 0)
            def _():
                sa.tick(it, u)

            @pl.when(it > LAG)
            def _():
                sb.tick(it - LAG, u)

        for n in range(2):
            tick(2 * n)
            hs = pl.ds(n * HC, HC)
            at = pl.ds(pl.multiple_of(it * CB + n * HC, HC), HC)
            dw = dot(ht[sl, :, hs], dqkv_ref[...], TN)
            dwq[at, :] = dw[:, :dq].astype(BF16)
            skv[sl, hs, :] = dw[:, dq:]
            tick(2 * n + 1)
            dwo[:, at] = dot(ot_ref[...], yt[sl, :, hs]).astype(BF16)
        to_peer(it).start()

        @pl.when(it >= 1)
        def _():
            pair_sum(it - 1)

    RB = 16
    part[...] = jnp.zeros_like(part)

    @pl.loop(0, rows // RB)
    def _(r):
        rr = trow(r, RB)
        xf = x_ref[rr, :].astype(F32)
        inv = lax.rsqrt(jnp.mean(xf * xf, axis=-1, keepdims=True) + NORM_EPS)
        xh = xf * inv
        dh = dhr[rr, :].astype(F32)
        part[...] += jnp.sum(dh * xh, axis=0, keepdims=True)
        a = dh * g_ref[...]
        di = inv * (a - xh * jnp.mean(a * xh, axis=-1, keepdims=True))
        gx_ref[rr, :] = (dy_ref[rr, :].astype(F32) + di).astype(BF16)

    GW = dm // tp

    def gcol(dev):
        return pl.ds(pl.multiple_of(dev * GW, GW), GW)

    def dev(o):
        return lax.rem(rg.me + o, tp)

    def scat(o):
        return remote(part.at[:, gcol(dev(o))], slots.at[o], gss, grs, dev(o))

    for o in range(1, tp):
        scat(o).start()
    pair_sum(nz - 1)
    rest = list(range(nz - LAG, nz))
    for s in rest[:2]:
        for u in range(SUBS):
            sb.tick(s, u)
    acc = part[:, gcol(rg.me)]
    wait_bytes(slots.at[pl.ds(1, tp - 1)], grs)
    for o in range(1, tp):
        acc = acc + slots[o]
    tot[...] = acc

    def bcast(o):
        return remote(tot, dg_ref.at[:, gcol(rg.me)], bss, brs, dev(o))

    for o in range(1, tp):
        bcast(o).start()
    dg_ref[:, gcol(rg.me)] = acc
    sa.drain()
    wait_bytes(slots.at[pl.ds(1, tp - 1)], gss)
    for s in rest[2:]:
        for u in range(SUBS):
            sb.tick(s, u)
    wait_bytes(slots.at[pl.ds(1, tp - 1)], brs)
    wait_bytes(slots.at[pl.ds(1, tp - 1)], bss)
    sb.drain()


def write_kernel(n, *refs):
    sem = refs[-1]
    cps = [pltpu.make_async_copy(refs[i], refs[n + i], sem.at[i]) for i in range(n)]
    for cp in cps:
        cp.start()
    for cp in cps:
        cp.wait()


def solution(mesh):
    tp = mesh.shape["tp"]
    nz = tp // 2
    DMA = pltpu.SemaphoreType.DMA

    def device_step(x, dy, pos, gain, wq, wk, wv, wo):
        rows, dm = x.shape
        seq = rows * tp
        nt = seq // TILE
        dq = wq.shape[1]
        nh = dq // HEAD_DIM
        qr = nh * TILE
        wd = dq + 2 * HEAD_DIM
        kvr = tp // (wk.shape[1] // HEAD_DIM)
        expo = np.arange(0, HEAD_DIM, 2, dtype=np.float64) / HEAD_DIM
        frq = (ROPE_THETA ** -expo).astype(np.float32)
        frq = jnp.asarray(np.concatenate([frq, frq]).reshape(1, HEAD_DIM))
        g2 = gain.reshape(1, dm)
        pos2 = pos.reshape(nt, TILE)

        def sds(shape, dt):
            return jax.ShapeDtypeStruct(shape, dt)

        V = pltpu.VMEM
        full = sds((seq, dm), BF16)
        blocks = sds((nt, rows, dm), BF16)
        W1 = dm // 3
        W2 = dm // 2 - W1
        h_full, dy_full, mix_own, mix_peer, dh_own, dh_peer, ot, dqkv, part1 = pl.pallas_call(
            functools.partial(first_kernel, tp, kvr),
            out_shape=[full, full, blocks, blocks, blocks, blocks, V((dq, seq), BF16), V((seq, wd), BF16), V((2, rows, W1), BF16)],
            in_specs=[ANY, VM, VM, VM, ANY, ANY, ANY, ANY, ANY],
            out_specs=[ANY] * 6 + [VM] * 3,
            scratch_shapes=[V((rows, dm), BF16), V((rows, dm), BF16), V((dm, wd), BF16), V((dq, dm), BF16), V((2, 2 * TILE, dm), BF16), V((2, 2 * TILE, dm), BF16),
                            V((nt, qr, HEAD_DIM), BF16), V((seq, HEAD_DIM), BF16), V((seq, HEAD_DIM), BF16), V((HEAD_DIM, seq), BF16),
                            V((HEAD_DIM, seq), BF16), V((nt, 2, qr), F32), V((seq, HEAD_DIM), F32), V((seq, HEAD_DIM), F32), V((seq, TILE), F32),
                            V((nt, TILE), F32), V((seq, HEAD_DIM), F32), V((seq, HEAD_DIM), F32), V((nt, qr, HEAD_DIM), BF16),
                            V((2 * TILE, wd), BF16), DMA, DMA((4,)), DMA((2,)), DMA((2, 2)), DMA((2,)), DMA((2,)), DMA, DMA((2, 2, 4)), DMA((2, 2, 4)), DMA]
            + Gather.scratch(tp) + Gather.scratch(tp) + Scatter.scratch(tp, rows, W1),
            compiler_params=pltpu.CompilerParams(collective_id=1, has_side_effects=True, vmem_limit_bytes=58 * 1024 * 1024),
            name="gather_attend_scatter",
        )(x, g2, pos2, frq, dy, wq, wk, wv, wo)

        ot, dqkv, part1 = (pltpu.with_memory_space_constraint(a, pltpu.VMEM) for a in (ot, dqkv, part1))
        CB = dm // nz
        res = pl.pallas_call(
            functools.partial(second_kernel, tp),
            out_shape=[V((rows, dm), BF16), V((rows, dm), BF16), V((1, dm), F32), V((dm, dq), BF16), V((dm, HEAD_DIM), F32),
                       V((dm, HEAD_DIM), F32), V((dq, dm), BF16)],
            in_specs=[ANY, ANY, ANY, ANY, VM, ANY, ANY, VM, ANY, ANY, VM, VM],
            out_specs=[VM] * 7,
            scratch_shapes=[V((rows, dm), BF16), V((rows, dm), BF16), DMA((2,)), V((2, seq, CB), BF16), V((2, seq, CB), BF16), V((2, CB, 2 * HEAD_DIM), F32), V((nz, CB, 2 * HEAD_DIM), F32),
                            V((rows, dm), BF16), V((1, dm), F32), V((tp, 1, dm // tp), F32), V((1, dm // tp), F32),
                            DMA((2,)), DMA((2,)), DMA((2,)), DMA((nz,)), DMA, DMA, DMA, DMA]
            + Scatter.scratch(tp, rows, dm // 2) + Scatter.scratch(tp, rows, W2),
            compiler_params=pltpu.CompilerParams(collective_id=2, has_side_effects=True, vmem_limit_bytes=40 * 1024 * 1024),
            name="scatter_grads",
        )(dh_own, dh_peer, mix_own, mix_peer, part1, x, dy, g2, h_full, dy_full, dqkv, ot)
        out, grad_x, d_gain, d_wq, d_wk, d_wv, d_wo = pl.pallas_call(
            functools.partial(write_kernel, len(res)),
            out_shape=[sds(r.shape, r.dtype) for r in res],
            in_specs=[VM] * len(res),
            out_specs=[ANY] * len(res),
            scratch_shapes=[DMA((len(res),))],
            compiler_params=pltpu.CompilerParams(vmem_limit_bytes=1024 * 1024),
            name="write_results",
        )(*res)
        return out, grad_x, d_wq, d_wk, d_wv, d_wo, d_gain.reshape(dm)

    specs_in = (P(('dp', 'tp'), None), P(('dp', 'tp'), None), P('dp'), P(), P(None, 'tp'), P(), P(), P('tp', None))
    specs_out = (P(('dp', 'tp'), None), P(('dp', 'tp'), None), P('dp', 'tp'), P('dp', 'tp'), P('dp', 'tp'), P(('dp', 'tp'), None), P('dp'))
    return jax.shard_map(device_step, mesh=mesh, in_specs=specs_in, out_specs=specs_out, check_vma=False)
```

```python
import functools
import jax
import jax.numpy as jnp
import numpy as np
from jax import lax
from jax.experimental import pallas as pl
from jax.experimental.pallas import tpu as pltpu
from jax.sharding import PartitionSpec as P

HEAD_DIM = 128
TILE = 128
SUBS = 4
SCORE_SCALE = HEAD_DIM ** -0.5
ROPE_THETA = 1000000.0
NORM_EPS = 1e-05
MASKED = -1e30
MESH = pl.DeviceIdType.MESH
F32 = jnp.float32
BF16 = jnp.bfloat16
ANY = pl.BlockSpec(memory_space=pl.ANY)
VM = pl.BlockSpec(memory_space=pltpu.VMEM)
NT = (((1,), (1,)), ((), ()))
TN = (((0,), (0,)), ((), ()))
VMEM_LIMIT = 63 * 1024 * 1024


def dot(a, b, dims=(((1,), (0,)), ((), ()))):
    return lax.dot_general(a, b, dims, preferred_element_type=F32)


class Ring:
    def __init__(self, tp):
        self.tp = tp
        self.nz = tp // 2
        self.me = lax.axis_index("tp")
        self.c = self.me // 2
        self.k = self.me % 2
        self.up = lax.rem(self.c + 1, self.nz) * 2 + self.k
        self.dn = lax.rem(self.c + self.nz - 1, self.nz) * 2 + self.k
        self.pt = self.c * 2 + 1 - self.k

    def greet(self, devs):
        bar = pltpu.get_barrier_semaphore()
        for d in devs:
            pl.semaphore_signal(bar, inc=1, device_id={"tp": d}, device_id_type=MESH)

    def greet_near(self):
        self.greet((self.up, self.dn, self.pt))

    def greet_all(self):
        self.greet([lax.rem(self.me + o, self.tp) for o in range(1, self.tp)])

    def met(self, count):
        pl.semaphore_wait(pltpu.get_barrier_semaphore(), count)

    def chip(self, n):
        return lax.rem(n + 2 * self.nz, self.nz)


def remote(src, dst, ss, rs, dev):
    return pltpu.make_async_remote_copy(src, dst, ss, rs, device_id={"tp": dev}, device_id_type=MESH)


def wait_bytes(ref, sem):
    pltpu.make_async_copy(ref, ref, sem).wait()


class Gather:
    def __init__(self, rg, src, dst, rows, ss, rs, drs, ls):
        self.rg, self.src, self.dst, self.R = rg, src, dst, rows
        self.ss, self.rs, self.drs, self.ls = ss, rs, drs, ls
        self.H = rows // 2
        self.steps = rg.nz - 1

    def rows(self, chip, core, half):
        return pl.ds(pl.multiple_of((self.rg.chip(chip) * 2 + core) * self.R + half * self.H, self.H), self.H)

    def half(self, d, s):
        return s % 2 if d == 0 else 1 - s % 2

    def origin(self, d, s):
        h = (s + 2) // 2
        return self.rg.c - h if d == 0 else self.rg.c + h

    def dev(self, d):
        return self.rg.up if d == 0 else self.rg.dn

    def own(self, d, s):
        h = self.half(d, s)
        return remote(self.src.at[pl.ds(h * self.H, self.H), :], self.dst.at[self.rows(self.rg.c, self.rg.k, h), :],
                      self.ss, self.rs.at[d, s], self.dev(d))

    def recv_rows(self, d, s, core):
        return self.rows(self.origin(d, s), core, self.half(d, s))

    def fwd(self, d, s):
        r = self.recv_rows(d, s - 2, self.rg.k)
        return remote(self.dst.at[r, :], self.dst.at[r, :], self.ss, self.rs.at[d, s], self.dev(d))

    def recv(self, d, s):
        r = self.recv_rows(d, s, self.rg.k)
        return remote(self.dst.at[r, :], self.dst.at[r, :], self.ss, self.rs.at[d, s], self.dev(d))

    def pair(self, d, s):
        r = self.recv_rows(d, s, self.rg.k)
        return remote(self.dst.at[r, :], self.dst.at[r, :], self.ss, self.drs.at[s // 2], self.rg.pt)

    def block(self, dev):
        return pl.ds(pl.multiple_of(dev * self.R, self.R), self.R)

    def pair_own(self):
        return remote(self.src, self.dst.at[self.block(self.rg.me), :], self.ss, self.drs.at[0], self.rg.pt)

    def local(self):
        return pltpu.make_async_copy(self.src, self.dst.at[self.block(self.rg.me), :], self.ls)

    def start_ring(self, s):
        for d in range(2):
            self.own(d, s).start()

    def start_local(self):
        self.local().start()
        self.pair_own().start()

    def tick(self, s):
        for d in range(2):
            self.recv(d, s).wait_recv()
            if s + 2 < self.steps:
                self.fwd(d, s + 2).start()
            self.pair(d, s).start()

    def wait_pair(self, g):
        n = 2 * self.H * min(2, self.steps - 2 * g)
        if g == 0:
            self.local().wait()
            n += self.R
        wait_bytes(self.dst.at[pl.ds(0, n), :], self.drs.at[g])

    def groups(self):
        return (self.steps + 1) // 2

    def drain(self):
        wait_bytes(self.dst.at[pl.ds(0, self.R + 4 * self.H * self.steps), :], self.ss)

    @staticmethod
    def scratch(tp):
        n = tp // 2 - 1
        dma = pltpu.SemaphoreType.DMA
        return [dma, dma((2, n)), dma(((n + 1) // 2,)), dma]


class Scatter:
    def __init__(self, rg, own, peer, off, pre, psem, buf, ss, rs, final):
        self.rg, self.own, self.peer, self.pre, self.psem = rg, own, peer, pre, psem
        self.buf, self.ss, self.rs, self.final = buf, ss, rs, final
        self.H = own.shape[-1] // 2
        self.W = pre.shape[-1]
        self.off = off
        self.CW = self.W // SUBS

    def blk(self, d, s):
        return self.rg.chip(self.rg.c - 1 - s) if d == 0 else self.rg.chip(self.rg.c + 1 + s)

    def load(self, w, d, s):
        src = (self.own, self.peer)[w].at[self.blk(d, s), :, pl.ds(d * self.H + self.off, self.W)]
        return pltpu.make_async_copy(src, self.pre.at[s % 2, w, d], self.psem.at[s % 2, w, d])

    def start_loads(self, s):
        for w in range(2):
            for d in range(2):
                self.load(w, d, s).start()

    def wait_loads(self, s):
        for w in range(2):
            for d in range(2):
                self.load(w, d, s).wait()

    def send(self, d, u, s):
        return remote(self.buf.at[d, u, s], self.buf.at[d, u, s + 1], self.ss, self.rs.at[d, u, s],
                      self.rg.up if d == 0 else self.rg.dn)

    def cols(self, u):
        return pl.ds(u * self.CW if isinstance(u, int) else pl.multiple_of(u * self.CW, self.CW), self.CW)

    def mine(self, d, s, u):
        c = self.cols(u)
        return self.pre[s % 2, 0, d, :, c].astype(F32) + self.pre[s % 2, 1, d, :, c].astype(F32)

    def init(self):
        self.wait_loads(0)
        self.start_loads(1)
        for u in range(SUBS):
            for d in range(2):
                self.buf[d, u, 0] = self.mine(d, 0, u).astype(BF16)
                self.send(d, u, 0).start()

    def tick(self, s, u):
        last = self.rg.nz - 1

        def loads():
            self.wait_loads(s)

            @pl.when(s < last)
            def _():
                self.start_loads(s + 1)

        if isinstance(u, int):
            if u == 0:
                loads()
        else:
            pl.when(u == 0)(loads)
        for d in range(2):
            self.send(d, u, s - 1).wait_recv()

            @pl.when(s < last)
            def _():
                self.buf[d, u, s] = (self.mine(d, s, u) + self.buf[d, u, s].astype(F32)).astype(BF16)
                self.send(d, u, s).start()

            @pl.when(s == last)
            def _():
                self.final(d, u, self.mine(d, s, u) + self.buf[d, u, s].astype(F32))

    def drain(self):
        wait_bytes(self.buf.at[:, :, pl.ds(0, self.rg.nz - 1)], self.ss)

    @staticmethod
    def scratch(tp, rows, W):
        nz = tp // 2
        dma = pltpu.SemaphoreType.DMA
        return [pltpu.VMEM((2, 2, 2, rows, W), BF16), dma((2, 2, 2)), pltpu.VMEM((2, SUBS, nz, rows, W // SUBS), BF16),
                dma, dma((2, SUBS, nz - 1))]


def weight_copies(kv, wq, wk, wv, wo, w_all, wo_v, sem):
    dq = wq.shape[1]
    kvc = pl.ds(pl.multiple_of(kv * HEAD_DIM, HEAD_DIM), HEAD_DIM)
    return [pltpu.make_async_copy(wq, w_all.at[:, pl.ds(0, dq)], sem.at[0]),
            pltpu.make_async_copy(wk.at[:, kvc], w_all.at[:, pl.ds(dq, HEAD_DIM)], sem.at[1]),
            pltpu.make_async_copy(wv.at[:, kvc], w_all.at[:, pl.ds(dq + HEAD_DIM, HEAD_DIM)], sem.at[2]),
            pltpu.make_async_copy(wo, wo_v, sem.at[3])]


def rope(t, cos, sin):
    return t * cos + pltpu.roll(t, HEAD_DIM // 2, 1) * sin


def rope_t(t, cos, sin):
    return t * cos - pltpu.roll(t, HEAD_DIM // 2, 1) * sin


def to_col(row):
    return jnp.broadcast_to(row, (TILE, TILE)).T


def trow(i, n=TILE):
    return pl.ds(pl.multiple_of(i * n, n), n)


def keep_t(kdc, kdr, i, seq):
    key = lax.broadcasted_iota(jnp.int32, (seq, TILE), 0)
    qry = lax.broadcasted_iota(jnp.int32, (seq, TILE), 1) + i * TILE
    return (key <= qry) & (kdc == kdr)


def first_kernel(tp, kvr, x_hbm, g_ref, pos_ref, frq_ref, dy_ref, wq, wk, wv, wo,
                 h_full, dy_full, mix_own, mix_peer, dh_own, dh_peer, ot_ref, dqkv_ref, out_ref,
                 x_ref, hown, w_all, wo_v, tile, stage, q3_ref, k_ref, v_ref, vt, kt, st_ref, cos_ref, sin_ref, kdc_ref, kdr_ref,
                 dk_acc, dv_acc, do3, dqkv_t, xsem, wsem, tsem, ysem, msem, mss, mrs, dsem, dss, drs, *sems):
    rg = Ring(tp)
    rg.greet_near()
    xcp = pltpu.make_async_copy(x_hbm, x_ref, xsem)
    xcp.start()
    rows, dm = x_ref.shape
    seq = rows * tp
    nt = seq // TILE
    np_ = nt // 2
    dq = wq.shape[1]
    nh = dq // HEAD_DIM
    half = TILE // 2
    ga = Gather(rg, hown, h_full, rows, *sems[:4])
    gd = Gather(rg, dy_ref, dy_full, rows, *sems[4:8])

    def final(d, u, val):
        xs = pl.ds(pl.multiple_of(d * sc.H + u * sc.CW, sc.CW), sc.CW)
        out_ref[d, :, sc.cols(u)] = (x_ref[:, xs].astype(F32) + val).astype(BF16)

    sc = Scatter(rg, mix_own, mix_peer, 0, *sems[8:], final)
    wcp = weight_copies(rg.me // kvr, wq, wk, wv, wo, w_all, wo_v, wsem)
    RB = 16
    xcp.wait()

    @pl.loop(0, rows // RB)
    def _(r):
        xf = x_ref[trow(r, RB), :].astype(F32)
        inv = lax.rsqrt(jnp.mean(xf * xf, axis=-1, keepdims=True) + NORM_EPS)
        hown[trow(r, RB), :] = (xf * inv * g_ref[...]).astype(BF16)

    rg.met(3)
    ga.start_ring(0)
    ga.start_ring(1)
    ga.start_local()
    gd.start_local()
    for cp in wcp:
        cp.start()
    lane = lax.broadcasted_iota(jnp.int32, (TILE, TILE), 1)
    sgn = jnp.where(lane < HEAD_DIM // 2, -1.0, 1.0).astype(F32)
    kdr_ref[...] = (pos_ref[...] - (lax.broadcasted_iota(jnp.int32, pos_ref.shape, 0) * TILE
                                    + lax.broadcasted_iota(jnp.int32, pos_ref.shape, 1))).astype(F32)

    @pl.loop(0, nt)
    def _(i):
        ang = to_col(pos_ref[pl.ds(i, 1), :].astype(F32)) * frq_ref[...]
        cos_ref[trow(i), :] = jnp.cos(ang)
        sin_ref[trow(i), :] = jnp.sin(ang) * sgn
        kdc_ref[trow(i), :] = to_col(kdr_ref[pl.ds(i, 1), :])

    dk_acc[...] = jnp.zeros_like(dk_acc)
    dv_acc[...] = jnp.zeros_like(dv_acc)
    for s in range(ga.steps):
        ga.tick(s)
        if s >= ga.steps - 2:
            gd.start_ring(s - (ga.steps - 2))
    for n in range(ga.groups()):
        ga.wait_pair(n)
    for cp in wcp:
        cp.wait()

    def hload(i):
        return pltpu.make_async_copy(h_full.at[trow(i, 2 * TILE), :], tile.at[i % 2], tsem.at[i % 2])

    hload(0).start()

    @pl.loop(0, np_)
    def _(p):
        hload(p).wait()

        @pl.when(p + 1 < np_)
        def _():
            hload(p + 1).start()

        @pl.when(p == np_ // 2)
        def _():
            gd.tick(0)
        qkv = dot(tile[p % 2], w_all[...])
        for j in range(2):
            i = 2 * p + j
            js = slice(j * TILE, (j + 1) * TILE)
            cos, sin = cos_ref[trow(i), :], sin_ref[trow(i), :]
            for h in range(nh + 1):
                t = qkv[js, h * HEAD_DIM:(h + 1) * HEAD_DIM].astype(BF16).astype(F32)
                t = rope(t, cos, sin)
                if h < nh:
                    q3_ref[i, pl.ds(h * TILE, TILE), :] = t.astype(BF16)
                else:
                    k_ref[trow(i), :] = t.astype(BF16)
                    kt[:, trow(i)] = t.T.astype(BF16)
            v = qkv[js, (nh + 1) * HEAD_DIM:]
            v_ref[trow(i), :] = v.astype(BF16)
            vt[:, trow(i)] = v.T.astype(BF16)

    def half_rows(j, core):
        return pl.ds(pl.multiple_of(j * TILE + core * half, half), half)

    def mix_mine(i):
        return pltpu.make_async_copy(stage.at[i % 2, half_rows(0, rg.k), :], mix_own.at[i], msem.at[i % 2])

    def mix_other(i):
        return remote(stage.at[i % 2, half_rows(0, 1 - rg.k), :], mix_peer.at[i], mss.at[i % 2], mrs, rg.pt)

    NC = dm // 4

    @pl.loop(0, nt)
    def _(i):
        for n in range(2):
            @pl.when(i == n * np_)
            def _():
                gd.tick(1 + n)

        s = dot(k_ref[...], q3_ref[i], NT) * SCORE_SCALE
        keep = keep_t(kdc_ref[...], kdr_ref[pl.ds(i, 1), :], i, seq)
        pbs = []
        for h in range(nh):
            sh = jnp.where(keep, s[:, h * TILE:(h + 1) * TILE], MASKED)
            m = jnp.max(sh, axis=0, keepdims=True)
            e = jnp.exp(sh - m)
            li = 1.0 / jnp.sum(e, axis=0, keepdims=True)
            st_ref[i, pl.ds(0, 1), pl.ds(h * TILE, TILE)] = m
            st_ref[i, pl.ds(1, 1), pl.ds(h * TILE, TILE)] = li
            pbs.append((e * li).astype(BF16))
        ot = dot(vt[...], jnp.concatenate(pbs, axis=1))
        os = []
        for h in range(nh):
            oh = ot[:, h * TILE:(h + 1) * TILE]
            ot_ref[pl.ds(h * HEAD_DIM, HEAD_DIM), trow(i)] = oh.astype(BF16)
            os.append(oh.T.astype(BF16))
        o = jnp.concatenate(os, axis=1)

        @pl.when(i >= 2)
        def _():
            mix_mine(i - 2).wait()
            mix_other(i - 2).wait_send()
        for n in range(4):
            ns = pl.ds(n * NC, NC)
            stage[i % 2, pl.ds(0, TILE), ns] = dot(o, wo_v[:, ns]).astype(BF16)
        mix_mine(i).start()
        mix_other(i).start()

    for i in (nt - 2, nt - 1):
        mix_mine(i).wait()
        mix_other(i).wait_send()
    wait_bytes(mix_peer, mrs)
    sc.start_loads(0)

    def yload(chip, sl, j):
        return pltpu.make_async_copy(dy_full.at[trow(rg.chip(chip)), :], tile.at[sl, pl.ds(j * TILE, TILE), :], ysem.at[sl, j])

    def pair_of(g):
        return (rg.c + g + 1, rg.c - g - 1) if g + 1 < np_ else (rg.c + np_, rg.c)

    def start_y(g, js=(0, 1)):
        for j in js:
            yload(pair_of(g)[j], g % 2, j).start()

    def d_o(g, meanwhile=None):
        if meanwhile is not None:
            meanwhile()
        for j in range(2):
            yload(pair_of(g)[j], g % 2, j).wait()
        do = dot(tile[g % 2], wo_v[...], NT).astype(BF16)
        for j in range(2):
            t = rg.chip(pair_of(g)[j])
            for h in range(nh):
                do3[t, pl.ds(h * TILE, TILE), :] = do[j * TILE:(j + 1) * TILE, h * HEAD_DIM:(h + 1) * HEAD_DIM]

    gd.tick(3)
    gd.wait_pair(0)
    gd.wait_pair(1)
    start_y(0)
    start_y(1)
    gd.tick(4)
    sc.init()
    ga.drain()
    d_o(0)
    d_o(1)
    start_y(3, (1,))
    gd.tick(5)
    gd.wait_pair(2)
    start_y(2)
    d_o(2)
    gd.tick(6)
    gd.wait_pair(3)
    start_y(3, (0,))
    d_o(3, lambda: sc.tick(jnp.int32(1), 0))

    def dh_mine(i, sl, j, n):
        ns = pl.ds(n * NC, NC)
        return pltpu.make_async_copy(stage.at[sl, half_rows(j, rg.k), ns], dh_own.at[i, :, ns], dsem.at[sl, j, n])

    def dh_other(i, sl, j, n):
        ns = pl.ds(n * NC, NC)
        return remote(stage.at[sl, half_rows(j, 1 - rg.k), ns], dh_peer.at[i, :, ns], dss.at[sl, j, n], drs, rg.pt)

    def attn(i, j):
        q3 = q3_ref[i]
        do = do3[i]
        s = dot(k_ref[...], q3, NT) * SCORE_SCALE
        keep = keep_t(kdc_ref[...], kdr_ref[pl.ds(i, 1), :], i, seq)
        dp = dot(v_ref[...], do, NT)
        pbs, dss_ = [], []
        for h in range(nh):
            hs = slice(h * TILE, (h + 1) * TILE)
            m = st_ref[i, pl.ds(0, 1), pl.ds(h * TILE, TILE)]
            li = st_ref[i, pl.ds(1, 1), pl.ds(h * TILE, TILE)]
            p = jnp.exp(jnp.where(keep, s[:, hs], MASKED) - m) * li
            dph = dp[:, hs].astype(BF16).astype(F32)
            dl = jnp.sum(dph * p, axis=0, keepdims=True)
            dss_.append((p * (dph - dl) * SCORE_SCALE).astype(BF16))
            pbs.append(p.astype(BF16))
        pb = jnp.concatenate(pbs, axis=1)
        ds = jnp.concatenate(dss_, axis=1)
        dv_acc[...] += dot(pb, do)
        dk_acc[...] += dot(ds, q3)
        dqt = dot(kt[...], ds)
        cos, sin = cos_ref[trow(i), :], sin_ref[trow(i), :]
        jr = pl.ds(j * TILE, TILE)
        for h in range(nh):
            t = dqt[:, h * TILE:(h + 1) * TILE].T.astype(BF16).astype(F32)
            dqkv_t[jr, pl.ds(h * HEAD_DIM, HEAD_DIM)] = rope_t(t, cos, sin).astype(BF16)
        t = dk_acc[trow(i), :].astype(BF16).astype(F32)
        dqkv_t[jr, pl.ds(dq, HEAD_DIM)] = rope_t(t, cos, sin).astype(BF16)
        dqkv_t[jr, pl.ds(dq + HEAD_DIM, HEAD_DIM)] = dv_acc[trow(i), :].astype(BF16)

    per = 6
    ticks = SUBS * (rg.nz - 1)

    @pl.loop(0, np_)
    def _(it):
        ip = np_ - 1 - it
        sl = it % 2

        def tick(n):
            at = 1 + per * it + n
            sc.tick(1 + at // SUBS, at % SUBS)

        tick(0)
        attn(2 * ip + 1, 1)
        tick(1)
        attn(2 * ip, 0)
        tick(2)
        dqkv_ref[trow(ip, 2 * TILE), :] = dqkv_t[...]

        for n in range(4):
            @pl.when(it >= 2)
            def _():
                for j in range(2):
                    dh_mine(2 * (ip + 2) + j, sl, j, n).wait()
                    dh_other(2 * (ip + 2) + j, sl, j, n).wait_send()
            ns = pl.ds(n * NC, NC)
            stage[sl, :, ns] = dot(dqkv_t[...], w_all[ns, :], NT).astype(BF16)
            for j in range(2):
                dh_mine(2 * ip + j, sl, j, n).start()
                dh_other(2 * ip + j, sl, j, n).start()
            if n < 3:
                tick(3 + n)

    @pl.loop(1 + per * np_, ticks)
    def _(at):
        sc.tick(1 + at // SUBS, at % SUBS)
    gd.drain()
    sc.drain()
    for it in (np_ - 2, np_ - 1):
        ip = np_ - 1 - it
        for j in range(2):
            for n in range(4):
                dh_mine(2 * ip + j, it % 2, j, n).wait()
                dh_other(2 * ip + j, it % 2, j, n).wait_send()

    wait_bytes(dh_peer, drs)


def second_kernel(tp, dh_own, dh_peer, mix_own, mix_peer, part1_ref, x_hbm, dy_hbm, g_ref, h_full, dy_full, dqkv_ref, ot_ref,
                  out_ref, gx_ref, dg_ref, dwq, dwk, dwv, dwo,
                  x_ref, dy_ref, xsem, ht, yt, skv, peer, dhr, part, slots, tot, hsem, ysem, pss, prs, gss, grs, bss, brs, *rsem):
    rg = Ring(tp)
    rg.greet_all()
    rows, dm = x_ref.shape
    nz = rg.nz
    dq = dwq.shape[1]
    CB = dm // nz
    LAG = 3
    done = part1_ref.shape[-1]

    def final_a(d, u, val):
        dhr[:, pl.ds(d * sa.H + u * sa.CW, sa.CW)] = val.astype(BF16)

    def final_b(d, u, val):
        cs = pl.ds(d * sb.H + sb.off + u * sb.CW, sb.CW)
        out_ref[:, cs] = (x_ref[:, cs].astype(F32) + val).astype(BF16)

    sa = Scatter(rg, dh_own, dh_peer, 0, *rsem[:5], final_a)
    sb = Scatter(rg, mix_own, mix_peer, done, *rsem[5:], final_b)
    sa.start_loads(0)
    sb.start_loads(0)

    def col(it, n=None):
        return pl.ds(pl.multiple_of(it * CB, CB), CB)

    def hload(it):
        return pltpu.make_async_copy(h_full.at[:, col(it)], ht.at[it % 2], hsem.at[it % 2])

    def yload(it):
        return pltpu.make_async_copy(dy_full.at[:, col(it)], yt.at[it % 2], ysem.at[it % 2])

    hload(0).start()
    yload(0).start()
    xcp = [pltpu.make_async_copy(x_hbm, x_ref, xsem.at[0]), pltpu.make_async_copy(dy_hbm, dy_ref, xsem.at[1])]
    for cp in xcp:
        cp.start()
    rg.met(tp - 1)
    sa.init()
    for cp in xcp:
        cp.wait()
    for d in range(2):
        out_ref[:, pl.ds(d * sb.H, done)] = part1_ref[d]

    def to_peer(it):
        return remote(skv.at[it % 2], peer.at[it], pss.at[it % 2], prs.at[it], rg.pt)

    def pair_sum(it):
        to_peer(it).wait_recv()
        both = peer[it] + skv[it % 2]
        dwk[col(it), :] = both[:, :HEAD_DIM]
        dwv[col(it), :] = both[:, HEAD_DIM:]
        to_peer(it).wait_send()

    HC = CB // 2

    @pl.loop(0, nz)
    def _(it):
        sl = it % 2
        hload(it).wait()
        yload(it).wait()

        @pl.when(it + 1 < nz)
        def _():
            hload(it + 1).start()
            yload(it + 1).start()

        @pl.when(it == LAG)
        def _():
            sb.init()

        def tick(u):
            @pl.when(it > 0)
            def _():
                sa.tick(it, u)

            @pl.when(it > LAG)
            def _():
                sb.tick(it - LAG, u)

        for n in range(2):
            tick(2 * n)
            hs = pl.ds(n * HC, HC)
            at = pl.ds(pl.multiple_of(it * CB + n * HC, HC), HC)
            dw = dot(ht[sl, :, hs], dqkv_ref[...], TN)
            dwq[at, :] = dw[:, :dq].astype(BF16)
            skv[sl, hs, :] = dw[:, dq:]
            tick(2 * n + 1)
            dwo[:, at] = dot(ot_ref[...], yt[sl, :, hs]).astype(BF16)
        to_peer(it).start()

        @pl.when(it >= 1)
        def _():
            pair_sum(it - 1)

    RB = 16
    part[...] = jnp.zeros_like(part)

    @pl.loop(0, rows // RB)
    def _(r):
        rr = trow(r, RB)
        xf = x_ref[rr, :].astype(F32)
        inv = lax.rsqrt(jnp.mean(xf * xf, axis=-1, keepdims=True) + NORM_EPS)
        xh = xf * inv
        dh = dhr[rr, :].astype(F32)
        part[...] += jnp.sum(dh * xh, axis=0, keepdims=True)
        a = dh * g_ref[...]
        di = inv * (a - xh * jnp.mean(a * xh, axis=-1, keepdims=True))
        gx_ref[rr, :] = (dy_ref[rr, :].astype(F32) + di).astype(BF16)

    GW = dm // tp

    def gcol(dev):
        return pl.ds(pl.multiple_of(dev * GW, GW), GW)

    def dev(o):
        return lax.rem(rg.me + o, tp)

    def scat(o):
        return remote(part.at[:, gcol(dev(o))], slots.at[o], gss, grs, dev(o))

    for o in range(1, tp):
        scat(o).start()
    pair_sum(nz - 1)
    rest = list(range(nz - LAG, nz))
    for s in rest[:-2]:
        for u in range(SUBS):
            sb.tick(s, u)
    acc = part[:, gcol(rg.me)]
    wait_bytes(slots.at[pl.ds(1, tp - 1)], grs)
    for o in range(1, tp):
        acc = acc + slots[o]
    tot[...] = acc

    def bcast(o):
        return remote(tot, dg_ref.at[:, gcol(rg.me)], bss, brs, dev(o))

    for o in range(1, tp):
        bcast(o).start()
    dg_ref[:, gcol(rg.me)] = acc
    sa.drain()
    wait_bytes(slots.at[pl.ds(1, tp - 1)], gss)
    for s in rest[-2:]:
        for u in range(SUBS):
            sb.tick(s, u)
    wait_bytes(slots.at[pl.ds(1, tp - 1)], brs)
    wait_bytes(slots.at[pl.ds(1, tp - 1)], bss)
    sb.drain()


def write_kernel(n, *refs):
    sem = refs[-1]
    cps = [pltpu.make_async_copy(refs[i], refs[n + i], sem.at[i]) for i in range(n)]
    for cp in cps:
        cp.start()
    for cp in cps:
        cp.wait()


def solution(mesh):
    tp = mesh.shape["tp"]
    nz = tp // 2
    DMA = pltpu.SemaphoreType.DMA

    def device_step(x, dy, pos, gain, wq, wk, wv, wo):
        rows, dm = x.shape
        seq = rows * tp
        nt = seq // TILE
        dq = wq.shape[1]
        nh = dq // HEAD_DIM
        qr = nh * TILE
        wd = dq + 2 * HEAD_DIM
        kvr = tp // (wk.shape[1] // HEAD_DIM)
        expo = np.arange(0, HEAD_DIM, 2, dtype=np.float64) / HEAD_DIM
        frq = (ROPE_THETA ** -expo).astype(np.float32)
        frq = jnp.asarray(np.concatenate([frq, frq]).reshape(1, HEAD_DIM))
        g2 = gain.reshape(1, dm)
        pos2 = pos.reshape(nt, TILE)

        def sds(shape, dt):
            return jax.ShapeDtypeStruct(shape, dt)

        V = pltpu.VMEM
        full = sds((seq, dm), BF16)
        blocks = sds((nt, rows, dm), BF16)
        W1 = dm // 3
        W2 = dm // 2 - W1
        h_full, dy_full, mix_own, mix_peer, dh_own, dh_peer, ot, dqkv, part1 = pl.pallas_call(
            functools.partial(first_kernel, tp, kvr),
            out_shape=[full, full, blocks, blocks, blocks, blocks, V((dq, seq), BF16), V((seq, wd), BF16), V((2, rows, W1), BF16)],
            in_specs=[ANY, VM, VM, VM, ANY, ANY, ANY, ANY, ANY],
            out_specs=[ANY] * 6 + [VM] * 3,
            scratch_shapes=[V((rows, dm), BF16), V((rows, dm), BF16), V((dm, wd), BF16), V((dq, dm), BF16), V((2, 2 * TILE, dm), BF16), V((2, 2 * TILE, dm), BF16),
                            V((nt, qr, HEAD_DIM), BF16), V((seq, HEAD_DIM), BF16), V((seq, HEAD_DIM), BF16), V((HEAD_DIM, seq), BF16),
                            V((HEAD_DIM, seq), BF16), V((nt, 2, qr), F32), V((seq, HEAD_DIM), F32), V((seq, HEAD_DIM), F32), V((seq, TILE), F32),
                            V((nt, TILE), F32), V((seq, HEAD_DIM), F32), V((seq, HEAD_DIM), F32), V((nt, qr, HEAD_DIM), BF16),
                            V((2 * TILE, wd), BF16), DMA, DMA((4,)), DMA((2,)), DMA((2, 2)), DMA((2,)), DMA((2,)), DMA, DMA((2, 2, 4)), DMA((2, 2, 4)), DMA]
            + Gather.scratch(tp) + Gather.scratch(tp) + Scatter.scratch(tp, rows, W1),
            compiler_params=pltpu.CompilerParams(collective_id=1, has_side_effects=True, vmem_limit_bytes=58 * 1024 * 1024),
            name="gather_attend_scatter",
        )(x, g2, pos2, frq, dy, wq, wk, wv, wo)

        ot, dqkv, part1 = (pltpu.with_memory_space_constraint(a, pltpu.VMEM) for a in (ot, dqkv, part1))
        CB = dm // nz
        res = pl.pallas_call(
            functools.partial(second_kernel, tp),
            out_shape=[V((rows, dm), BF16), V((rows, dm), BF16), V((1, dm), F32), V((dm, dq), BF16), V((dm, HEAD_DIM), F32),
                       V((dm, HEAD_DIM), F32), V((dq, dm), BF16)],
            in_specs=[ANY, ANY, ANY, ANY, VM, ANY, ANY, VM, ANY, ANY, VM, VM],
            out_specs=[VM] * 7,
            scratch_shapes=[V((rows, dm), BF16), V((rows, dm), BF16), DMA((2,)), V((2, seq, CB), BF16), V((2, seq, CB), BF16), V((2, CB, 2 * HEAD_DIM), F32), V((nz, CB, 2 * HEAD_DIM), F32),
                            V((rows, dm), BF16), V((1, dm), F32), V((tp, 1, dm // tp), F32), V((1, dm // tp), F32),
                            DMA((2,)), DMA((2,)), DMA((2,)), DMA((nz,)), DMA, DMA, DMA, DMA]
            + Scatter.scratch(tp, rows, dm // 2) + Scatter.scratch(tp, rows, W2),
            compiler_params=pltpu.CompilerParams(collective_id=2, has_side_effects=True, vmem_limit_bytes=40 * 1024 * 1024),
            name="scatter_grads",
        )(dh_own, dh_peer, mix_own, mix_peer, part1, x, dy, g2, h_full, dy_full, dqkv, ot)
        out, grad_x, d_gain, d_wq, d_wk, d_wv, d_wo = pl.pallas_call(
            functools.partial(write_kernel, len(res)),
            out_shape=[sds(r.shape, r.dtype) for r in res],
            in_specs=[VM] * len(res),
            out_specs=[ANY] * len(res),
            scratch_shapes=[DMA((len(res),))],
            compiler_params=pltpu.CompilerParams(vmem_limit_bytes=1024 * 1024),
            name="write_results",
        )(*res)
        return out, grad_x, d_wq, d_wk, d_wv, d_wo, d_gain.reshape(dm)

    specs_in = (P(('dp', 'tp'), None), P(('dp', 'tp'), None), P('dp'), P(), P(None, 'tp'), P(), P(), P('tp', None))
    specs_out = (P(('dp', 'tp'), None), P(('dp', 'tp'), None), P('dp', 'tp'), P('dp', 'tp'), P('dp', 'tp'), P(('dp', 'tp'), None), P('dp'))
    return jax.shard_map(device_step, mesh=mesh, in_specs=specs_in, out_specs=specs_out, check_vma=False)
```

```python
import functools
import jax
import jax.numpy as jnp
import numpy as np
from jax import lax
from jax.experimental import pallas as pl
from jax.experimental.pallas import tpu as pltpu
from jax.sharding import PartitionSpec as P

HEAD_DIM = 128
TILE = 128
SUBS = 4
SCORE_SCALE = HEAD_DIM ** -0.5
ROPE_THETA = 1000000.0
NORM_EPS = 1e-05
MASKED = -1e30
MESH = pl.DeviceIdType.MESH
F32 = jnp.float32
BF16 = jnp.bfloat16
ANY = pl.BlockSpec(memory_space=pl.ANY)
VM = pl.BlockSpec(memory_space=pltpu.VMEM)
NT = (((1,), (1,)), ((), ()))
TN = (((0,), (0,)), ((), ()))
VMEM_LIMIT = 63 * 1024 * 1024


def dot(a, b, dims=(((1,), (0,)), ((), ()))):
    return lax.dot_general(a, b, dims, preferred_element_type=F32)


class Ring:
    def __init__(self, tp):
        self.tp = tp
        self.nz = tp // 2
        self.me = lax.axis_index("tp")
        self.c = self.me // 2
        self.k = self.me % 2
        self.up = lax.rem(self.c + 1, self.nz) * 2 + self.k
        self.dn = lax.rem(self.c + self.nz - 1, self.nz) * 2 + self.k
        self.pt = self.c * 2 + 1 - self.k

    def greet(self, devs):
        bar = pltpu.get_barrier_semaphore()
        for d in devs:
            pl.semaphore_signal(bar, inc=1, device_id={"tp": d}, device_id_type=MESH)

    def greet_near(self):
        self.greet((self.up, self.dn, self.pt))

    def met(self, count):
        pl.semaphore_wait(pltpu.get_barrier_semaphore(), count)

    def chip(self, n):
        return lax.rem(n + 2 * self.nz, self.nz)


def remote(src, dst, ss, rs, dev):
    return pltpu.make_async_remote_copy(src, dst, ss, rs, device_id={"tp": dev}, device_id_type=MESH)


def wait_bytes(ref, sem):
    pltpu.make_async_copy(ref, ref, sem).wait()


class Gather:
    def __init__(self, rg, src, dst, rows, ss, rs, drs, ls):
        self.rg, self.src, self.dst, self.R = rg, src, dst, rows
        self.ss, self.rs, self.drs, self.ls = ss, rs, drs, ls
        self.H = rows // 2
        self.steps = rg.nz - 1

    def rows(self, chip, core, half):
        return pl.ds(pl.multiple_of((self.rg.chip(chip) * 2 + core) * self.R + half * self.H, self.H), self.H)

    def half(self, d, s):
        return s % 2 if d == 0 else 1 - s % 2

    def origin(self, d, s):
        h = (s + 2) // 2
        return self.rg.c - h if d == 0 else self.rg.c + h

    def dev(self, d):
        return self.rg.up if d == 0 else self.rg.dn

    def own(self, d, s):
        h = self.half(d, s)
        return remote(self.src.at[pl.ds(h * self.H, self.H), :], self.dst.at[self.rows(self.rg.c, self.rg.k, h), :],
                      self.ss, self.rs.at[d, s], self.dev(d))

    def recv_rows(self, d, s, core):
        return self.rows(self.origin(d, s), core, self.half(d, s))

    def fwd(self, d, s):
        r = self.recv_rows(d, s - 2, self.rg.k)
        return remote(self.dst.at[r, :], self.dst.at[r, :], self.ss, self.rs.at[d, s], self.dev(d))

    def recv(self, d, s):
        r = self.recv_rows(d, s, self.rg.k)
        return remote(self.dst.at[r, :], self.dst.at[r, :], self.ss, self.rs.at[d, s], self.dev(d))

    def pair(self, d, s):
        r = self.recv_rows(d, s, self.rg.k)
        return remote(self.dst.at[r, :], self.dst.at[r, :], self.ss, self.drs.at[s // 2], self.rg.pt)

    def block(self, dev):
        return pl.ds(pl.multiple_of(dev * self.R, self.R), self.R)

    def pair_own(self):
        return remote(self.src, self.dst.at[self.block(self.rg.me), :], self.ss, self.drs.at[0], self.rg.pt)

    def local(self):
        return pltpu.make_async_copy(self.src, self.dst.at[self.block(self.rg.me), :], self.ls)

    def start_ring(self, s):
        for d in range(2):
            self.own(d, s).start()

    def start_local(self):
        self.local().start()
        self.pair_own().start()

    def tick(self, s):
        for d in range(2):
            self.recv(d, s).wait_recv()
            if s + 2 < self.steps:
                self.fwd(d, s + 2).start()
            self.pair(d, s).start()

    def wait_pair(self, g):
        n = 2 * self.H * min(2, self.steps - 2 * g)
        if g == 0:
            self.local().wait()
            n += self.R
        wait_bytes(self.dst.at[pl.ds(0, n), :], self.drs.at[g])

    def groups(self):
        return (self.steps + 1) // 2

    def drain(self):
        wait_bytes(self.dst.at[pl.ds(0, self.R + 4 * self.H * self.steps), :], self.ss)

    @staticmethod
    def scratch(tp):
        n = tp // 2 - 1
        dma = pltpu.SemaphoreType.DMA
        return [dma, dma((2, n)), dma(((n + 1) // 2,)), dma]


class Scatter:
    def __init__(self, rg, own, peer, off, pre, psem, buf, ss, rs, final):
        self.rg, self.own, self.peer, self.pre, self.psem = rg, own, peer, pre, psem
        self.buf, self.ss, self.rs, self.final = buf, ss, rs, final
        self.H = own.shape[-1] // 2
        self.W = pre.shape[-1]
        self.off = off
        self.CW = self.W // SUBS

    def blk(self, d, s):
        return self.rg.chip(self.rg.c - 1 - s) if d == 0 else self.rg.chip(self.rg.c + 1 + s)

    def load(self, w, d, s):
        src = (self.own, self.peer)[w].at[self.blk(d, s), :, pl.ds(d * self.H + self.off, self.W)]
        return pltpu.make_async_copy(src, self.pre.at[s % 2, w, d], self.psem.at[s % 2, w, d])

    def start_loads(self, s):
        for w in range(2):
            for d in range(2):
                self.load(w, d, s).start()

    def wait_loads(self, s):
        for w in range(2):
            for d in range(2):
                self.load(w, d, s).wait()

    def send(self, d, u, s):
        return remote(self.buf.at[d, u, s], self.buf.at[d, u, s + 1], self.ss, self.rs.at[d, u, s],
                      self.rg.up if d == 0 else self.rg.dn)

    def cols(self, u):
        return pl.ds(u * self.CW if isinstance(u, int) else pl.multiple_of(u * self.CW, self.CW), self.CW)

    def mine(self, d, s, u):
        c = self.cols(u)
        return self.pre[s % 2, 0, d, :, c].astype(F32) + self.pre[s % 2, 1, d, :, c].astype(F32)

    def init(self):
        self.wait_loads(0)
        self.start_loads(1)
        for u in range(SUBS):
            for d in range(2):
                self.buf[d, u, 0] = self.mine(d, 0, u).astype(BF16)
                self.send(d, u, 0).start()

    def tick(self, s, u):
        last = self.rg.nz - 1

        def loads():
            self.wait_loads(s)

            @pl.when(s < last)
            def _():
                self.start_loads(s + 1)

        if isinstance(u, int):
            if u == 0:
                loads()
        else:
            pl.when(u == 0)(loads)
        for d in range(2):
            self.send(d, u, s - 1).wait_recv()

            @pl.when(s < last)
            def _():
                self.buf[d, u, s] = (self.mine(d, s, u) + self.buf[d, u, s].astype(F32)).astype(BF16)
                self.send(d, u, s).start()

            @pl.when(s == last)
            def _():
                self.final(d, u, self.mine(d, s, u) + self.buf[d, u, s].astype(F32))

    def drain(self):
        wait_bytes(self.buf.at[:, :, pl.ds(0, self.rg.nz - 1)], self.ss)

    @staticmethod
    def scratch(tp, rows, W):
        nz = tp // 2
        dma = pltpu.SemaphoreType.DMA
        return [pltpu.VMEM((2, 2, 2, rows, W), BF16), dma((2, 2, 2)), pltpu.VMEM((2, SUBS, nz, rows, W // SUBS), BF16),
                dma, dma((2, SUBS, nz - 1))]


def weight_copies(kv, wq, wk, wv, wo, w_all, wo_v, sem):
    dq = wq.shape[1]
    kvc = pl.ds(pl.multiple_of(kv * HEAD_DIM, HEAD_DIM), HEAD_DIM)
    return [pltpu.make_async_copy(wq, w_all.at[:, pl.ds(0, dq)], sem.at[0]),
            pltpu.make_async_copy(wk.at[:, kvc], w_all.at[:, pl.ds(dq, HEAD_DIM)], sem.at[1]),
            pltpu.make_async_copy(wv.at[:, kvc], w_all.at[:, pl.ds(dq + HEAD_DIM, HEAD_DIM)], sem.at[2]),
            pltpu.make_async_copy(wo, wo_v, sem.at[3])]


def rope(t, cos, sin):
    return t * cos + pltpu.roll(t, HEAD_DIM // 2, 1) * sin


def rope_t(t, cos, sin):
    return t * cos - pltpu.roll(t, HEAD_DIM // 2, 1) * sin


def to_col(row):
    return jnp.broadcast_to(row, (TILE, TILE)).T


def trow(i, n=TILE):
    return pl.ds(pl.multiple_of(i * n, n), n)


def keep_t(kdc, kdr, i, seq):
    key = lax.broadcasted_iota(jnp.int32, (seq, TILE), 0)
    qry = lax.broadcasted_iota(jnp.int32, (seq, TILE), 1) + i * TILE
    return (key <= qry) & (kdc == kdr)


def first_kernel(tp, kvr, x_hbm, g_ref, pos_ref, frq_ref, dy_ref, wq, wk, wv, wo,
                 h_full, dy_full, mix_own, mix_peer, dh_own, dh_peer, ot_ref, dqkv_ref, out_ref,
                 x_ref, hown, w_all, wo_v, tile, stage, q3_ref, k_ref, v_ref, vt, kt, st_ref, cos_ref, sin_ref, kdc_ref, kdr_ref,
                 dk_acc, dv_acc, do3, dqkv_t, xsem, wsem, tsem, ysem, msem, mss, mrs, dsem, dss, drs, *sems):
    rg = Ring(tp)
    rg.greet_near()
    xcp = pltpu.make_async_copy(x_hbm, x_ref, xsem)
    xcp.start()
    rows, dm = x_ref.shape
    seq = rows * tp
    nt = seq // TILE
    np_ = nt // 2
    dq = wq.shape[1]
    nh = dq // HEAD_DIM
    half = TILE // 2
    ga = Gather(rg, hown, h_full, rows, *sems[:4])
    gd = Gather(rg, dy_ref, dy_full, rows, *sems[4:8])

    def final(d, u, val):
        xs = pl.ds(pl.multiple_of(d * sc.H + u * sc.CW, sc.CW), sc.CW)
        out_ref[d, :, sc.cols(u)] = (x_ref[:, xs].astype(F32) + val).astype(BF16)

    sc = Scatter(rg, mix_own, mix_peer, 0, *sems[8:], final)
    wcp = weight_copies(rg.me // kvr, wq, wk, wv, wo, w_all, wo_v, wsem)
    RB = 16
    xcp.wait()

    @pl.loop(0, rows // RB)
    def _(r):
        xf = x_ref[trow(r, RB), :].astype(F32)
        inv = lax.rsqrt(jnp.mean(xf * xf, axis=-1, keepdims=True) + NORM_EPS)
        hown[trow(r, RB), :] = (xf * inv * g_ref[...]).astype(BF16)

    rg.met(3)
    ga.start_ring(0)
    ga.start_ring(1)
    ga.start_local()
    gd.start_local()
    for cp in wcp:
        cp.start()
    lane = lax.broadcasted_iota(jnp.int32, (TILE, TILE), 1)
    sgn = jnp.where(lane < HEAD_DIM // 2, -1.0, 1.0).astype(F32)
    kdr_ref[...] = (pos_ref[...] - (lax.broadcasted_iota(jnp.int32, pos_ref.shape, 0) * TILE
                                    + lax.broadcasted_iota(jnp.int32, pos_ref.shape, 1))).astype(F32)

    @pl.loop(0, nt)
    def _(i):
        ang = to_col(pos_ref[pl.ds(i, 1), :].astype(F32)) * frq_ref[...]
        cos_ref[trow(i), :] = jnp.cos(ang)
        sin_ref[trow(i), :] = jnp.sin(ang) * sgn
        kdc_ref[trow(i), :] = to_col(kdr_ref[pl.ds(i, 1), :])

    dk_acc[...] = jnp.zeros_like(dk_acc)
    dv_acc[...] = jnp.zeros_like(dv_acc)
    for s in range(ga.steps):
        ga.tick(s)
        if s >= ga.steps - 2:
            gd.start_ring(s - (ga.steps - 2))
    for n in range(ga.groups()):
        ga.wait_pair(n)
    for cp in wcp:
        cp.wait()

    def hload(i):
        return pltpu.make_async_copy(h_full.at[trow(i, 2 * TILE), :], tile.at[i % 2], tsem.at[i % 2])

    hload(0).start()

    @pl.loop(0, np_)
    def _(p):
        hload(p).wait()

        @pl.when(p + 1 < np_)
        def _():
            hload(p + 1).start()

        @pl.when(p == np_ // 2)
        def _():
            gd.tick(0)
        qkv = dot(tile[p % 2], w_all[...])
        for j in range(2):
            i = 2 * p + j
            js = slice(j * TILE, (j + 1) * TILE)
            cos, sin = cos_ref[trow(i), :], sin_ref[trow(i), :]
            for h in range(nh + 1):
                t = qkv[js, h * HEAD_DIM:(h + 1) * HEAD_DIM].astype(BF16).astype(F32)
                t = rope(t, cos, sin)
                if h < nh:
                    q3_ref[i, pl.ds(h * TILE, TILE), :] = t.astype(BF16)
                else:
                    k_ref[trow(i), :] = t.astype(BF16)
                    kt[:, trow(i)] = t.T.astype(BF16)
            v = qkv[js, (nh + 1) * HEAD_DIM:]
            v_ref[trow(i), :] = v.astype(BF16)
            vt[:, trow(i)] = v.T.astype(BF16)

    def half_rows(j, core):
        return pl.ds(pl.multiple_of(j * TILE + core * half, half), half)

    def mix_mine(i):
        return pltpu.make_async_copy(stage.at[i % 2, half_rows(0, rg.k), :], mix_own.at[i], msem.at[i % 2])

    def mix_other(i):
        return remote(stage.at[i % 2, half_rows(0, 1 - rg.k), :], mix_peer.at[i], mss.at[i % 2], mrs, rg.pt)

    NC = dm // 4

    @pl.loop(0, nt)
    def _(i):
        for n in range(2):
            @pl.when(i == n * np_)
            def _():
                gd.tick(1 + n)

        s = dot(k_ref[...], q3_ref[i], NT) * SCORE_SCALE
        keep = keep_t(kdc_ref[...], kdr_ref[pl.ds(i, 1), :], i, seq)
        pbs = []
        for h in range(nh):
            sh = jnp.where(keep, s[:, h * TILE:(h + 1) * TILE], MASKED)
            m = jnp.max(sh, axis=0, keepdims=True)
            e = jnp.exp(sh - m)
            li = 1.0 / jnp.sum(e, axis=0, keepdims=True)
            st_ref[i, pl.ds(0, 1), pl.ds(h * TILE, TILE)] = m
            st_ref[i, pl.ds(1, 1), pl.ds(h * TILE, TILE)] = li
            pbs.append((e * li).astype(BF16))
        ot = dot(vt[...], jnp.concatenate(pbs, axis=1))
        os = []
        for h in range(nh):
            oh = ot[:, h * TILE:(h + 1) * TILE]
            ot_ref[pl.ds(h * HEAD_DIM, HEAD_DIM), trow(i)] = oh.astype(BF16)
            os.append(oh.T.astype(BF16))
        o = jnp.concatenate(os, axis=1)

        @pl.when(i >= 2)
        def _():
            mix_mine(i - 2).wait()
            mix_other(i - 2).wait_send()
        for n in range(4):
            ns = pl.ds(n * NC, NC)
            stage[i % 2, pl.ds(0, TILE), ns] = dot(o, wo_v[:, ns]).astype(BF16)
        mix_mine(i).start()
        mix_other(i).start()

    for i in (nt - 2, nt - 1):
        mix_mine(i).wait()
        mix_other(i).wait_send()
    wait_bytes(mix_peer, mrs)
    sc.start_loads(0)

    def yload(chip, sl, j):
        return pltpu.make_async_copy(dy_full.at[trow(rg.chip(chip)), :], tile.at[sl, pl.ds(j * TILE, TILE), :], ysem.at[sl, j])

    def pair_of(g):
        return (rg.c + g + 1, rg.c - g - 1) if g + 1 < np_ else (rg.c + np_, rg.c)

    def start_y(g, js=(0, 1)):
        for j in js:
            yload(pair_of(g)[j], g % 2, j).start()

    def d_o(g, meanwhile=None):
        if meanwhile is not None:
            meanwhile()
        for j in range(2):
            yload(pair_of(g)[j], g % 2, j).wait()
        do = dot(tile[g % 2], wo_v[...], NT).astype(BF16)
        for j in range(2):
            t = rg.chip(pair_of(g)[j])
            for h in range(nh):
                do3[t, pl.ds(h * TILE, TILE), :] = do[j * TILE:(j + 1) * TILE, h * HEAD_DIM:(h + 1) * HEAD_DIM]

    gd.tick(3)
    gd.wait_pair(0)
    gd.wait_pair(1)
    start_y(0)
    start_y(1)
    gd.tick(4)
    sc.init()
    ga.drain()
    d_o(0)
    d_o(1)
    start_y(3, (1,))
    gd.tick(5)
    gd.wait_pair(2)
    start_y(2)
    d_o(2)
    gd.tick(6)
    gd.wait_pair(3)
    start_y(3, (0,))
    d_o(3, lambda: sc.tick(jnp.int32(1), 0))

    def dh_mine(i, sl, j, n):
        ns = pl.ds(n * NC, NC)
        return pltpu.make_async_copy(stage.at[sl, half_rows(j, rg.k), ns], dh_own.at[i, :, ns], dsem.at[sl, j, n])

    def dh_other(i, sl, j, n):
        ns = pl.ds(n * NC, NC)
        return remote(stage.at[sl, half_rows(j, 1 - rg.k), ns], dh_peer.at[i, :, ns], dss.at[sl, j, n], drs, rg.pt)

    def attn(i, j):
        q3 = q3_ref[i]
        do = do3[i]
        s = dot(k_ref[...], q3, NT) * SCORE_SCALE
        keep = keep_t(kdc_ref[...], kdr_ref[pl.ds(i, 1), :], i, seq)
        dp = dot(v_ref[...], do, NT)
        pbs, dss_ = [], []
        for h in range(nh):
            hs = slice(h * TILE, (h + 1) * TILE)
            m = st_ref[i, pl.ds(0, 1), pl.ds(h * TILE, TILE)]
            li = st_ref[i, pl.ds(1, 1), pl.ds(h * TILE, TILE)]
            p = jnp.exp(jnp.where(keep, s[:, hs], MASKED) - m) * li
            dph = dp[:, hs].astype(BF16).astype(F32)
            dl = jnp.sum(dph * p, axis=0, keepdims=True)
            dss_.append((p * (dph - dl) * SCORE_SCALE).astype(BF16))
            pbs.append(p.astype(BF16))
        pb = jnp.concatenate(pbs, axis=1)
        ds = jnp.concatenate(dss_, axis=1)
        dv_acc[...] += dot(pb, do)
        dk_acc[...] += dot(ds, q3)
        dqt = dot(kt[...], ds)
        cos, sin = cos_ref[trow(i), :], sin_ref[trow(i), :]
        jr = pl.ds(j * TILE, TILE)
        for h in range(nh):
            t = dqt[:, h * TILE:(h + 1) * TILE].T.astype(BF16).astype(F32)
            dqkv_t[jr, pl.ds(h * HEAD_DIM, HEAD_DIM)] = rope_t(t, cos, sin).astype(BF16)
        t = dk_acc[trow(i), :].astype(BF16).astype(F32)
        dqkv_t[jr, pl.ds(dq, HEAD_DIM)] = rope_t(t, cos, sin).astype(BF16)
        dqkv_t[jr, pl.ds(dq + HEAD_DIM, HEAD_DIM)] = dv_acc[trow(i), :].astype(BF16)

    per = 6
    ticks = SUBS * (rg.nz - 1)

    @pl.loop(0, np_)
    def _(it):
        ip = np_ - 1 - it
        sl = it % 2

        def tick(n):
            at = 1 + per * it + n
            sc.tick(1 + at // SUBS, at % SUBS)

        tick(0)
        attn(2 * ip + 1, 1)
        tick(1)
        attn(2 * ip, 0)
        tick(2)
        dqkv_ref[trow(ip, 2 * TILE), :] = dqkv_t[...]

        for n in range(4):
            @pl.when(it >= 2)
            def _():
                for j in range(2):
                    dh_mine(2 * (ip + 2) + j, sl, j, n).wait()
                    dh_other(2 * (ip + 2) + j, sl, j, n).wait_send()
            ns = pl.ds(n * NC, NC)
            stage[sl, :, ns] = dot(dqkv_t[...], w_all[ns, :], NT).astype(BF16)
            for j in range(2):
                dh_mine(2 * ip + j, sl, j, n).start()
                dh_other(2 * ip + j, sl, j, n).start()
            if n < 3:
                tick(3 + n)

    @pl.loop(1 + per * np_, ticks)
    def _(at):
        sc.tick(1 + at // SUBS, at % SUBS)
    gd.drain()
    sc.drain()
    for it in (np_ - 2, np_ - 1):
        ip = np_ - 1 - it
        for j in range(2):
            for n in range(4):
                dh_mine(2 * ip + j, it % 2, j, n).wait()
                dh_other(2 * ip + j, it % 2, j, n).wait_send()

    wait_bytes(dh_peer, drs)


def second_kernel(tp, dh_own, dh_peer, mix_own, mix_peer, part1_ref, x_hbm, dy_hbm, g_ref, h_full, dy_full, dqkv_ref, ot_ref,
                  out_ref, gx_ref, dg_ref, dwq, dwk, dwv, dwo,
                  x_ref, dy_ref, xsem, ht, yt, skv, peer, dhr, part, slots, tot, hsem, ysem, pss, prs, gss, grs, bss, brs, *rsem):
    rg = Ring(tp)
    rg.greet_near()
    rows, dm = x_ref.shape
    nz = rg.nz
    dq = dwq.shape[1]
    CB = dm // nz
    LAG = 3
    done = part1_ref.shape[-1]

    def final_a(d, u, val):
        dhr[:, pl.ds(d * sa.H + u * sa.CW, sa.CW)] = val.astype(BF16)

    def final_b(d, u, val):
        cs = pl.ds(d * sb.H + sb.off + u * sb.CW, sb.CW)
        out_ref[:, cs] = (x_ref[:, cs].astype(F32) + val).astype(BF16)

    sa = Scatter(rg, dh_own, dh_peer, 0, *rsem[:5], final_a)
    sb = Scatter(rg, mix_own, mix_peer, done, *rsem[5:], final_b)
    sa.start_loads(0)
    sb.start_loads(0)

    def col(it, n=None):
        return pl.ds(pl.multiple_of(it * CB, CB), CB)

    def hload(it):
        return pltpu.make_async_copy(h_full.at[:, col(it)], ht.at[it % 2], hsem.at[it % 2])

    def yload(it):
        return pltpu.make_async_copy(dy_full.at[:, col(it)], yt.at[it % 2], ysem.at[it % 2])

    hload(0).start()
    yload(0).start()
    xcp = [pltpu.make_async_copy(x_hbm, x_ref, xsem.at[0]), pltpu.make_async_copy(dy_hbm, dy_ref, xsem.at[1])]
    for cp in xcp:
        cp.start()
    rg.met(3)
    sa.init()
    for cp in xcp:
        cp.wait()
    for d in range(2):
        out_ref[:, pl.ds(d * sb.H, done)] = part1_ref[d]

    def to_peer(it):
        return remote(skv.at[it % 2], peer.at[it], pss.at[it % 2], prs.at[it], rg.pt)

    def pair_sum(it):
        to_peer(it).wait_recv()
        both = peer[it] + skv[it % 2]
        dwk[col(it), :] = both[:, :HEAD_DIM]
        dwv[col(it), :] = both[:, HEAD_DIM:]
        to_peer(it).wait_send()

    HC = CB // 2

    @pl.loop(0, nz)
    def _(it):
        sl = it % 2
        hload(it).wait()
        yload(it).wait()

        @pl.when(it + 1 < nz)
        def _():
            hload(it + 1).start()
            yload(it + 1).start()

        @pl.when(it == LAG)
        def _():
            sb.init()

        def tick(u):
            @pl.when(it > 0)
            def _():
                sa.tick(it, u)

            @pl.when(it > LAG)
            def _():
                sb.tick(it - LAG, u)

        for n in range(2):
            tick(2 * n)
            hs = pl.ds(n * HC, HC)
            at = pl.ds(pl.multiple_of(it * CB + n * HC, HC), HC)
            dw = dot(ht[sl, :, hs], dqkv_ref[...], TN)
            dwq[at, :] = dw[:, :dq].astype(BF16)
            skv[sl, hs, :] = dw[:, dq:]
            tick(2 * n + 1)
            dwo[:, at] = dot(ot_ref[...], yt[sl, :, hs]).astype(BF16)
        to_peer(it).start()

        @pl.when(it >= 1)
        def _():
            pair_sum(it - 1)

    RB = 16
    part[...] = jnp.zeros_like(part)

    def normed(rr):
        xf = x_ref[rr, :].astype(F32)
        inv = lax.rsqrt(jnp.mean(xf * xf, axis=-1, keepdims=True) + NORM_EPS)
        return xf * inv, inv

    @pl.loop(0, rows // RB)
    def _(r):
        rr = trow(r, RB)
        part[...] += jnp.sum(dhr[rr, :].astype(F32) * normed(rr)[0], axis=0, keepdims=True)

    GW = dm // tp

    def gcol(dev):
        return pl.ds(pl.multiple_of(dev * GW, GW), GW)

    def dev(o):
        return lax.rem(rg.me + o, tp)

    def scat(o):
        return remote(part.at[:, gcol(dev(o))], slots.at[o], gss, grs, dev(o))

    for o in range(1, tp):
        scat(o).start()

    @pl.loop(0, rows // RB)
    def _(r):
        rr = trow(r, RB)
        xh, inv = normed(rr)
        a = dhr[rr, :].astype(F32) * g_ref[...]
        di = inv * (a - xh * jnp.mean(a * xh, axis=-1, keepdims=True))
        gx_ref[rr, :] = (dy_ref[rr, :].astype(F32) + di).astype(BF16)

    pair_sum(nz - 1)
    rest = list(range(nz - LAG, nz))
    for s in rest[:-2]:
        for u in range(SUBS):
            sb.tick(s, u)
    acc = part[:, gcol(rg.me)]
    wait_bytes(slots.at[pl.ds(1, tp - 1)], grs)
    for o in range(1, tp):
        acc = acc + slots[o]
    tot[...] = acc

    def bcast(o):
        return remote(tot, dg_ref.at[:, gcol(rg.me)], bss, brs, dev(o))

    for o in range(1, tp):
        bcast(o).start()
    dg_ref[:, gcol(rg.me)] = acc
    sa.drain()
    wait_bytes(slots.at[pl.ds(1, tp - 1)], gss)
    for s in rest[-2:]:
        for u in range(SUBS):
            sb.tick(s, u)
    wait_bytes(slots.at[pl.ds(1, tp - 1)], brs)
    wait_bytes(slots.at[pl.ds(1, tp - 1)], bss)
    sb.drain()


def write_kernel(n, *refs):
    sem = refs[-1]
    cps = [pltpu.make_async_copy(refs[i], refs[n + i], sem.at[i]) for i in range(n)]
    for cp in cps:
        cp.start()
    for cp in cps:
        cp.wait()


def solution(mesh):
    tp = mesh.shape["tp"]
    nz = tp // 2
    DMA = pltpu.SemaphoreType.DMA

    def device_step(x, dy, pos, gain, wq, wk, wv, wo):
        rows, dm = x.shape
        seq = rows * tp
        nt = seq // TILE
        dq = wq.shape[1]
        nh = dq // HEAD_DIM
        qr = nh * TILE
        wd = dq + 2 * HEAD_DIM
        kvr = tp // (wk.shape[1] // HEAD_DIM)
        expo = np.arange(0, HEAD_DIM, 2, dtype=np.float64) / HEAD_DIM
        frq = (ROPE_THETA ** -expo).astype(np.float32)
        frq = jnp.asarray(np.concatenate([frq, frq]).reshape(1, HEAD_DIM))
        g2 = gain.reshape(1, dm)
        pos2 = pos.reshape(nt, TILE)

        def sds(shape, dt):
            return jax.ShapeDtypeStruct(shape, dt)

        V = pltpu.VMEM
        full = sds((seq, dm), BF16)
        blocks = sds((nt, rows, dm), BF16)
        W1 = dm // 3
        W2 = dm // 2 - W1
        h_full, dy_full, mix_own, mix_peer, dh_own, dh_peer, ot, dqkv, part1 = pl.pallas_call(
            functools.partial(first_kernel, tp, kvr),
            out_shape=[full, full, blocks, blocks, blocks, blocks, V((dq, seq), BF16), V((seq, wd), BF16), V((2, rows, W1), BF16)],
            in_specs=[ANY, VM, VM, VM, ANY, ANY, ANY, ANY, ANY],
            out_specs=[ANY] * 6 + [VM] * 3,
            scratch_shapes=[V((rows, dm), BF16), V((rows, dm), BF16), V((dm, wd), BF16), V((dq, dm), BF16), V((2, 2 * TILE, dm), BF16), V((2, 2 * TILE, dm), BF16),
                            V((nt, qr, HEAD_DIM), BF16), V((seq, HEAD_DIM), BF16), V((seq, HEAD_DIM), BF16), V((HEAD_DIM, seq), BF16),
                            V((HEAD_DIM, seq), BF16), V((nt, 2, qr), F32), V((seq, HEAD_DIM), F32), V((seq, HEAD_DIM), F32), V((seq, TILE), F32),
                            V((nt, TILE), F32), V((seq, HEAD_DIM), F32), V((seq, HEAD_DIM), F32), V((nt, qr, HEAD_DIM), BF16),
                            V((2 * TILE, wd), BF16), DMA, DMA((4,)), DMA((2,)), DMA((2, 2)), DMA((2,)), DMA((2,)), DMA, DMA((2, 2, 4)), DMA((2, 2, 4)), DMA]
            + Gather.scratch(tp) + Gather.scratch(tp) + Scatter.scratch(tp, rows, W1),
            compiler_params=pltpu.CompilerParams(collective_id=1, has_side_effects=True, vmem_limit_bytes=58 * 1024 * 1024),
            name="gather_attend_scatter",
        )(x, g2, pos2, frq, dy, wq, wk, wv, wo)

        ot, dqkv, part1 = (pltpu.with_memory_space_constraint(a, pltpu.VMEM) for a in (ot, dqkv, part1))
        CB = dm // nz
        res = pl.pallas_call(
            functools.partial(second_kernel, tp),
            out_shape=[V((rows, dm), BF16), V((rows, dm), BF16), V((1, dm), F32), V((dm, dq), BF16), V((dm, HEAD_DIM), F32),
                       V((dm, HEAD_DIM), F32), V((dq, dm), BF16)],
            in_specs=[ANY, ANY, ANY, ANY, VM, ANY, ANY, VM, ANY, ANY, VM, VM],
            out_specs=[VM] * 7,
            scratch_shapes=[V((rows, dm), BF16), V((rows, dm), BF16), DMA((2,)), V((2, seq, CB), BF16), V((2, seq, CB), BF16), V((2, CB, 2 * HEAD_DIM), F32), V((nz, CB, 2 * HEAD_DIM), F32),
                            V((rows, dm), BF16), V((1, dm), F32), V((tp, 1, dm // tp), F32), V((1, dm // tp), F32),
                            DMA((2,)), DMA((2,)), DMA((2,)), DMA((nz,)), DMA, DMA, DMA, DMA]
            + Scatter.scratch(tp, rows, dm // 2) + Scatter.scratch(tp, rows, W2),
            compiler_params=pltpu.CompilerParams(collective_id=2, has_side_effects=True, vmem_limit_bytes=40 * 1024 * 1024),
            name="scatter_grads",
        )(dh_own, dh_peer, mix_own, mix_peer, part1, x, dy, g2, h_full, dy_full, dqkv, ot)
        out, grad_x, d_gain, d_wq, d_wk, d_wv, d_wo = pl.pallas_call(
            functools.partial(write_kernel, len(res)),
            out_shape=[sds(r.shape, r.dtype) for r in res],
            in_specs=[VM] * len(res),
            out_specs=[ANY] * len(res),
            scratch_shapes=[DMA((len(res),))],
            compiler_params=pltpu.CompilerParams(vmem_limit_bytes=1024 * 1024),
            name="write_results",
        )(*res)
        return out, grad_x, d_wq, d_wk, d_wv, d_wo, d_gain.reshape(dm)

    specs_in = (P(('dp', 'tp'), None), P(('dp', 'tp'), None), P('dp'), P(), P(None, 'tp'), P(), P(), P('tp', None))
    specs_out = (P(('dp', 'tp'), None), P(('dp', 'tp'), None), P('dp', 'tp'), P('dp', 'tp'), P('dp', 'tp'), P(('dp', 'tp'), None), P('dp'))
    return jax.shard_map(device_step, mesh=mesh, in_specs=specs_in, out_specs=specs_out, check_vma=False)
```
